32 devices in a mesh: wide: 8 (over y, x, core), narrow: 4 (over z).
Axes of the slice: x: 2, y: 2, z: 4, core: 2. Of those that a mesh axis runs over, the one named last changes fastest.
Arguments:
- tokens: bfloat16 [64, 512, 512], P(('wide', 'narrow')), may hold values from -6 to 6
- seg_ids: int32 [64, 512], P(('wide', 'narrow')), may hold values from 0 to 7, as said below
- positives: int32 [256], replicated, may hold values from 0 to 63
- norm1_gain: bfloat16 [512], replicated, may hold values from 0.5 to 1.5
- w_query: bfloat16 [512, 512], replicated, may hold values from -0.0625 to 0.0625
- w_key: bfloat16 [512, 512], replicated, may hold values from -0.25 to 0.25
- w_value: bfloat16 [512, 512], replicated, may hold values from -0.25 to 0.25
- w_attn_out: bfloat16 [512, 512], replicated, may hold values from -1 to 1
- rel_bias: bfloat16 [32, 8], replicated, may hold values from -4 to 4
- norm2_gain: bfloat16 [512], replicated, may hold values from 0.5 to 1.5
- w_in: bfloat16 [512, 2048], replicated, may hold values from -0.25 to 0.25
- w_ffn_out: bfloat16 [2048, 512], replicated, may hold values from -0.1875 to 0.1875
- w_proj: bfloat16 [512, 512], replicated, may hold values from -0.25 to 0.25
Outputs:
- loss: float32 [], replicated
- tokens_grad: bfloat16 [64, 512, 512], P(('wide', 'narrow'))
- norm1_gain_grad: float32 [512], replicated
- w_query_grad: float32 [512, 512], replicated
- w_key_grad: float32 [512, 512], replicated
- w_value_grad: float32 [512, 512], replicated
- w_attn_out_grad: float32 [512, 512], replicated
- rel_bias_grad: float32 [32, 8], replicated
- norm2_gain_grad: float32 [512], replicated
- w_in_grad: float32 [512, 2048], replicated
- w_ffn_out_grad: float32 [2048, 512], replicated
- w_proj_grad: float32 [512, 512], replicated
The draws below stay inside these ranges and needn't reach their ends.
Inputs may be any that keep to these rules, and one draw needn't show every extreme that they name: `seg_ids`: each row of the first half holds 8 queries of 64 tokens, numbered 0 to 7 in order. Each row of the second half holds passage 0 and then passage 1, each of 64 to 448 tokens; the first such row has a passage 0 of exactly 448 tokens. `positives`: passages are numbered by row of the second half and then by their number within the row.
All inputs are finite; a program needn't handle non-finite values.
Results may differ from the reference program's by a relative error of at most 0.04.
The reference program's roundings to bfloat16 on the way count: a program that leaves them out, or rounds other values in their place, can miss the bound.
Values may be sent and summed in bfloat16 or wider, within the bound.
No kernel may reach another device: no remote copies, remote signals or barrier semaphores. Data moves between devices by JAX's collectives and lax.ppermute only.
A program may use at most 192 MiB of HBM per device.

```python
import math
import jax
import jax.numpy as jnp
import numpy as np
from jax import lax

D = 512
FF = 2048
H = 8
DH = 64
NB = 32
MAXD = 128
PD = 512
L = 512
QLEN = 64
PPR = 2
PMOST = 448
SLOTS = 8
ROWS_ALL = 64
QUERIES = 256
PASSAGES = 64


def draw_seg_ids(key, part):
    half_rows = ROWS_ALL // 2
    positions = jnp.arange(L, dtype=jnp.int32)
    first_len = jax.random.randint(key, (half_rows,), L - PMOST, PMOST + 1, dtype=jnp.int32)
    first_len = jnp.where(jnp.arange(half_rows, dtype=jnp.int32) == 0, PMOST, first_len)
    passage_rows = (positions[None, :] >= first_len[:, None]).astype(jnp.int32)
    query_rows = jnp.broadcast_to(positions // QLEN, (half_rows, L))
    return jnp.concatenate([query_rows, passage_rows], axis=0).astype(jnp.int32)


def touch_ends(values, stream_key, low, largest):
    index_at = [jax.random.randint(jax.random.fold_in(stream_key, axis), (), 0, length) for axis, length in enumerate(values.shape)]
    longest = values.shape.index(max(values.shape))
    neighbour = index_at[:longest] + [(index_at[longest] + 1) % values.shape[longest]] + index_at[longest + 1:]
    return values.at[tuple(index_at)].set(low).at[tuple(neighbour)].set(largest)


def block_scale(own_key, extent, cuts, low, high):
    def one(position, shards_of):
        draws = jax.random.uniform(jax.random.fold_in(jax.random.fold_in(own_key, 6), position), (shards_of,), jnp.float32, low / len(cuts), high / len(cuts))
        return jnp.repeat(jnp.exp(draws), extent[position] // shards_of).reshape((-1,) + (1,) * (len(extent) - position - 1))

    level = one(*cuts[0])
    for cut in cuts[1:]:
        level = level * one(*cut)
    return level


def gaussian(stream_key, extent, width, limit, pieces=(), held_as=jnp.bfloat16):
    factor_of = block_scale(stream_key, extent, pieces, -0.22, 0.18) if pieces else 1.0
    values = jax.random.normal(stream_key, extent, jnp.float32) * width * factor_of
    return jnp.minimum(jnp.maximum(values, -limit), limit).astype(held_as)


def setup_inputs(seed: int = 0) -> dict:
    splits = jax.random.split(jax.random.key(seed), 14)
    return {
        "tokens": gaussian(splits[0], (ROWS_ALL, L, D), 1.0, 6.0, ((0, 32),)),
        "seg_ids": draw_seg_ids(jax.random.fold_in(splits[13], 71), 0),
        "positives": touch_ends(jax.random.randint(splits[2], (QUERIES,), 0, PASSAGES), jax.random.fold_in(splits[2], 1), 0, PASSAGES - 1).astype(jnp.int32),
        "norm1_gain": jnp.clip(1.0 + 0.1 * jax.random.normal(splits[3], (D,), jnp.float32), 0.5, 1.5).astype(jnp.bfloat16),
        "w_query": gaussian(splits[4], (D, D), (16 * D) ** -0.5, 0.0625),
        "w_key": gaussian(splits[5], (D, D), D ** -0.5, 0.25),
        "w_value": gaussian(splits[6], (D, D), D ** -0.5, 0.25),
        "w_attn_out": gaussian(splits[7], (D, D), (D // 16) ** -0.5, 1.0),
        "rel_bias": gaussian(splits[8], (NB, H), 1.0, 4.0),
        "norm2_gain": jnp.clip(1.0 + 0.1 * jax.random.normal(splits[9], (D,), jnp.float32), 0.5, 1.5).astype(jnp.bfloat16),
        "w_in": gaussian(splits[10], (D, FF), D ** -0.5, 0.25),
        "w_ffn_out": gaussian(splits[11], (FF, D), (FF // 2) ** -0.5, 0.1875),
        "w_proj": gaussian(splits[12], (D, PD), D ** -0.5, 0.25),
    }


@jax.custom_vjp
def low(v):
    return lax.optimization_barrier(v.astype(jnp.bfloat16)).astype(jnp.float32)

@jax.custom_vjp
def low_back(v):
    return v

def low_keep(v):
    return (low(v), None)

def low_pass(kept, grad):
    return (grad,)

def back_keep(v):
    return (v, None)

def back_low(kept, grad):
    return (low(grad),)
low.defvjp(low_keep, low_pass)
low_back.defvjp(back_keep, back_low)
EPS_NORM = 1e-06
LOGIT_SCALE = 50.0
MASKED = -1e+30

def bucket_offsets(length):
    offset = np.arange(-(length - 1), length)
    half_count = NB // 2
    exact_span = half_count // 2
    distance = -offset
    bucket = (distance < 0).astype(np.int64) * half_count
    distance = np.abs(distance)
    far_bucket = exact_span + (np.log(np.maximum(distance, 1) / exact_span) / np.log(MAXD / exact_span) * (half_count - exact_span)).astype(np.int64)
    far_bucket = np.minimum(far_bucket, half_count - 1)
    bucket = bucket + np.where(distance < exact_span, distance, far_bucket)
    return bucket.astype(np.int32)

def pair_buckets():
    table = bucket_offsets(L)
    return table[np.arange(L)[None, :] - np.arange(L)[:, None] + L - 1]

def matmul(left, right):
    return jnp.dot(left, right, precision=lax.Precision.HIGHEST)

def rms_scale(values):
    return lax.rsqrt(lax.optimization_barrier(jnp.mean(values * values, axis=-1, keepdims=True)) + EPS_NORM)

def encode_rows(params, rows, segments):
    gain_one, w_query, w_key, w_value, w_attn_out, rel_bias, gain_two, w_in, w_ffn_out, w_proj = params
    count_rows = rows.shape[0]
    bias_full = jnp.transpose(rel_bias[pair_buckets()], (2, 0, 1))
    normed_one = low(rows * rms_scale(rows) * gain_one)
    queries = low(low_back(matmul(normed_one, w_query))).reshape(count_rows, L, H, DH)
    keys_rows = low(low_back(matmul(normed_one, w_key))).reshape(count_rows, L, H, DH)
    values_rows = low(low_back(matmul(normed_one, w_value))).reshape(count_rows, L, H, DH)
    scores = jnp.einsum('rihd,rjhd->rhij', queries, keys_rows, precision=lax.Precision.HIGHEST) + bias_full[None]
    scores = low_back(scores)
    same_seg = segments[:, None, :, None] == segments[:, None, None, :]
    scores = jnp.where(same_seg, scores, MASKED)
    attn_probs = low(jax.nn.softmax(scores, axis=-1))
    attn_mixed = jnp.einsum('rhij,rjhd->rihd', attn_probs, values_rows, precision=lax.Precision.HIGHEST).reshape(count_rows, L, D)
    attn_mixed = low(low_back(attn_mixed))
    hidden = rows + low_back(matmul(attn_mixed, w_attn_out))
    normed_two = low(hidden * rms_scale(hidden) * gain_two)
    ffn_inner = low_back(matmul(normed_two, w_in))
    active = low(jnp.where(ffn_inner > 0, ffn_inner, 0.0))
    output = hidden + low_back(matmul(active, w_ffn_out))
    slot_mask = (segments[:, None, :] == jnp.arange(SLOTS, dtype=jnp.int32)[None, :, None]).astype(jnp.float32)
    counts = jnp.maximum(lax.optimization_barrier(jnp.sum(slot_mask, axis=-1, keepdims=True)), 1.0)
    pooled = low(jnp.einsum('rsl,rld->rsd', slot_mask, output, precision=lax.Precision.HIGHEST) / counts)
    projected = low_back(matmul(pooled, w_proj))
    embedded = low(projected * lax.rsqrt(lax.optimization_barrier(jnp.sum(projected * projected, axis=-1, keepdims=True)) + EPS_NORM))
    return embedded

def total_loss(rows, params, seg_ids, positives):
    per_block = math.gcd(ROWS_ALL, max(1, 4096 // L))
    grouped = rows.reshape(ROWS_ALL // per_block, per_block, L, D)
    seg_grouped = seg_ids.reshape(ROWS_ALL // per_block, per_block, L)
    encoder = jax.checkpoint(encode_rows)

    def encode_block(block):
        return encoder(params, block[0], block[1])
    embedded = lax.map(encode_block, (grouped, seg_grouped))
    embedded = embedded.reshape(ROWS_ALL, SLOTS, PD)
    half_rows = ROWS_ALL // 2
    query_emb = embedded[:half_rows].reshape(QUERIES, PD)
    passage_emb = embedded[half_rows:, :PPR].reshape(PASSAGES, PD)
    logits = low_back(LOGIT_SCALE * matmul(query_emb, passage_emb.T))
    pos_hits = (positives[:, None] == jnp.arange(PASSAGES, dtype=jnp.int32)[None, :]).astype(jnp.float32)
    return jnp.sum(jax.nn.logsumexp(logits, axis=-1) - lax.optimization_barrier(jnp.sum(logits * pos_hits, axis=-1)))

def reference(tokens, seg_ids, positives, norm1_gain, w_query, w_key, w_value, w_attn_out, rel_bias, norm2_gain, w_in, w_ffn_out, w_proj):
    params = (norm1_gain.astype(jnp.float32), w_query.astype(jnp.float32), w_key.astype(jnp.float32), w_value.astype(jnp.float32), w_attn_out.astype(jnp.float32), rel_bias.astype(jnp.float32), norm2_gain.astype(jnp.float32), w_in.astype(jnp.float32), w_ffn_out.astype(jnp.float32), w_proj.astype(jnp.float32))
    rows = tokens.astype(jnp.float32)

    def objective(row_values, param_values):
        return total_loss(row_values, param_values, seg_ids, positives)
    loss, pullback = jax.vjp(objective, rows, params)
    row_grad, param_grads = pullback(jnp.ones_like(loss))
    return (loss, row_grad.astype(jnp.bfloat16), param_grads[0], param_grads[1], param_grads[2], param_grads[3], param_grads[4], param_grads[5], param_grads[6], param_grads[7], param_grads[8], param_grads[9])
```

```python
import functools

import jax
import jax.numpy as jnp
import numpy as np
from jax import lax
from jax.experimental import pallas as pl
from jax.experimental.pallas import tpu as pltpu
from jax.sharding import PartitionSpec as P

NB = 32
MAXD = 128
QLEN = 64
PPR = 2

EPS_NORM = 1e-06
LOGIT_SCALE = 50.0
MASKED = -1e30
HIGHEST = lax.Precision.HIGHEST
F32 = jnp.float32
BF16 = jnp.bfloat16
AXES = ("wide", "narrow")
BLK = 128
VMEM_LIMIT = 60 * 1024 * 1024


def bucket_offsets(length):
    offset = np.arange(-(length - 1), length)
    half_count = NB // 2
    exact_span = half_count // 2
    distance = -offset
    bucket = (distance < 0).astype(np.int64) * half_count
    distance = np.abs(distance)
    far_bucket = exact_span + (
        np.log(np.maximum(distance, 1) / exact_span)
        / np.log(MAXD / exact_span)
        * (half_count - exact_span)
    ).astype(np.int64)
    far_bucket = np.minimum(far_bucket, half_count - 1)
    bucket = bucket + np.where(distance < exact_span, distance, far_bucket)
    return bucket.astype(np.int32)


def dot(left, right, left_dim=1, right_dim=0):
    return lax.dot_general(
        left, right, (((left_dim,), (right_dim,)), ((), ())), preferred_element_type=F32
    )


def split_two(values):
    high = values.astype(BF16)
    return high, (values - high.astype(F32)).astype(BF16)


def rms_scale(values):
    return lax.rsqrt(jnp.mean(values * values, axis=-1, keepdims=True) + EPS_NORM)


def norm_back(grad_normed, inputs, scale, gain):
    scaled = grad_normed * gain
    return scale * scaled - inputs * (
        scale * scale * scale * jnp.mean(inputs * scaled, axis=-1, keepdims=True)
    )


def slot_onehot(seg_row, slot_count):
    length = seg_row.shape[1]
    return seg_row == lax.broadcasted_iota(jnp.int32, (slot_count, length), 0)


def forward_kernel(
    seg_ref, tok_ref, g1_ref, wq_ref, wk_ref, wv_ref, wo_ref, off_ref, g2_ref, win_ref, wout_ref,
    n1_ref, q_ref, k_ref, v_ref, p_ref, o_ref, hid_ref, n2_ref, act_ref, abar_ref, m_ref,
    strip_ref, mask_ref, asum_ref, hsum_ref,
):
    step = pl.program_id(0)
    row_count = pl.num_programs(0)
    length, width = tok_ref.shape[1:]
    heads = p_ref.shape[1]
    head_size = width // heads
    blocks = length // BLK
    slots = abar_ref.shape[0] // m_ref.shape[0] * (length // QLEN)

    @pl.when(step == 0)
    def _():
        for head in range(heads):
            wide = jnp.broadcast_to(off_ref[head : head + 1, :], (BLK, 2 * length))
            rolled = pltpu.roll(wide, 2 * length - BLK + 1, 1, stride=1, stride_axis=0)
            strip_ref[head] = rolled[:, : 2 * length - BLK]

    x = tok_ref[0].astype(F32)
    n1 = (x * rms_scale(x) * g1_ref[...]).astype(BF16)
    n1_ref[0] = n1
    q_ref[0] = dot(n1, wq_ref[...]).astype(BF16)
    k_ref[0] = dot(n1, wk_ref[...]).astype(BF16)
    v_ref[0] = dot(n1, wv_ref[...]).astype(BF16)
    onehot = slot_onehot(seg_ref[0], slots)
    onehot_f = onehot.astype(F32)
    onehot_low = onehot_f.astype(BF16)
    same = dot(onehot_low, onehot_low, 0, 0)
    mask_ref[...] = jnp.where(same > 0.5, 0.0, MASKED)
    low_lane = lax.broadcasted_iota(jnp.int32, (BLK, 2 * head_size), 1) < head_size

    def pair(index, carry):
        lanes = pl.ds(pl.multiple_of(index * 2 * head_size, 2 * head_size), 2 * head_size)
        k_pair = k_ref[0, :, lanes]
        v_pair = v_ref[0, :, lanes]
        for block in range(blocks):
            rows = slice(block * BLK, (block + 1) * BLK)
            q_pair = q_ref[0, rows, lanes]
            mixed = []
            for part in range(2):
                head = index * 2 + part
                keep = low_lane if part == 0 else jnp.logical_not(low_lane)
                q_head = jnp.where(keep, q_pair, jnp.zeros_like(q_pair))
                start = (blocks - 1 - block) * BLK
                scores = dot(q_head, k_pair, 1, 1)
                scores = scores + strip_ref[head, :, start : start + length] + mask_ref[rows, :]
                top = jnp.max(scores, axis=-1, keepdims=True)
                exps = jnp.exp(scores - top)
                total = jnp.sum(exps, axis=-1, keepdims=True)
                probs = (exps * (1.0 / total)).astype(BF16)
                p_ref[0, head, rows, :] = probs
                mixed.append(dot(probs, v_pair))
            o_ref[0, rows, lanes] = jnp.where(low_lane, mixed[0], mixed[1]).astype(BF16)
        return carry

    lax.fori_loop(0, heads // 2, pair, 0)
    hidden = x + dot(o_ref[0], wo_ref[...])
    hid_ref[0] = hidden
    n2 = (hidden * rms_scale(hidden) * g2_ref[...]).astype(BF16)
    n2_ref[0] = n2
    act = jnp.maximum(dot(n2, win_ref[...]), 0.0).astype(BF16)
    act_ref[0] = act
    counts = jnp.maximum(jnp.sum(onehot_f, axis=-1, keepdims=True), 1.0)
    asum = dot(onehot_low, act) / counts
    high, low = split_two(hidden)
    hsum = (dot(onehot_low, high) + dot(onehot_low, low)) / counts
    asum_ref[pl.ds(step * slots, slots), :] = asum
    hsum_ref[pl.ds(step * slots, slots), :] = hsum

    @pl.when(step == row_count - 1)
    def _():
        high, low = split_two(asum_ref[...])
        abar_ref[...] = high
        pooled = hsum_ref[...] + dot(high, wout_ref[...]) + dot(low, wout_ref[...])
        m_ref[...] = pooled.astype(BF16)


def whole(shape):
    return pl.BlockSpec(shape, lambda r: (0,) * len(shape))


def per_row(shape):
    return pl.BlockSpec((1,) + shape, lambda r: (r,) + (0,) * len(shape))


def forward(seg3, tokens, g1, wq, wk, wv, wo, off_bias, g2, win, wout, slots):
    rows, length, width = tokens.shape
    heads = off_bias.shape[0]
    inner = win.shape[1]
    low = lambda *s: jax.ShapeDtypeStruct(s, BF16)
    rlw = (rows, length, width)
    return pl.pallas_call(
        forward_kernel,
        name="forward_rows",
        grid=(rows,),
        in_specs=[per_row((1, length)), per_row((length, width))]
        + [whole(a.shape) for a in (g1, wq, wk, wv, wo, off_bias, g2, win, wout)],
        out_specs=[per_row((length, width))] * 4
        + [per_row((heads, length, length))]
        + [per_row((length, width))] * 3
        + [per_row((length, inner)), whole((rows * slots, inner)), whole((rows * slots, width))],
        out_shape=[low(*rlw)] * 4
        + [low(rows, heads, length, length), low(*rlw), jax.ShapeDtypeStruct(rlw, F32), low(*rlw)]
        + [low(rows, length, inner), low(rows * slots, inner), low(rows * slots, width)],
        scratch_shapes=[
            pltpu.VMEM((heads, BLK, 2 * length - BLK), F32),
            pltpu.VMEM((length, length), F32),
            pltpu.VMEM((rows * slots, inner), F32),
            pltpu.VMEM((rows * slots, width), F32),
        ],
        compiler_params=pltpu.CompilerParams(vmem_limit_bytes=VMEM_LIMIT),
    )(seg3, tokens, g1, wq, wk, wv, wo, off_bias, g2, win, wout)


def contrast(pooled, target_col, w_proj, slots):
    half = pooled.shape[0] // 2
    z = dot(pooled, w_proj)
    inv = lax.rsqrt(jnp.sum(z * z, axis=-1, keepdims=True) + EPS_NORM)
    unit = z * inv
    emb = unit.astype(BF16)
    emb_q, emb_p = emb[:half], emb[half:]
    logits = LOGIT_SCALE * dot(emb_q, emb_p, 1, 1)
    column = lax.broadcasted_iota(jnp.int32, (half, half), 1)
    logits = jnp.where(column % slots < PPR, logits, MASKED)
    hits = column == target_col
    top = jnp.max(logits, axis=-1, keepdims=True)
    exps = jnp.exp(logits - top)
    total = jnp.sum(exps, axis=-1, keepdims=True)
    picked = jnp.sum(jnp.where(hits, logits, 0.0), axis=-1, keepdims=True)
    loss = jnp.sum(top + jnp.log(total) - picked, axis=0, keepdims=True)
    weights = (exps / total - hits.astype(F32)).astype(BF16)
    grad_q = LOGIT_SCALE * dot(weights, emb_p)
    grad_p = LOGIT_SCALE * dot(weights, emb_q, 0, 0)
    grad = jnp.concatenate([grad_q, grad_p], axis=0)
    dz = (inv * (grad - unit * jnp.sum(grad * unit, axis=-1, keepdims=True))).astype(BF16)
    grad_proj = dot(pooled, dz, 0, 0)
    dm = dot(dz, w_proj, 1, 1)
    return loss, grad_proj, dm


def contrast_kernel(pooled_ref, target_ref, wp_ref, loss_ref, gproj_ref, dm_ref, *, slots):
    loss, grad_proj, dm = contrast(pooled_ref[...], target_ref[...], wp_ref[...], slots)
    loss_ref[...] = loss
    gproj_ref[...] = grad_proj
    dm_ref[...] = dm


def contrast_call(pooled, target_col, w_proj, slots):
    count, width = pooled.shape
    if count > 1024:
        return contrast(pooled, target_col, w_proj, slots)
    return pl.pallas_call(
        functools.partial(contrast_kernel, slots=slots),
        name="contrast_all",
        out_shape=[
            jax.ShapeDtypeStruct((1, 1), F32),
            jax.ShapeDtypeStruct(w_proj.shape, F32),
            jax.ShapeDtypeStruct((count, width), F32),
        ],
        compiler_params=pltpu.CompilerParams(vmem_limit_bytes=VMEM_LIMIT),
    )(pooled, target_col, w_proj)


def ffn_back_kernel(
    seg_ref, dm_ref, act_ref, n2_ref, hid_ref, o_ref, g2_ref, win_ref, wout_ref, wo_ref,
    dh_ref, do_ref, big_ref, g2grad_ref,
    win_acc, wo_acc, g2_acc,
):
    step = pl.program_id(0)
    last = pl.num_programs(0) - 1
    length, width = hid_ref.shape[1:]
    slots = dm_ref.shape[1]

    onehot = slot_onehot(seg_ref[0], slots)
    onehot_f = onehot.astype(F32)
    onehot_low = onehot_f.astype(BF16)
    counts = jnp.maximum(jnp.sum(onehot_f, axis=-1, keepdims=True), 1.0)
    dy_slot = dm_ref[0] / counts
    dyb_slot = dy_slot.astype(BF16)
    dact_slot = dot(dyb_slot, wout_ref[...], 1, 1).astype(BF16)
    dact = dot(onehot_low, dact_slot, 0, 0).astype(BF16)
    act = act_ref[0]
    du = jnp.where(act > 0, dact, jnp.zeros_like(dact))
    win_part = dot(n2_ref[0], du, 0, 0)
    dn2 = dot(du, win_ref[...], 1, 1)
    hidden = hid_ref[0]
    scale = rms_scale(hidden)
    g2_part = jnp.sum(dn2 * hidden * scale, axis=0, keepdims=True)
    high, low = split_two(dy_slot)
    dy = dot(onehot_low, high, 0, 0) + dot(onehot_low, low, 0, 0)
    dh = dy + norm_back(dn2, hidden, scale, g2_ref[...])
    dh_ref[0] = dh
    dhb = dh.astype(BF16)
    do_ref[0] = dot(dhb, wo_ref[...], 1, 1).astype(BF16)
    wo_part = dot(o_ref[0], dhb, 0, 0)

    @pl.when(step == 0)
    def _():
        win_acc[...] = win_part
        wo_acc[...] = wo_part
        g2_acc[...] = g2_part

    @pl.when(step > 0)
    def _():
        win_acc[...] += win_part
        wo_acc[...] += wo_part
        g2_acc[...] += g2_part

    @pl.when(step == last)
    def _():
        parts = win_acc.shape[1] // width
        for part in range(parts):
            big_ref[part * width : (part + 1) * width, :] = win_acc[
                :, part * width : (part + 1) * width
            ].astype(BF16)
        big_ref[parts * width :, :] = wo_acc[...].astype(BF16)
        g2grad_ref[...] = g2_acc[...]


def ffn_back(seg3, dm3, act, n2, hidden, mixed, g2, win, wout, wo):
    rows, length, width = hidden.shape
    inner = win.shape[1]
    slots = dm3.shape[1]
    return pl.pallas_call(
        ffn_back_kernel,
        name="ffn_back",
        grid=(rows,),
        in_specs=[per_row((1, length)), per_row((slots, width)), per_row((length, inner))]
        + [per_row((length, width))] * 3
        + [whole(a.shape) for a in (g2, win, wout, wo)],
        out_specs=[per_row((length, width))] * 2
        + [whole((inner + width, width)), whole((1, width))],
        out_shape=[
            jax.ShapeDtypeStruct(hidden.shape, F32),
            jax.ShapeDtypeStruct(hidden.shape, BF16),
            jax.ShapeDtypeStruct((inner + width, width), BF16),
            jax.ShapeDtypeStruct((1, width), F32),
        ],
        scratch_shapes=[
            pltpu.VMEM((width, inner), F32),
            pltpu.VMEM((width, width), F32),
            pltpu.VMEM((1, width), F32),
        ],
        compiler_params=pltpu.CompilerParams(vmem_limit_bytes=VMEM_LIMIT),
    )(seg3, dm3, act, n2, hidden, mixed, g2, win, wout, wo)


def attn_back_kernel(
    tok_ref, n1_ref, q_ref, k_ref, v_ref, p_ref, o_ref, do_ref, dh_ref, g1_ref,
    wq_ref, wk_ref, wv_ref,
    tgrad_ref, qkv_ref, g1grad_ref, band_ref,
    dq_ref, dkt_ref, dvt_ref, acc_ref, wacc_ref, g1_acc,
):
    step = pl.program_id(0)
    last = pl.num_programs(0) - 1
    length, width = dh_ref.shape[1:]
    heads = p_ref.shape[1]
    head_size = width // heads
    blocks = length // BLK
    low_lane = lax.broadcasted_iota(jnp.int32, (length, 2 * head_size), 1) < head_size

    @pl.when(step == 0)
    def _():
        acc_ref[...] = jnp.zeros_like(acc_ref)

    def pair(index, carry):
        lanes = pl.ds(pl.multiple_of(index * 2 * head_size, 2 * head_size), 2 * head_size)
        q_pair = q_ref[0, :, lanes]
        k_pair = k_ref[0, :, lanes]
        v_pair = v_ref[0, :, lanes]
        do_pair = do_ref[0, :, lanes]
        q_turned = q_pair.T
        do_turned = do_pair.T
        product = do_pair.astype(F32) * o_ref[0, :, lanes].astype(F32)
        dq_parts = []
        for part in range(2):
            head = index * 2 + part
            keep = low_lane if part == 0 else jnp.logical_not(low_lane)
            do_head = jnp.where(keep, do_pair, jnp.zeros_like(do_pair))
            delta = jnp.sum(jnp.where(keep, product, 0.0), axis=-1, keepdims=True)
            probs = p_ref[0, head]
            dprobs = dot(do_head, v_pair, 1, 1)
            ds = probs.astype(F32) * (dprobs - delta)
            ds_low = ds.astype(BF16)
            sums = {}
            for i in range(blocks):
                for j in range(blocks):
                    place = max(-2, min(2, j - i)) + 2
                    tile = ds[i * BLK : (i + 1) * BLK, j * BLK : (j + 1) * BLK]
                    sums[place] = tile if place not in sums else sums[place] + tile
            for place, value in sums.items():
                acc_ref[head, :, place * BLK : (place + 1) * BLK] += value
            dq_parts.append(dot(ds_low, k_pair))
            own = slice(part * head_size, (part + 1) * head_size)
            place = pl.ds(pl.multiple_of(head * head_size, head_size), head_size)
            dkt_ref[place, :] = dot(q_turned[own], ds_low).astype(BF16)
            dvt_ref[place, :] = dot(do_turned[own], probs).astype(BF16)
        dq_ref[:, lanes] = jnp.where(low_lane, dq_parts[0], dq_parts[1]).astype(BF16)
        return carry

    lax.fori_loop(0, heads // 2, pair, 0)
    dq = dq_ref[...]
    dk = dkt_ref[...].T
    dv = dvt_ref[...].T
    n1 = n1_ref[0]
    parts = [dot(n1, d, 0, 0) for d in (dq, dk, dv)]
    dn1 = dot(dq, wq_ref[...], 1, 1) + dot(dk, wk_ref[...], 1, 1) + dot(dv, wv_ref[...], 1, 1)
    x = tok_ref[0].astype(F32)
    scale = rms_scale(x)
    g1_part = jnp.sum(dn1 * x * scale, axis=0, keepdims=True)
    tgrad_ref[0] = (dh_ref[0] + norm_back(dn1, x, scale, g1_ref[...])).astype(BF16)

    @pl.when(step == 0)
    def _():
        for index in range(3):
            wacc_ref[index] = parts[index]
        g1_acc[...] = g1_part

    @pl.when(step > 0)
    def _():
        for index in range(3):
            wacc_ref[index] += parts[index]
        g1_acc[...] += g1_part

    @pl.when(step == last)
    def _():
        for index in range(3):
            qkv_ref[index * width : (index + 1) * width, :] = wacc_ref[index].astype(BF16)
        g1grad_ref[...] = g1_acc[...]
        for head in range(heads):
            far_low = jnp.sum(acc_ref[head, :, :BLK], axis=0, keepdims=True)
            far_high = jnp.sum(acc_ref[head, :, 4 * BLK :], axis=0, keepdims=True)
            band = jnp.concatenate(
                [acc_ref[head, :, BLK : 4 * BLK], jnp.zeros((BLK, BLK), F32)], axis=1
            )
            rows = BLK // 2
            while rows >= 1:
                band = band[:rows] + pltpu.roll(band[rows:], 4 * BLK - rows, 1)
                rows //= 2
            band_ref[head : head + 1, : 4 * BLK] = band
            band_ref[head : head + 1, 4 * BLK : 5 * BLK] = far_low
            band_ref[head : head + 1, 5 * BLK :] = far_high


def attn_back(tokens, n1, q, k, v, probs, mixed, do, dh, g1, wq, wk, wv):
    rows, length, width = tokens.shape
    heads = probs.shape[1]
    return pl.pallas_call(
        attn_back_kernel,
        name="attn_back",
        grid=(rows,),
        in_specs=[per_row((length, width))] * 5
        + [per_row((heads, length, length))]
        + [per_row((length, width))] * 3
        + [whole(a.shape) for a in (g1, wq, wk, wv)],
        out_specs=[
            per_row((length, width)),
            whole((3 * width, width)),
            whole((1, width)),
            whole((heads, 6 * BLK)),
        ],
        out_shape=[
            jax.ShapeDtypeStruct(tokens.shape, BF16),
            jax.ShapeDtypeStruct((3 * width, width), BF16),
            jax.ShapeDtypeStruct((1, width), F32),
            jax.ShapeDtypeStruct((heads, 6 * BLK), F32),
        ],
        scratch_shapes=[
            pltpu.VMEM((length, width), BF16),
            pltpu.VMEM((width, length), BF16),
            pltpu.VMEM((width, length), BF16),
            pltpu.VMEM((heads, BLK, 5 * BLK), F32),
            pltpu.VMEM((3, width, width), F32),
            pltpu.VMEM((1, width), F32),
        ],
        compiler_params=pltpu.CompilerParams(vmem_limit_bytes=VMEM_LIMIT),
    )(tokens, n1, q, k, v, probs, mixed, do, dh, g1, wq, wk, wv)


def band_table(length):
    buckets = bucket_offsets(length)
    zero = length - 1
    table = np.zeros((6 * BLK, NB), np.float32)
    for column in range(4 * BLK):
        offset = column - BLK if column < 3 * BLK else column - 5 * BLK
        if -2 * BLK < offset < 2 * BLK and abs(offset) < length:
            table[column, buckets[zero + offset]] = 1.0
    far = buckets[: zero - BLK], buckets[zero + BLK + 1 :]
    assert len(set(far[0])) == 1 and len(set(far[1])) == 1
    table[4 * BLK : 5 * BLK, far[0][0]] = 1.0
    table[5 * BLK :, far[1][0]] = 1.0
    return table


def bit_order(wide, narrow):
    total = wide * narrow
    assert total & (total - 1) == 0 and narrow & (narrow - 1) == 0
    outer = [b for b in (1 << s for s in range(total.bit_length())) if narrow <= b < total]
    inner = [b for b in (1 << s for s in range(total.bit_length())) if b < narrow]
    return outer, inner


def swap(values, bit, total):
    return lax.ppermute(values, AXES, [(i, i ^ bit) for i in range(total)])


def gather_rows(values, bits, linear, total):
    for bit in bits:
        other = swap(values, bit, total)
        high = (linear & bit) != 0
        values = jnp.concatenate(
            [jnp.where(high, other, values), jnp.where(high, values, other)], axis=0
        )
    return values


def reorder(values, bits, shard):
    count = len(bits)
    taken = list(reversed(bits))
    want = sorted(bits, reverse=True)
    shape = values.shape
    split = values.reshape((2,) * count + (shard,) + shape[1:])
    perm = [taken.index(b) for b in want]
    return split.transpose(perm + list(range(count, split.ndim))).reshape(shape)


def scatter_sum(values, small, bits, linear, total):
    rows = values.shape[0]
    for bit in bits:
        rows //= 2
        high = ((linear & bit) != 0).astype(jnp.int32)
        send = lax.dynamic_slice_in_dim(values, (1 - high) * rows, rows)
        if small is not None:
            send = jnp.concatenate([send, small.astype(BF16)], axis=0)
        got = swap(send, bit, total)
        keep = lax.dynamic_slice_in_dim(values, high * rows, rows)
        values = (keep.astype(F32) + got[:rows].astype(F32)).astype(BF16)
        if small is not None:
            small = lax.reduce_precision(small, 8, 7) + got[rows:].astype(F32)
    return values, small


def local(
    tokens, seg_ids, positives, norm1_gain, w_query, w_key, w_value, w_attn_out,
    rel_bias, norm2_gain, w_in, w_ffn_out, w_proj,
):
    rows, length, width = tokens.shape
    heads = rel_bias.shape[1]
    slots = length // QLEN
    inner = w_in.shape[1]
    wide, narrow = lax.axis_size("wide"), lax.axis_size("narrow")
    total = wide * narrow
    linear = lax.axis_index("wide") * narrow + lax.axis_index("narrow")
    outer_bits, inner_bits = bit_order(wide, narrow)
    g1 = norm1_gain.astype(F32).reshape(1, width)
    g2 = norm2_gain.astype(F32).reshape(1, width)
    seg3 = seg_ids.reshape(rows, 1, length)
    buckets = bucket_offsets(length)
    offset_onehot = np.zeros((NB, 2 * length), np.float32)
    offset_onehot[buckets, np.arange(2 * length - 1)] = 1.0
    off_bias = dot(rel_bias, jnp.asarray(offset_onehot, BF16), 0, 0)

    n1, q, k, v, probs, mixed, hidden, n2, act, abar, pooled = forward(
        seg3, tokens, g1, w_query, w_key, w_value, w_attn_out, off_bias, g2, w_in, w_ffn_out, slots
    )
    shard = rows * slots
    order = inner_bits + outer_bits[1:] + outer_bits[:1]
    pooled_all = reorder(gather_rows(pooled, order, linear, total), order, shard)
    target_col = ((positives // PPR) * slots + positives % PPR).reshape(-1, 1)
    loss, grad_proj, dm = contrast_call(pooled_all, target_col, w_proj, slots)
    dm_own = lax.dynamic_slice_in_dim(dm, linear * shard, shard).reshape(rows, slots, width)
    dh, do, big, grad_g2 = ffn_back(
        seg3, dm_own, act, n2, hidden, mixed, g2, w_in, w_ffn_out, w_attn_out
    )
    tokens_grad, qkv, grad_g1, band = attn_back(
        tokens, n1, q, k, v, probs, mixed, do, dh, g1, w_query, w_key, w_value
    )
    grad_bias = jnp.dot(band, jnp.asarray(band_table(length)), precision=HIGHEST)

    abar_all = reorder(gather_rows(abar, order, linear, total), order, shard)
    grad_ffn_out = dot(abar_all, dm.astype(BF16), 0, 0)

    small = jnp.concatenate(
        [
            grad_g1,
            grad_g2,
            jnp.pad(grad_bias.reshape(1, -1), ((0, 0), (0, width - heads * NB))),
            jnp.zeros((5, width), F32),
        ],
        axis=0,
    )
    down = outer_bits + inner_bits
    packed = jnp.concatenate([big, qkv], axis=0)
    part, small = scatter_sum(packed, small, down, linear, total)
    full = gather_rows(part, list(reversed(down)), linear, total)
    grads = full.astype(F32)
    blocks = [grads[i * width : (i + 1) * width] for i in range(inner // width + 4)]
    parts = inner // width
    grad_in = jnp.concatenate(blocks[:parts], axis=1)
    return (
        loss[0, 0],
        tokens_grad,
        small[0],
        blocks[parts + 1],
        blocks[parts + 2],
        blocks[parts + 3],
        blocks[parts],
        small[2, : heads * NB].reshape(heads, NB).T,
        small[1],
        grad_in,
        grad_ffn_out,
        grad_proj,
    )


def solution(mesh):
    rows = P(AXES, None, None)
    in_specs = (rows, P(AXES, None)) + (P(),) * 11
    out_specs = (P(), rows) + (P(),) * 10
    return jax.shard_map(local, mesh=mesh, in_specs=in_specs, out_specs=out_specs, check_vma=False)
```

```python
import functools

import jax
import jax.numpy as jnp
import numpy as np
from jax import lax
from jax.experimental import pallas as pl
from jax.experimental.pallas import tpu as pltpu
from jax.sharding import PartitionSpec as P

NB = 32
MAXD = 128
QLEN = 64
PPR = 2

EPS_NORM = 1e-06
LOGIT_SCALE = 50.0
MASKED = -1e30
HIGHEST = lax.Precision.HIGHEST
F32 = jnp.float32
BF16 = jnp.bfloat16
AXES = ("wide", "narrow")
BLK = 128
VMEM_LIMIT = 60 * 1024 * 1024


def bucket_offsets(length):
    offset = np.arange(-(length - 1), length)
    half_count = NB // 2
    exact_span = half_count // 2
    distance = -offset
    bucket = (distance < 0).astype(np.int64) * half_count
    distance = np.abs(distance)
    far_bucket = exact_span + (
        np.log(np.maximum(distance, 1) / exact_span)
        / np.log(MAXD / exact_span)
        * (half_count - exact_span)
    ).astype(np.int64)
    far_bucket = np.minimum(far_bucket, half_count - 1)
    bucket = bucket + np.where(distance < exact_span, distance, far_bucket)
    return bucket.astype(np.int32)


def dot(left, right, left_dim=1, right_dim=0):
    return lax.dot_general(
        left, right, (((left_dim,), (right_dim,)), ((), ())), preferred_element_type=F32
    )


def split_two(values):
    high = values.astype(BF16)
    return high, (values - high.astype(F32)).astype(BF16)


def rms_scale(values):
    return lax.rsqrt(jnp.mean(values * values, axis=-1, keepdims=True) + EPS_NORM)


def norm_back(grad_normed, inputs, scale, gain):
    scaled = grad_normed * gain
    return scale * scaled - inputs * (
        scale * scale * scale * jnp.mean(inputs * scaled, axis=-1, keepdims=True)
    )


def slot_onehot(seg_row, slot_count):
    length = seg_row.shape[1]
    return seg_row == lax.broadcasted_iota(jnp.int32, (slot_count, length), 0)


def gain_row(ref):
    return ref[...].astype(F32).reshape(1, ref.shape[0])


def forward_kernel(
    seg_ref, tok_ref, g1_ref, wq_ref, wk_ref, wv_ref, wo_ref, rel_ref, hot_ref, g2_ref, win_ref, wout_ref,
    n1_ref, q_ref, k_ref, v_ref, p_ref, o_ref, hid_ref, n2_ref, act_ref, abar_ref, m_ref,
    strip_ref, mask_ref, asum_ref, hsum_ref,
):
    step = pl.program_id(0)
    row_count = pl.num_programs(0)
    length, width = tok_ref.shape[1:]
    heads = p_ref.shape[1]
    head_size = width // heads
    blocks = length // BLK
    slots = abar_ref.shape[0] // m_ref.shape[0] * (length // QLEN)

    @pl.when(step == 0)
    def _():
        off_bias = dot(rel_ref[...], hot_ref[...], 0, 0)
        for head in range(heads):
            wide = jnp.broadcast_to(off_bias[head : head + 1, :], (BLK, 2 * length))
            rolled = pltpu.roll(wide, 2 * length - BLK + 1, 1, stride=1, stride_axis=0)
            strip_ref[head] = rolled[:, : 2 * length - BLK]

    x = tok_ref[0].astype(F32)
    n1 = (x * rms_scale(x) * gain_row(g1_ref)).astype(BF16)
    n1_ref[0] = n1
    q_ref[0] = dot(n1, wq_ref[...]).astype(BF16)
    k_ref[0] = dot(n1, wk_ref[...]).astype(BF16)
    v_ref[0] = dot(n1, wv_ref[...]).astype(BF16)
    onehot = slot_onehot(seg_ref[pl.ds(step, 1), :], slots)
    onehot_f = onehot.astype(F32)
    onehot_low = onehot_f.astype(BF16)
    same = dot(onehot_low, onehot_low, 0, 0)
    mask_ref[...] = jnp.where(same > 0.5, 0.0, MASKED)
    low_lane = lax.broadcasted_iota(jnp.int32, (BLK, 2 * head_size), 1) < head_size

    def pair(index, carry):
        lanes = pl.ds(pl.multiple_of(index * 2 * head_size, 2 * head_size), 2 * head_size)
        k_pair = k_ref[0, :, lanes]
        v_pair = v_ref[0, :, lanes]
        for block in range(blocks):
            rows = slice(block * BLK, (block + 1) * BLK)
            q_pair = q_ref[0, rows, lanes]
            for part in range(2):
                head = index * 2 + part
                keep = low_lane if part == 0 else jnp.logical_not(low_lane)
                q_head = jnp.where(keep, q_pair, jnp.zeros_like(q_pair))
                start = (blocks - 1 - block) * BLK
                scores = dot(q_head, k_pair, 1, 1)
                scores = scores + strip_ref[head, :, start : start + length] + mask_ref[rows, :]
                top = jnp.max(scores, axis=-1, keepdims=True)
                exps = jnp.exp(scores - top)
                total = jnp.sum(exps, axis=-1, keepdims=True)
                p_ref[0, head, rows, :] = (exps * (1.0 / total)).astype(BF16)
        low_all = lax.broadcasted_iota(jnp.int32, (length, 2 * head_size), 1) < head_size
        mixed = [dot(p_ref[0, index * 2 + part], v_pair) for part in range(2)]
        o_ref[0, :, lanes] = jnp.where(low_all, mixed[0], mixed[1]).astype(BF16)
        return carry

    lax.fori_loop(0, heads // 2, pair, 0)
    hidden = x + dot(o_ref[0], wo_ref[...])
    hid_ref[0] = hidden
    n2 = (hidden * rms_scale(hidden) * gain_row(g2_ref)).astype(BF16)
    n2_ref[0] = n2
    act = jnp.maximum(dot(n2, win_ref[...]), 0.0).astype(BF16)
    act_ref[0] = act
    counts = jnp.maximum(jnp.sum(onehot_f, axis=-1, keepdims=True), 1.0)
    asum = dot(onehot_low, act) / counts
    high, low = split_two(hidden)
    hsum = (dot(onehot_low, high) + dot(onehot_low, low)) / counts
    asum_ref[pl.ds(step * slots, slots), :] = asum
    hsum_ref[pl.ds(step * slots, slots), :] = hsum

    @pl.when(step == row_count - 1)
    def _():
        high, low = split_two(asum_ref[...])
        abar_ref[...] = high
        pooled = hsum_ref[...] + dot(high, wout_ref[...]) + dot(low, wout_ref[...])
        m_ref[...] = pooled.astype(BF16)


def whole(shape):
    return pl.BlockSpec(shape, lambda r: (0,) * len(shape))


def per_row(shape):
    return pl.BlockSpec((1,) + shape, lambda r: (r,) + (0,) * len(shape))


def forward(seg, tokens, g1, wq, wk, wv, wo, rel_bias, hot, g2, win, wout, slots):
    rows, length, width = tokens.shape
    heads = rel_bias.shape[1]
    inner = win.shape[1]
    low = lambda *s: jax.ShapeDtypeStruct(s, BF16)
    rlw = (rows, length, width)
    return pl.pallas_call(
        forward_kernel,
        name="forward_rows",
        grid=(rows,),
        in_specs=[whole(seg.shape), per_row((length, width))]
        + [whole(a.shape) for a in (g1, wq, wk, wv, wo, rel_bias, hot, g2, win, wout)],
        out_specs=[per_row((length, width))] * 4
        + [per_row((heads, length, length))]
        + [per_row((length, width))] * 3
        + [per_row((length, inner)), whole((rows * slots, inner)), whole((rows * slots, width))],
        out_shape=[low(*rlw)] * 4
        + [low(rows, heads, length, length), low(*rlw), jax.ShapeDtypeStruct(rlw, F32), low(*rlw)]
        + [low(rows, length, inner), low(rows * slots, inner), low(rows * slots, width)],
        scratch_shapes=[
            pltpu.VMEM((heads, BLK, 2 * length - BLK), F32),
            pltpu.VMEM((length, length), F32),
            pltpu.VMEM((rows * slots, inner), F32),
            pltpu.VMEM((rows * slots, width), F32),
        ],
        compiler_params=pltpu.CompilerParams(vmem_limit_bytes=VMEM_LIMIT),
    )(seg, tokens, g1, wq, wk, wv, wo, rel_bias, hot, g2, win, wout)


def chunk_masks(order):
    count = len(order)
    return [
        sum(bit for place, bit in enumerate(order) if p >> (count - 1 - place) & 1)
        for p in range(1 << count)
    ]


def padded_rows(rows, total):
    return -(-rows // (16 * total)) * 16 * total


def take_chunks(source_ref, keep_ref, send_ref, where, masks):
    total = len(masks)
    chunk = 2 * keep_ref.shape[0] // total
    for p in range(total):
        first = pl.multiple_of((where ^ masks[p]) * chunk, chunk)
        values = source_ref[pl.ds(first, chunk), :].astype(BF16)
        ref, at = (keep_ref, p) if p < total // 2 else (send_ref, p - total // 2)
        ref[at * chunk : (at + 1) * chunk, :] = values


def contrast(pooled, targets, w_proj, slots):
    half = pooled.shape[0] // 2
    z = dot(pooled, w_proj)
    inv = lax.rsqrt(jnp.sum(z * z, axis=-1, keepdims=True) + EPS_NORM)
    unit = z * inv
    emb = unit.astype(BF16)
    emb_q, emb_p = emb[:half], emb[half:]
    logits = LOGIT_SCALE * dot(emb_p, emb_q, 1, 1)
    line = lax.broadcasted_iota(jnp.int32, (half, half), 0)
    logits = jnp.where(line % slots < PPR, logits, MASKED)
    hits = line == (targets // PPR) * slots + targets % PPR
    top = jnp.max(logits, axis=0, keepdims=True)
    exps = jnp.exp(logits - top)
    sums = jnp.sum(exps, axis=0, keepdims=True)
    picked = jnp.sum(jnp.where(hits, logits, 0.0), axis=0, keepdims=True)
    loss = jnp.sum(top + jnp.log(sums) - picked, axis=1, keepdims=True)
    weights = (exps / sums - hits.astype(F32)).astype(BF16)
    grad_q = LOGIT_SCALE * dot(weights, emb_p, 0, 0)
    grad_p = LOGIT_SCALE * dot(weights, emb_q)
    grad = jnp.concatenate([grad_q, grad_p], axis=0)
    dz = (inv * (grad - unit * jnp.sum(grad * unit, axis=-1, keepdims=True))).astype(BF16)
    grad_proj = dot(pooled, dz, 0, 0)
    dm = dot(dz, w_proj, 1, 1)
    return loss, grad_proj, dm


def contrast_kernel(
    where_ref, near_ref, far_ref, target_ref, wp_ref,
    loss_ref, gproj_ref, own_ref, low_ref, pooled_ref, dm_ref, *, slots, masks
):
    total = len(masks)
    chunk = own_ref.shape[0]
    firsts = [pl.multiple_of((where_ref[0] ^ mask) * chunk, chunk) for mask in masks]
    for p in range(total):
        ref, at = (near_ref, p) if p < total // 2 else (far_ref, p - total // 2)
        pooled_ref[pl.ds(firsts[p], chunk), :] = ref[at * chunk : (at + 1) * chunk, :]
    targets = target_ref[...].reshape(1, target_ref.shape[0])
    loss, grad_proj, dm = contrast(pooled_ref[...], targets, wp_ref[...], slots)
    loss_ref[...] = loss
    gproj_ref[...] = grad_proj
    dm_ref[...] = dm
    own_ref[...] = dm_ref[pl.ds(firsts[0], chunk), :]
    low_ref[...] = dm.astype(BF16)


def contrast_call(where, near, far, targets, w_proj, slots, masks):
    count, width = 2 * near.shape[0], near.shape[1]
    total = len(masks)
    chunk = count // total
    if count > 1024:
        both = jnp.concatenate([near, far], axis=0).reshape(total, chunk, width)
        places = where ^ jnp.asarray(np.asarray(masks, np.int32))
        pooled = jnp.zeros_like(both).at[places].set(both).reshape(count, width)
        loss, grad_proj, dm = contrast(pooled, targets.reshape(1, -1), w_proj, slots)
        own = dm.reshape(total, chunk, width)[where[0]]
        return loss, grad_proj, own, dm.astype(BF16)
    vmem = pl.BlockSpec(memory_space=pltpu.VMEM)
    return pl.pallas_call(
        functools.partial(contrast_kernel, slots=slots, masks=masks),
        name="contrast_all",
        in_specs=[pl.BlockSpec(memory_space=pltpu.SMEM)] + [vmem] * 4,
        out_shape=[
            jax.ShapeDtypeStruct((1, 1), F32),
            jax.ShapeDtypeStruct(w_proj.shape, F32),
            jax.ShapeDtypeStruct((chunk, width), F32),
            jax.ShapeDtypeStruct((count, width), BF16),
        ],
        scratch_shapes=[pltpu.VMEM((count, width), BF16), pltpu.VMEM((count, width), F32)],
        compiler_params=pltpu.CompilerParams(vmem_limit_bytes=VMEM_LIMIT),
    )(where, near, far, targets, w_proj)


def ffn_out_kernel(where_ref, near_ref, far_ref, dm_ref, out_ref, all_ref, *, masks):
    total = len(masks)
    chunk = all_ref.shape[0] // total
    for p in range(total):
        ref, at = (near_ref, p) if p < total // 2 else (far_ref, p - total // 2)
        first = pl.multiple_of((where_ref[0] ^ masks[p]) * chunk, chunk)
        all_ref[pl.ds(first, chunk), :] = ref[at * chunk : (at + 1) * chunk, :]
    out_ref[...] = dot(all_ref[...], dm_ref[...], 0, 0)


def ffn_out_grad(where, near, far, dm, masks):
    half, inner = near.shape
    width = dm.shape[1]
    side = pl.BlockSpec((half, width), lambda i: (0, i))
    return pl.pallas_call(
        functools.partial(ffn_out_kernel, masks=masks),
        name="ffn_out_grad",
        grid=(inner // width,),
        in_specs=[pl.BlockSpec(memory_space=pltpu.SMEM), side, side, whole(dm.shape)],
        out_specs=pl.BlockSpec((width, width), lambda i: (i, 0)),
        out_shape=jax.ShapeDtypeStruct((inner, width), F32),
        scratch_shapes=[pltpu.VMEM((2 * half, width), BF16)],
        compiler_params=pltpu.CompilerParams(vmem_limit_bytes=VMEM_LIMIT),
    )(where, near, far, dm)


def ffn_back_kernel(
    where_ref, seg_ref, dm_ref, act_ref, n2_ref, hid_ref, o_ref, g2_ref, win_ref, wout_ref, wo_ref,
    dh_ref, do_ref, keep_ref, send_ref, g2grad_ref,
    acc_ref, g2_acc, *, masks
):
    step = pl.program_id(0)
    last = pl.num_programs(0) - 1
    length, width = hid_ref.shape[1:]
    slots = length // QLEN

    onehot = slot_onehot(seg_ref[pl.ds(step, 1), :], slots)
    onehot_f = onehot.astype(F32)
    onehot_low = onehot_f.astype(BF16)
    counts = jnp.maximum(jnp.sum(onehot_f, axis=-1, keepdims=True), 1.0)
    dy_slot = dm_ref[pl.ds(pl.multiple_of(step * slots, slots), slots), :] / counts
    dyb_slot = dy_slot.astype(BF16)
    dact_slot = dot(dyb_slot, wout_ref[...], 1, 1).astype(BF16)
    dact = dot(onehot_low, dact_slot, 0, 0).astype(BF16)
    act = act_ref[0]
    du = jnp.where(act > 0, dact, jnp.zeros_like(dact))
    win_part = dot(n2_ref[0], du, 0, 0)
    dn2 = dot(du, win_ref[...], 1, 1)
    hidden = hid_ref[0]
    scale = rms_scale(hidden)
    g2_part = jnp.sum(dn2 * hidden * scale, axis=0, keepdims=True)
    high, low = split_two(dy_slot)
    dy = dot(onehot_low, high, 0, 0) + dot(onehot_low, low, 0, 0)
    dh = dy + norm_back(dn2, hidden, scale, gain_row(g2_ref))
    dh_ref[0] = dh
    dhb = dh.astype(BF16)
    do_ref[0] = dot(dhb, wo_ref[...], 1, 1).astype(BF16)
    wo_part = dot(o_ref[0], dhb, 0, 0)

    inner = win_part.shape[1]
    parts = [win_part[:, at : at + width] for at in range(0, inner, width)] + [wo_part]

    @pl.when(step == 0)
    def _():
        for index, part in enumerate(parts):
            acc_ref[index * width : (index + 1) * width, :] = part
        if acc_ref.shape[0] > len(parts) * width:
            acc_ref[len(parts) * width :, :] = jnp.zeros_like(acc_ref[len(parts) * width :, :])
        g2_acc[...] = g2_part

    @pl.when(step > 0)
    def _():
        for index, part in enumerate(parts):
            acc_ref[index * width : (index + 1) * width, :] += part
        g2_acc[...] += g2_part

    @pl.when(step == last)
    def _():
        take_chunks(acc_ref, keep_ref, send_ref, where_ref[0], masks)
        g2grad_ref[...] = g2_acc[...]


def ffn_back(where, seg, dm, act, n2, hidden, mixed, g2, win, wout, wo, masks):
    rows, length, width = hidden.shape
    inner = win.shape[1]
    lines = padded_rows(inner + width, len(masks))
    return pl.pallas_call(
        functools.partial(ffn_back_kernel, masks=masks),
        name="ffn_back",
        grid=(rows,),
        in_specs=[pl.BlockSpec(memory_space=pltpu.SMEM), whole(seg.shape), whole(dm.shape)]
        + [per_row((length, inner))]
        + [per_row((length, width))] * 3
        + [whole(a.shape) for a in (g2, win, wout, wo)],
        out_specs=[per_row((length, width))] * 2
        + [whole((lines // 2, width))] * 2
        + [whole((1, width))],
        out_shape=[
            jax.ShapeDtypeStruct(hidden.shape, F32),
            jax.ShapeDtypeStruct(hidden.shape, BF16),
            jax.ShapeDtypeStruct((lines // 2, width), BF16),
            jax.ShapeDtypeStruct((lines // 2, width), BF16),
            jax.ShapeDtypeStruct((1, width), F32),
        ],
        scratch_shapes=[
            pltpu.VMEM((lines, width), F32),
            pltpu.VMEM((1, width), F32),
        ],
        compiler_params=pltpu.CompilerParams(vmem_limit_bytes=VMEM_LIMIT),
    )(where, seg, dm, act, n2, hidden, mixed, g2, win, wout, wo)


def attn_back_kernel(*refs, group, masks):
    where_ref, n1_ref, q_ref, k_ref, v_ref, p_ref, o_ref, do_ref = refs[:8]
    before_refs = refs[8 : 8 + group]
    tail = refs[8 + group :]
    dqkv_ref, band_ref, grad_refs = tail[0], tail[1], tail[2:-4]
    dkt_ref, dvt_ref, acc_ref, wacc_ref = tail[-4:]
    step = pl.program_id(0)
    last = pl.num_programs(0) - 1
    length, width = n1_ref.shape[1:]
    heads = p_ref.shape[1]
    own_width = q_ref.shape[2]
    head_size = own_width // heads
    blocks = length // BLK
    low_lane = lax.broadcasted_iota(jnp.int32, (length, 2 * head_size), 1) < head_size

    @pl.when(step == 0)
    def _():
        acc_ref[...] = jnp.zeros_like(acc_ref)

    def pair(index, carry):
        lanes = pl.ds(pl.multiple_of(index * 2 * head_size, 2 * head_size), 2 * head_size)
        q_pair = q_ref[0, :, lanes]
        k_pair = k_ref[0, :, lanes]
        v_pair = v_ref[0, :, lanes]
        do_pair = do_ref[0, :, lanes]
        q_turned = q_pair.T
        do_turned = do_pair.T
        product = do_pair.astype(F32) * o_ref[0, :, lanes].astype(F32)
        dq_parts = []
        for part in range(2):
            head = index * 2 + part
            keep = low_lane if part == 0 else jnp.logical_not(low_lane)
            do_head = jnp.where(keep, do_pair, jnp.zeros_like(do_pair))
            delta = jnp.sum(jnp.where(keep, product, 0.0), axis=-1, keepdims=True)
            probs = p_ref[0, head]
            dprobs = dot(do_head, v_pair, 1, 1)
            ds = probs.astype(F32) * (dprobs - delta)
            ds_low = ds.astype(BF16)
            sums = {}
            for i in range(blocks):
                for j in range(blocks):
                    place = max(-2, min(2, j - i)) + 2
                    tile = ds[i * BLK : (i + 1) * BLK, j * BLK : (j + 1) * BLK]
                    sums[place] = tile if place not in sums else sums[place] + tile
            for place, value in sums.items():
                acc_ref[head, :, place * BLK : (place + 1) * BLK] += value
            dq_parts.append(dot(ds_low, k_pair))
            own = slice(part * head_size, (part + 1) * head_size)
            place = pl.ds(pl.multiple_of(head * head_size, head_size), head_size)
            dkt_ref[place, :] = dot(q_turned[own], ds_low).astype(BF16)
            dvt_ref[place, :] = dot(do_turned[own], probs).astype(BF16)
        dqkv_ref[0, 0, :, lanes] = jnp.where(low_lane, dq_parts[0], dq_parts[1]).astype(BF16)
        return carry

    lax.fori_loop(0, heads // 2, pair, 0)
    dq = dqkv_ref[0, 0]
    dk = dkt_ref[...].T
    dv = dvt_ref[...].T
    dqkv_ref[0, 1] = dk
    dqkv_ref[0, 2] = dv
    parts = [dot(n1_ref[0], d, 0, 0) for d in (dq, dk, dv)]

    here = slice(group * own_width, (group + 1) * own_width)
    if len(grad_refs) == 1:
        here = slice(0, own_width)

    @pl.when(step == 0)
    def _():
        for index in range(3):
            wacc_ref[index * width : (index + 1) * width, here] = parts[index]

    @pl.when(step > 0)
    def _():
        for index in range(3):
            wacc_ref[index * width : (index + 1) * width, here] += parts[index]

    @pl.when(step == last)
    def _():
        if len(grad_refs) == 1:
            grad_refs[0][...] = wacc_ref[...].astype(BF16)
        else:
            for index, ref in enumerate(before_refs):
                lanes = slice(index * own_width, (index + 1) * own_width)
                wacc_ref[: 3 * width, lanes] = ref[...].astype(F32)
            if wacc_ref.shape[0] > 3 * width:
                wacc_ref[3 * width :, :] = jnp.zeros_like(wacc_ref[3 * width :, :])
            take_chunks(wacc_ref, grad_refs[0], grad_refs[1], where_ref[0], masks)
        for head in range(heads):
            far_low = jnp.sum(acc_ref[head, :, :BLK], axis=0, keepdims=True)
            far_high = jnp.sum(acc_ref[head, :, 4 * BLK :], axis=0, keepdims=True)
            band = jnp.concatenate(
                [acc_ref[head, :, BLK : 4 * BLK], jnp.zeros((BLK, BLK), F32)], axis=1
            )
            rows = BLK // 2
            while rows >= 1:
                band = band[:rows] + pltpu.roll(band[rows:], 4 * BLK - rows, 1)
                rows //= 2
            band_ref[head : head + 1, : 4 * BLK] = band
            band_ref[head : head + 1, 4 * BLK : 5 * BLK] = far_low
            band_ref[head : head + 1, 5 * BLK :] = far_high


def attn_back(where, n1, q, k, v, probs, mixed, do, before, groups, masks):
    group = len(before)
    rows, length, width = n1.shape
    heads = probs.shape[1] // groups
    own_width = width // groups
    lanes = pl.BlockSpec((1, length, own_width), lambda r: (r, 0, group))
    low = lambda *s: jax.ShapeDtypeStruct(s, BF16)
    if group < groups - 1:
        grads = [low(3 * width, own_width)]
        acc = (3 * width, own_width)
    else:
        lines = padded_rows(3 * width, len(masks))
        grads = [low(lines // 2, width)] * 2
        acc = (lines, width)
    return pl.pallas_call(
        functools.partial(attn_back_kernel, group=group, masks=masks),
        name=f"attn_back_{group}",
        grid=(rows,),
        in_specs=[pl.BlockSpec(memory_space=pltpu.SMEM), per_row((length, width))]
        + [lanes] * 3
        + [pl.BlockSpec((1, heads, length, length), lambda r: (r, group, 0, 0)), lanes, lanes]
        + [whole(g.shape) for g in before],
        out_specs=[per_row((3, length, own_width)), whole((heads, 6 * BLK))]
        + [whole(g.shape) for g in grads],
        out_shape=[
            low(rows, 3, length, own_width),
            jax.ShapeDtypeStruct((heads, 6 * BLK), F32),
        ]
        + grads,
        scratch_shapes=[
            pltpu.VMEM((own_width, length), BF16),
            pltpu.VMEM((own_width, length), BF16),
            pltpu.VMEM((heads, BLK, 5 * BLK), F32),
            pltpu.VMEM(acc, F32),
        ],
        compiler_params=pltpu.CompilerParams(vmem_limit_bytes=VMEM_LIMIT),
    )(where, n1, q, k, v, probs, mixed, do, *before)


def finish_kernel(*refs, groups):
    tok_ref, dh_ref, g1_ref, g2grad_ref, table_ref, wq_ref, wk_ref, wv_ref = refs[:8]
    dqkv_refs, band_refs = refs[8 : 8 + groups], refs[8 + groups : 8 + 2 * groups]
    tgrad_ref, small_out, g1_acc, small_ref = refs[8 + 2 * groups :]
    step = pl.program_id(0)
    last = pl.num_programs(0) - 1
    own_width = dqkv_refs[0].shape[3]
    heads = band_refs[0].shape[0]
    dn1 = None
    for index, weight in enumerate((wq_ref, wk_ref, wv_ref)):
        whole_grad = jnp.concatenate([ref[0, index] for ref in dqkv_refs], axis=1)
        part = dot(whole_grad, weight[...], 1, 1)
        dn1 = part if dn1 is None else dn1 + part
    x = tok_ref[0].astype(F32)
    scale = rms_scale(x)
    g1_part = jnp.sum(dn1 * x * scale, axis=0, keepdims=True)
    tgrad_ref[0] = (dh_ref[0] + norm_back(dn1, x, scale, gain_row(g1_ref))).astype(BF16)

    @pl.when(step == 0)
    def _():
        g1_acc[...] = g1_part

    @pl.when(step > 0)
    def _():
        g1_acc[...] += g1_part

    @pl.when(step == last)
    def _():
        width = small_ref.shape[1]
        small_ref[...] = jnp.zeros_like(small_ref)
        for at in range(width // BLK):
            lanes = slice(at * BLK, (at + 1) * BLK)
            small_ref[at : at + 1, BLK : 2 * BLK] = g1_acc[:, lanes]
            small_ref[at : at + 1, 2 * BLK : 3 * BLK] = g2grad_ref[:, lanes]
        for group in range(groups):
            band = band_refs[group][...]
            high = band.astype(BF16)
            rest = band - high.astype(F32)
            low = rest.astype(BF16)
            least = (rest - low.astype(F32)).astype(BF16)
            table = table_ref[...]
            bias = dot(high, table) + dot(low, table) + dot(least, table)
            small_ref[group * heads : (group + 1) * heads, : bias.shape[1]] = bias
        small_out[...] = small_ref[...].astype(BF16)


def finish(tokens, dh, g1, g2grad, table, wq, wk, wv, dqkvs, bands):
    rows, length, width = tokens.shape
    groups = len(dqkvs)
    lead = groups * bands[0].shape[0]
    return pl.pallas_call(
        functools.partial(finish_kernel, groups=groups),
        name="finish_rows",
        grid=(rows,),
        in_specs=[per_row((length, width))] * 2
        + [whole(a.shape) for a in (g1, g2grad, table, wq, wk, wv)]
        + [per_row(d.shape[1:]) for d in dqkvs]
        + [whole(b.shape) for b in bands],
        out_specs=[per_row((length, width)), whole((lead, width))],
        out_shape=[
            jax.ShapeDtypeStruct(tokens.shape, BF16),
            jax.ShapeDtypeStruct((lead, width), BF16),
        ],
        scratch_shapes=[pltpu.VMEM((1, width), F32), pltpu.VMEM((lead, width), F32)],
        compiler_params=pltpu.CompilerParams(vmem_limit_bytes=VMEM_LIMIT),
    )(tokens, dh, g1, g2grad, table, wq, wk, wv, *dqkvs, *bands)


def band_table(length):
    buckets = bucket_offsets(length)
    zero = length - 1
    table = np.zeros((6 * BLK, NB), np.float32)
    for column in range(4 * BLK):
        offset = column - BLK if column < 3 * BLK else column - 5 * BLK
        if -2 * BLK < offset < 2 * BLK and abs(offset) < length:
            table[column, buckets[zero + offset]] = 1.0
    far = buckets[: zero - BLK], buckets[zero + BLK + 1 :]
    assert len(set(far[0])) == 1 and len(set(far[1])) == 1
    table[4 * BLK : 5 * BLK, far[0][0]] = 1.0
    table[5 * BLK :, far[1][0]] = 1.0
    return table


def unpack_kernel(where_ref, *refs, masks, weights):
    big_refs, qkv_refs = refs[0:2], refs[2:4]
    outs = refs[4:-3]
    big_all, qkv_all, small_all = refs[-3:]
    win_out, wo_out, wq_out, wk_out, wv_out, g1_out, g2_out, bias_out = outs
    total = len(masks)
    width = wo_out.shape[1]
    lead = bias_out.shape[0]
    for p in range(total):
        side, at = (0, p) if p < total // 2 else (1, p - total // 2)
        chunk = 2 * big_refs[0].shape[0] // total
        first = pl.multiple_of((where_ref[0] ^ masks[p]) * chunk, chunk)
        big_all[pl.ds(first, chunk), :] = big_refs[side][at * chunk : (at + 1) * chunk, :].astype(F32)
        rows = 2 * qkv_refs[0].shape[0] // total
        chunk = rows - lead
        first = pl.multiple_of((where_ref[0] ^ masks[p]) * chunk, chunk)
        piece = qkv_refs[side][at * rows : (at + 1) * rows, :].astype(F32)
        qkv_all[pl.ds(first, chunk), :] = piece[:chunk]
        first = pl.multiple_of((where_ref[0] ^ masks[p]) * lead, lead)
        small_all[pl.ds(first, lead), :] = piece[chunk:, : small_all.shape[1]]
    small = small_all[:lead, :]
    for p in range(1, total):
        small = small + small_all[p * lead : (p + 1) * lead, :]
    parts = win_out.shape[1] // width
    for part in range(parts):
        win_out[:, part * width : (part + 1) * width] = big_all[part * width : (part + 1) * width, :]
    wo_out[...] = big_all[parts * width : (parts + 1) * width, :]
    for index, ref in enumerate((wq_out, wk_out, wv_out)):
        ref[...] = qkv_all[index * width : (index + 1) * width, :]
    for at in range(width // BLK):
        lanes = slice(at * BLK, (at + 1) * BLK)
        g1_out[:, lanes] = small[at : at + 1, BLK : 2 * BLK]
        g2_out[:, lanes] = small[at : at + 1, 2 * BLK : 3 * BLK]
    bias_out[...] = small[:, : bias_out.shape[1]]


def unpack(where, big, qkv, inner, width, heads, masks):
    full = lambda *s: jax.ShapeDtypeStruct(s, F32)
    vmem = pl.BlockSpec(memory_space=pltpu.VMEM)
    total = len(masks)
    return pl.pallas_call(
        functools.partial(unpack_kernel, masks=masks, weights=None),
        name="unpack_grads",
        in_specs=[pl.BlockSpec(memory_space=pltpu.SMEM)] + [vmem] * 4,
        out_shape=[full(width, inner)] + [full(width, width)] * 4 + [full(1, width)] * 2 + [full(heads, NB)],
        scratch_shapes=[
            pltpu.VMEM((2 * big[0].shape[0], width), F32),
            pltpu.VMEM((2 * qkv[0].shape[0] - total * heads, width), F32),
            pltpu.VMEM((total * heads, 3 * BLK), F32),
        ],
        compiler_params=pltpu.CompilerParams(vmem_limit_bytes=VMEM_LIMIT),
    )(where, *big, *qkv)


def bit_groups(wide, narrow):
    total = wide * narrow
    assert total & (total - 1) == 0 and narrow & (narrow - 1) == 0
    bits = [1 << s for s in range(total.bit_length() - 1)]
    outer = [b for b in bits if b >= narrow]
    inner = [b for b in bits if b < narrow]
    pairs = lambda items: [items[i : i + 2] for i in range(0, len(items), 2)]
    return [outer[:1]] + pairs(outer[1:]) + pairs(inner)


def group_masks(group):
    return chunk_masks(group)[1:]


def swap(values, mask, total):
    return lax.ppermute(values, AXES, [(i, i ^ mask) for i in range(total)])


def gather_stages(values, groups, total):
    pieces = [values]
    for group in reversed(groups):
        values = pieces[0] if len(pieces) == 1 else jnp.concatenate(pieces, axis=0)
        pieces = [values] + [swap(values, mask, total) for mask in group_masks(group)]
    return pieces


def split_rows(values, count):
    rows = values.shape[0] // count
    return [values[i * rows : (i + 1) * rows] for i in range(count)]


def scatter_stages(keep, send, groups, total):
    blocks = [keep, send]
    for index, group in enumerate(groups):
        got = [swap(b, mask, total) for b, mask in zip(blocks[1:], group_masks(group))]
        count = 1 << len(groups[index + 1]) if index + 1 < len(groups) else 1
        parts = [split_rows(b, count) for b in [blocks[0]] + got]
        blocks = []
        for column in zip(*parts):
            total_part = column[0].astype(F32)
            for other in column[1:]:
                total_part = total_part + other.astype(F32)
            blocks.append(total_part.astype(BF16))
    return blocks[0]


GROUPS = 2


def local(
    tokens, seg_ids, positives, norm1_gain, w_query, w_key, w_value, w_attn_out,
    rel_bias, norm2_gain, w_in, w_ffn_out, w_proj,
):
    rows, length, width = tokens.shape
    heads = rel_bias.shape[1]
    slots = length // QLEN
    inner = w_in.shape[1]
    wide, narrow = lax.axis_size("wide"), lax.axis_size("narrow")
    total = wide * narrow
    linear = lax.axis_index("wide") * narrow + lax.axis_index("narrow")
    where = jnp.full((1,), linear, jnp.int32)
    groups = bit_groups(wide, narrow)
    masks = chunk_masks([b for g in groups for b in g])
    buckets = bucket_offsets(length)
    hot = np.zeros((NB, 2 * length), np.float32)
    hot[buckets, np.arange(2 * length - 1)] = 1.0

    n1, q, k, v, probs, mixed, hidden, n2, act, abar, pooled = forward(
        seg_ids, tokens, norm1_gain, w_query, w_key, w_value, w_attn_out, rel_bias,
        jnp.asarray(hot, BF16), norm2_gain, w_in, w_ffn_out, slots,
    )
    near, far = gather_stages(pooled, groups, total)
    loss, grad_proj, dm_own, dm_low = contrast_call(
        where, near, far, positives, w_proj, slots, masks
    )
    dh, do, big_keep, big_send, grad_g2 = ffn_back(
        where, seg_ids, dm_own, act, n2, hidden, mixed, norm2_gain, w_in, w_ffn_out, w_attn_out,
        masks,
    )
    big = scatter_stages(big_keep, big_send, groups, total)
    big = gather_stages(big, groups, total)
    dqkvs, bands, before = [], [], []
    for _ in range(GROUPS):
        dqkv, band, *grads = attn_back(
            where, n1, q, k, v, probs, mixed, do, before, GROUPS, masks
        )
        dqkvs.append(dqkv)
        bands.append(band)
        before = before + grads[:1]
    tokens_grad, small = finish(
        tokens, dh, norm1_gain, grad_g2, jnp.asarray(band_table(length), BF16),
        w_query, w_key, w_value, dqkvs, bands,
    )
    qkv = scatter_stages(grads[0], grads[1], groups, total)
    qkv = gather_stages(jnp.concatenate([qkv, small], axis=0), groups, total)

    grad_ffn_out = ffn_out_grad(where, *gather_stages(abar, groups, total), dm_low, masks)

    win, wo, wq, wk, wv, grad_g1, grad_g2, grad_bias = unpack(
        where, big, qkv, inner, width, heads, masks
    )
    return (
        loss[0, 0],
        tokens_grad,
        grad_g1[0],
        wq,
        wk,
        wv,
        wo,
        grad_bias.T,
        grad_g2[0],
        win,
        grad_ffn_out,
        grad_proj,
    )


def solution(mesh):
    rows = P(AXES, None, None)
    in_specs = (rows, P(AXES, None)) + (P(),) * 11
    out_specs = (P(), rows) + (P(),) * 10
    return jax.shard_map(local, mesh=mesh, in_specs=in_specs, out_specs=out_specs, check_vma=False)
```

```python
import functools

import jax
import jax.numpy as jnp
import numpy as np
from jax import lax
from jax.experimental import pallas as pl
from jax.experimental.pallas import tpu as pltpu
from jax.sharding import PartitionSpec as P

NB = 32
MAXD = 128
QLEN = 64
PPR = 2

EPS_NORM = 1e-06
LOGIT_SCALE = 50.0
MASKED = -1e30
HIGHEST = lax.Precision.HIGHEST
F32 = jnp.float32
BF16 = jnp.bfloat16
AXES = ("wide", "narrow")
BLK = 128
VMEM_LIMIT = 60 * 1024 * 1024
VMEM_SHARED = 44 * 1024 * 1024
VMEM_SMALL = 28 * 1024 * 1024


def bucket_offsets(length):
    offset = np.arange(-(length - 1), length)
    half_count = NB // 2
    exact_span = half_count // 2
    distance = -offset
    bucket = (distance < 0).astype(np.int64) * half_count
    distance = np.abs(distance)
    far_bucket = exact_span + (
        np.log(np.maximum(distance, 1) / exact_span)
        / np.log(MAXD / exact_span)
        * (half_count - exact_span)
    ).astype(np.int64)
    far_bucket = np.minimum(far_bucket, half_count - 1)
    bucket = bucket + np.where(distance < exact_span, distance, far_bucket)
    return bucket.astype(np.int32)


def dot(left, right, left_dim=1, right_dim=0):
    return lax.dot_general(
        left, right, (((left_dim,), (right_dim,)), ((), ())), preferred_element_type=F32
    )


def split_two(values):
    high = values.astype(BF16)
    return high, (values - high.astype(F32)).astype(BF16)


def rms_scale(values):
    return lax.rsqrt(jnp.mean(values * values, axis=-1, keepdims=True) + EPS_NORM)


def norm_back(grad_normed, inputs, scale, gain):
    scaled = grad_normed * gain
    return scale * scaled - inputs * (
        scale * scale * scale * jnp.mean(inputs * scaled, axis=-1, keepdims=True)
    )


def slot_onehot(seg_row, slot_count):
    length = seg_row.shape[1]
    return seg_row == lax.broadcasted_iota(jnp.int32, (slot_count, length), 0)


def gain_row(ref):
    return ref[...].astype(F32).reshape(1, ref.shape[0])


def forward_kernel(
    seg_ref, tok_ref, g1_ref, wq_ref, wk_ref, wv_ref, wo_ref, rel_ref, hot_ref, g2_ref, win_ref, wout_ref,
    n1_ref, q_ref, k_ref, v_ref, p_ref, o_ref, hid_ref, n2_ref, act_ref, abar_ref, m_ref,
    strip_ref, mask_ref, asum_ref, hsum_ref,
):
    step = pl.program_id(0)
    row_count = pl.num_programs(0)
    length, width = tok_ref.shape[1:]
    heads = p_ref.shape[1]
    head_size = width // heads
    blocks = length // BLK
    slots = abar_ref.shape[0] // m_ref.shape[0] * (length // QLEN)

    @pl.when(step == 0)
    def _():
        off_bias = dot(rel_ref[...], hot_ref[...])
        for head in range(heads):
            wide = jnp.broadcast_to(off_bias[head : head + 1, :], (BLK, 2 * length))
            rolled = pltpu.roll(wide, 2 * length - BLK + 1, 1, stride=1, stride_axis=0)
            strip_ref[head] = rolled[:, : 2 * length - BLK]

    x = tok_ref[0].astype(F32)
    n1 = (x * rms_scale(x) * gain_row(g1_ref)).astype(BF16)
    n1_ref[0] = n1
    q_ref[0] = dot(n1, wq_ref[...]).astype(BF16)
    k_ref[0] = dot(n1, wk_ref[...]).astype(BF16)
    v_ref[0] = dot(n1, wv_ref[...]).astype(BF16)
    onehot = slot_onehot(seg_ref[pl.ds(step, 1), :], slots)
    onehot_f = onehot.astype(F32)
    onehot_low = onehot_f.astype(BF16)
    same = dot(onehot_low, onehot_low, 0, 0)
    mask_ref[...] = jnp.where(same > 0.5, 0.0, MASKED)
    low_lane = lax.broadcasted_iota(jnp.int32, (BLK, 2 * head_size), 1) < head_size

    def pair(index, carry):
        lanes = pl.ds(pl.multiple_of(index * 2 * head_size, 2 * head_size), 2 * head_size)
        k_pair = k_ref[0, :, lanes]
        v_pair = v_ref[0, :, lanes]
        for block in range(blocks):
            rows = slice(block * BLK, (block + 1) * BLK)
            q_pair = q_ref[0, rows, lanes]
            for part in range(2):
                head = index * 2 + part
                keep = low_lane if part == 0 else jnp.logical_not(low_lane)
                q_head = jnp.where(keep, q_pair, jnp.zeros_like(q_pair))
                start = (blocks - 1 - block) * BLK
                scores = dot(q_head, k_pair, 1, 1)
                scores = scores + strip_ref[head, :, start : start + length] + mask_ref[rows, :]
                top = jnp.max(scores, axis=-1, keepdims=True)
                exps = jnp.exp(scores - top)
                total = jnp.sum(exps, axis=-1, keepdims=True)
                p_ref[0, head, rows, :] = (exps * (1.0 / total)).astype(BF16)
        low_all = lax.broadcasted_iota(jnp.int32, (length, 2 * head_size), 1) < head_size
        mixed = [dot(p_ref[0, index * 2 + part], v_pair) for part in range(2)]
        o_ref[0, :, lanes] = jnp.where(low_all, mixed[0], mixed[1]).astype(BF16)
        return carry

    lax.fori_loop(0, heads // 2, pair, 0)
    hidden = x + dot(o_ref[0], wo_ref[...])
    hid_ref[0] = hidden
    n2 = (hidden * rms_scale(hidden) * gain_row(g2_ref)).astype(BF16)
    n2_ref[0] = n2
    act = jnp.maximum(dot(n2, win_ref[...]), 0.0).astype(BF16)
    act_ref[0] = act
    counts = jnp.maximum(jnp.sum(onehot_f, axis=-1, keepdims=True), 1.0)
    asum = dot(onehot_low, act) / counts
    high, low = split_two(hidden)
    hsum = (dot(onehot_low, high) + dot(onehot_low, low)) / counts
    asum_ref[pl.ds(step * slots, slots), :] = asum
    hsum_ref[pl.ds(step * slots, slots), :] = hsum

    @pl.when(step == row_count - 1)
    def _():
        high, low = split_two(asum_ref[...])
        abar_ref[...] = high
        pooled = hsum_ref[...] + dot(high, wout_ref[...]) + dot(low, wout_ref[...])
        m_ref[...] = pooled.astype(BF16)


def whole(shape):
    return pl.BlockSpec(shape, lambda r: (0,) * len(shape))


def per_row(shape):
    return pl.BlockSpec((1,) + shape, lambda r: (r,) + (0,) * len(shape))


def forward(seg, tokens, g1, wq, wk, wv, wo, rel_bias, hot, g2, win, wout, slots):
    rows, length, width = tokens.shape
    heads = rel_bias.shape[0]
    inner = win.shape[1]
    low = lambda *s: jax.ShapeDtypeStruct(s, BF16)
    rlw = (rows, length, width)
    return pl.pallas_call(
        forward_kernel,
        name="forward_rows",
        grid=(rows,),
        in_specs=[whole(seg.shape), per_row((length, width))]
        + [whole(a.shape) for a in (g1, wq, wk, wv, wo, rel_bias, hot, g2, win, wout)],
        out_specs=[per_row((length, width))] * 4
        + [per_row((heads, length, length))]
        + [per_row((length, width))] * 3
        + [per_row((length, inner)), whole((rows * slots, inner)), whole((rows * slots, width))],
        out_shape=[low(*rlw)] * 4
        + [low(rows, heads, length, length), low(*rlw), jax.ShapeDtypeStruct(rlw, F32), low(*rlw)]
        + [low(rows, length, inner), low(rows * slots, inner), low(rows * slots, width)],
        scratch_shapes=[
            pltpu.VMEM((heads, BLK, 2 * length - BLK), F32),
            pltpu.VMEM((length, length), F32),
            pltpu.VMEM((rows * slots, inner), F32),
            pltpu.VMEM((rows * slots, width), F32),
        ],
        compiler_params=pltpu.CompilerParams(vmem_limit_bytes=VMEM_LIMIT),
    )(seg, tokens, g1, wq, wk, wv, wo, rel_bias, hot, g2, win, wout)


def chunk_masks(order):
    count = len(order)
    return [
        sum(bit for place, bit in enumerate(order) if p >> (count - 1 - place) & 1)
        for p in range(1 << count)
    ]


def padded_rows(rows, total):
    return -(-rows // (16 * total)) * 16 * total


def take_chunks(source_ref, keep_ref, send_ref, where, masks):
    total = len(masks)
    chunk = 2 * keep_ref.shape[0] // total
    for p in range(total):
        first = pl.multiple_of((where ^ masks[p]) * chunk, chunk)
        values = source_ref[pl.ds(first, chunk), :].astype(BF16)
        ref, at = (keep_ref, p) if p < total // 2 else (send_ref, p - total // 2)
        ref[at * chunk : (at + 1) * chunk, :] = values


def contrast(pooled, targets, w_proj, slots):
    half = pooled.shape[0] // 2
    z = dot(pooled, w_proj)
    inv = lax.rsqrt(jnp.sum(z * z, axis=-1, keepdims=True) + EPS_NORM)
    unit = z * inv
    emb = unit.astype(BF16)
    emb_q, emb_p = emb[:half], emb[half:]
    logits = LOGIT_SCALE * dot(emb_p, emb_q, 1, 1)
    line = lax.broadcasted_iota(jnp.int32, (half, half), 0)
    logits = jnp.where(line % slots < PPR, logits, MASKED)
    hits = line == (targets // PPR) * slots + targets % PPR
    top = jnp.max(logits, axis=0, keepdims=True)
    exps = jnp.exp(logits - top)
    sums = jnp.sum(exps, axis=0, keepdims=True)
    picked = jnp.sum(jnp.where(hits, logits, 0.0), axis=0, keepdims=True)
    loss = jnp.sum(top + jnp.log(sums) - picked, axis=1, keepdims=True)
    weights = (exps / sums - hits.astype(F32)).astype(BF16)
    grad_q = LOGIT_SCALE * dot(weights, emb_p, 0, 0)
    grad_p = LOGIT_SCALE * dot(weights, emb_q)
    grad = jnp.concatenate([grad_q, grad_p], axis=0)
    dz = (inv * (grad - unit * jnp.sum(grad * unit, axis=-1, keepdims=True))).astype(BF16)
    grad_proj = dot(pooled, dz, 0, 0)
    dm = dot(dz, w_proj, 1, 1)
    return loss, grad_proj, dm


def contrast_kernel(
    where_ref, near_ref, far_ref, target_ref, wp_ref,
    loss_ref, gproj_ref, own_ref, low_ref, pooled_ref, dm_ref, *, slots, masks
):
    total = len(masks)
    chunk = own_ref.shape[0]
    firsts = [pl.multiple_of((where_ref[0] ^ mask) * chunk, chunk) for mask in masks]
    for p in range(total):
        ref, at = (near_ref, p) if p < total // 2 else (far_ref, p - total // 2)
        pooled_ref[pl.ds(firsts[p], chunk), :] = ref[at * chunk : (at + 1) * chunk, :]
    targets = target_ref[...].reshape(1, target_ref.shape[0])
    loss, grad_proj, dm = contrast(pooled_ref[...], targets, wp_ref[...], slots)
    loss_ref[...] = loss
    gproj_ref[...] = grad_proj
    dm_ref[...] = dm
    own_ref[...] = dm_ref[pl.ds(firsts[0], chunk), :]
    low_ref[...] = dm.astype(BF16)


def contrast_call(where, near, far, targets, w_proj, slots, masks):
    count, width = 2 * near.shape[0], near.shape[1]
    total = len(masks)
    chunk = count // total
    if count > 1024:
        both = jnp.concatenate([near, far], axis=0).reshape(total, chunk, width)
        places = where ^ jnp.asarray(np.asarray(masks, np.int32))
        pooled = jnp.zeros_like(both).at[places].set(both).reshape(count, width)
        loss, grad_proj, dm = contrast(pooled, targets.reshape(1, -1), w_proj, slots)
        own = dm.reshape(total, chunk, width)[where[0]]
        return loss, grad_proj, own, dm.astype(BF16)
    vmem = pl.BlockSpec(memory_space=pltpu.VMEM)
    return pl.pallas_call(
        functools.partial(contrast_kernel, slots=slots, masks=masks),
        name="contrast_all",
        in_specs=[pl.BlockSpec(memory_space=pltpu.SMEM)] + [vmem] * 4,
        out_shape=[
            jax.ShapeDtypeStruct((1, 1), F32),
            jax.ShapeDtypeStruct(w_proj.shape, F32),
            jax.ShapeDtypeStruct((chunk, width), F32),
            jax.ShapeDtypeStruct((count, width), BF16),
        ],
        scratch_shapes=[pltpu.VMEM((count, width), BF16), pltpu.VMEM((count, width), F32)],
        compiler_params=pltpu.CompilerParams(vmem_limit_bytes=VMEM_SHARED),
    )(where, near, far, targets, w_proj)


def ffn_out_kernel(where_ref, near_ref, far_ref, dm_ref, out_ref, all_ref, *, masks):
    total = len(masks)
    chunk = all_ref.shape[0] // total
    for p in range(total):
        ref, at = (near_ref, p) if p < total // 2 else (far_ref, p - total // 2)
        first = pl.multiple_of((where_ref[0] ^ masks[p]) * chunk, chunk)
        all_ref[pl.ds(first, chunk), :] = ref[at * chunk : (at + 1) * chunk, :]
    out_ref[...] = dot(all_ref[...], dm_ref[...], 0, 0)


def ffn_out_grad(where, near, far, dm, masks):
    half, inner = near.shape
    width = dm.shape[1]
    side = pl.BlockSpec((half, width), lambda i: (0, i))
    return pl.pallas_call(
        functools.partial(ffn_out_kernel, masks=masks),
        name="ffn_out_grad",
        grid=(inner // width,),
        in_specs=[pl.BlockSpec(memory_space=pltpu.SMEM), side, side, whole(dm.shape)],
        out_specs=pl.BlockSpec((width, width), lambda i: (i, 0)),
        out_shape=jax.ShapeDtypeStruct((inner, width), F32),
        scratch_shapes=[pltpu.VMEM((2 * half, width), BF16)],
        compiler_params=pltpu.CompilerParams(vmem_limit_bytes=VMEM_SHARED),
    )(where, near, far, dm)


def ffn_back_kernel(
    where_ref, seg_ref, dm_ref, act_ref, n2_ref, hid_ref, o_ref, g2_ref, win_ref, wout_ref, wo_ref,
    dh_ref, do_ref, keep_ref, send_ref, g2grad_ref,
    acc_ref, g2_acc, *, masks
):
    step = pl.program_id(0)
    last = pl.num_programs(0) - 1
    length, width = hid_ref.shape[1:]
    slots = length // QLEN

    onehot = slot_onehot(seg_ref[pl.ds(step, 1), :], slots)
    onehot_f = onehot.astype(F32)
    onehot_low = onehot_f.astype(BF16)
    counts = jnp.maximum(jnp.sum(onehot_f, axis=-1, keepdims=True), 1.0)
    dy_slot = dm_ref[pl.ds(pl.multiple_of(step * slots, slots), slots), :] / counts
    dyb_slot = dy_slot.astype(BF16)
    dact_slot = dot(dyb_slot, wout_ref[...], 1, 1).astype(BF16)
    dact = dot(onehot_low, dact_slot, 0, 0).astype(BF16)
    act = act_ref[0]
    du = jnp.where(act > 0, dact, jnp.zeros_like(dact))
    win_part = dot(n2_ref[0], du, 0, 0)
    dn2 = dot(du, win_ref[...], 1, 1)
    hidden = hid_ref[0]
    scale = rms_scale(hidden)
    g2_part = jnp.sum(dn2 * hidden * scale, axis=0, keepdims=True)
    high, low = split_two(dy_slot)
    dy = dot(onehot_low, high, 0, 0) + dot(onehot_low, low, 0, 0)
    dh = dy + norm_back(dn2, hidden, scale, gain_row(g2_ref))
    dh_ref[0] = dh
    dhb = dh.astype(BF16)
    do_ref[0] = dot(dhb, wo_ref[...], 1, 1).astype(BF16)
    wo_part = dot(o_ref[0], dhb, 0, 0)

    inner = win_part.shape[1]
    parts = [win_part[:, at : at + width] for at in range(0, inner, width)] + [wo_part]

    @pl.when(step == 0)
    def _():
        for index, part in enumerate(parts):
            acc_ref[index * width : (index + 1) * width, :] = part
        if acc_ref.shape[0] > len(parts) * width:
            acc_ref[len(parts) * width :, :] = jnp.zeros_like(acc_ref[len(parts) * width :, :])
        g2_acc[...] = g2_part

    @pl.when(step > 0)
    def _():
        for index, part in enumerate(parts):
            acc_ref[index * width : (index + 1) * width, :] += part
        g2_acc[...] += g2_part

    @pl.when(step == last)
    def _():
        take_chunks(acc_ref, keep_ref, send_ref, where_ref[0], masks)
        g2grad_ref[...] = g2_acc[...]


def ffn_back(where, seg, dm, act, n2, hidden, mixed, g2, win, wout, wo, masks):
    rows, length, width = hidden.shape
    inner = win.shape[1]
    lines = padded_rows(inner + width, len(masks))
    return pl.pallas_call(
        functools.partial(ffn_back_kernel, masks=masks),
        name="ffn_back",
        grid=(rows,),
        in_specs=[pl.BlockSpec(memory_space=pltpu.SMEM), whole(seg.shape), whole(dm.shape)]
        + [per_row((length, inner))]
        + [per_row((length, width))] * 3
        + [whole(a.shape) for a in (g2, win, wout, wo)],
        out_specs=[per_row((length, width))] * 2
        + [whole((lines // 2, width))] * 2
        + [whole((1, width))],
        out_shape=[
            jax.ShapeDtypeStruct(hidden.shape, F32),
            jax.ShapeDtypeStruct(hidden.shape, BF16),
            jax.ShapeDtypeStruct((lines // 2, width), BF16),
            jax.ShapeDtypeStruct((lines // 2, width), BF16),
            jax.ShapeDtypeStruct((1, width), F32),
        ],
        scratch_shapes=[
            pltpu.VMEM((lines, width), F32),
            pltpu.VMEM((1, width), F32),
        ],
        compiler_params=pltpu.CompilerParams(vmem_limit_bytes=VMEM_SHARED),
    )(where, seg, dm, act, n2, hidden, mixed, g2, win, wout, wo)


def attn_back_kernel(*refs, group, masks):
    where_ref, n1_ref, q_ref, k_ref, v_ref, p_ref, o_ref, do_ref = refs[:8]
    before_refs = refs[8 : 8 + group]
    tail = refs[8 + group :]
    dqkv_ref, band_ref, grad_refs = tail[0], tail[1], tail[2:-4]
    dkt_ref, dvt_ref, acc_ref, wacc_ref = tail[-4:]
    step = pl.program_id(0)
    last = pl.num_programs(0) - 1
    length, width = n1_ref.shape[1:]
    heads = p_ref.shape[1]
    own_width = q_ref.shape[2]
    head_size = own_width // heads
    blocks = length // BLK
    low_lane = lax.broadcasted_iota(jnp.int32, (length, 2 * head_size), 1) < head_size

    @pl.when(step == 0)
    def _():
        acc_ref[...] = jnp.zeros_like(acc_ref)

    def pair(index, carry):
        lanes = pl.ds(pl.multiple_of(index * 2 * head_size, 2 * head_size), 2 * head_size)
        q_pair = q_ref[0, :, lanes]
        k_pair = k_ref[0, :, lanes]
        v_pair = v_ref[0, :, lanes]
        do_pair = do_ref[0, :, lanes]
        q_turned = q_pair.T
        do_turned = do_pair.T
        product = do_pair.astype(F32) * o_ref[0, :, lanes].astype(F32)
        dq_parts = []
        for part in range(2):
            head = index * 2 + part
            keep = low_lane if part == 0 else jnp.logical_not(low_lane)
            do_head = jnp.where(keep, do_pair, jnp.zeros_like(do_pair))
            delta = jnp.sum(jnp.where(keep, product, 0.0), axis=-1, keepdims=True)
            probs = p_ref[0, head]
            dprobs = dot(do_head, v_pair, 1, 1)
            ds = probs.astype(F32) * (dprobs - delta)
            ds_low = ds.astype(BF16)
            sums = {}
            for i in range(blocks):
                for j in range(blocks):
                    place = max(-2, min(2, j - i)) + 2
                    tile = ds[i * BLK : (i + 1) * BLK, j * BLK : (j + 1) * BLK]
                    sums[place] = tile if place not in sums else sums[place] + tile
            for place, value in sums.items():
                acc_ref[head, :, place * BLK : (place + 1) * BLK] += value
            dq_parts.append(dot(ds_low, k_pair))
            own = slice(part * head_size, (part + 1) * head_size)
            place = pl.ds(pl.multiple_of(head * head_size, head_size), head_size)
            dkt_ref[place, :] = dot(q_turned[own], ds_low).astype(BF16)
            dvt_ref[place, :] = dot(do_turned[own], probs).astype(BF16)
        dqkv_ref[0, 0, :, lanes] = jnp.where(low_lane, dq_parts[0], dq_parts[1]).astype(BF16)
        return carry

    lax.fori_loop(0, heads // 2, pair, 0)
    dq = dqkv_ref[0, 0]
    dk = dkt_ref[...].T
    dv = dvt_ref[...].T
    dqkv_ref[0, 1] = dk
    dqkv_ref[0, 2] = dv
    parts = [dot(n1_ref[0], d, 0, 0) for d in (dq, dk, dv)]

    here = slice(group * own_width, (group + 1) * own_width)
    if len(grad_refs) == 1:
        here = slice(0, own_width)

    @pl.when(step == 0)
    def _():
        for index in range(3):
            wacc_ref[index * width : (index + 1) * width, here] = parts[index]

    @pl.when(step > 0)
    def _():
        for index in range(3):
            wacc_ref[index * width : (index + 1) * width, here] += parts[index]

    @pl.when(step == last)
    def _():
        if len(grad_refs) == 1:
            grad_refs[0][...] = wacc_ref[...].astype(BF16)
        else:
            for index, ref in enumerate(before_refs):
                lanes = slice(index * own_width, (index + 1) * own_width)
                wacc_ref[: 3 * width, lanes] = ref[...].astype(F32)
            if wacc_ref.shape[0] > 3 * width:
                wacc_ref[3 * width :, :] = jnp.zeros_like(wacc_ref[3 * width :, :])
            take_chunks(wacc_ref, grad_refs[0], grad_refs[1], where_ref[0], masks)
        for head in range(heads):
            far_low = jnp.sum(acc_ref[head, :, :BLK], axis=0, keepdims=True)
            far_high = jnp.sum(acc_ref[head, :, 4 * BLK :], axis=0, keepdims=True)
            band = jnp.concatenate(
                [acc_ref[head, :, BLK : 4 * BLK], jnp.zeros((BLK, BLK), F32)], axis=1
            )
            rows = BLK // 2
            while rows >= 1:
                band = band[:rows] + pltpu.roll(band[rows:], 4 * BLK - rows, 1)
                rows //= 2
            band_ref[head : head + 1, : 4 * BLK] = band
            band_ref[head : head + 1, 4 * BLK : 5 * BLK] = far_low
            band_ref[head : head + 1, 5 * BLK :] = far_high


def attn_back(where, n1, q, k, v, probs, mixed, do, before, groups, masks):
    group = len(before)
    rows, length, width = n1.shape
    heads = probs.shape[1] // groups
    own_width = width // groups
    lanes = pl.BlockSpec((1, length, own_width), lambda r: (r, 0, group))
    low = lambda *s: jax.ShapeDtypeStruct(s, BF16)
    if group < groups - 1:
        grads = [low(3 * width, own_width)]
        acc = (3 * width, own_width)
    else:
        lines = padded_rows(3 * width, len(masks))
        grads = [low(lines // 2, width)] * 2
        acc = (lines, width)
    return pl.pallas_call(
        functools.partial(attn_back_kernel, group=group, masks=masks),
        name=f"attn_back_{group}",
        grid=(rows,),
        in_specs=[pl.BlockSpec(memory_space=pltpu.SMEM), per_row((length, width))]
        + [lanes] * 3
        + [pl.BlockSpec((1, heads, length, length), lambda r: (r, group, 0, 0)), lanes, lanes]
        + [whole(g.shape) for g in before],
        out_specs=[per_row((3, length, own_width)), whole((heads, 6 * BLK))]
        + [whole(g.shape) for g in grads],
        out_shape=[
            low(rows, 3, length, own_width),
            jax.ShapeDtypeStruct((heads, 6 * BLK), F32),
        ]
        + grads,
        scratch_shapes=[
            pltpu.VMEM((own_width, length), BF16),
            pltpu.VMEM((own_width, length), BF16),
            pltpu.VMEM((heads, BLK, 5 * BLK), F32),
            pltpu.VMEM(acc, F32),
        ],
        compiler_params=pltpu.CompilerParams(vmem_limit_bytes=VMEM_SMALL),
    )(where, n1, q, k, v, probs, mixed, do, *before)


def finish_kernel(*refs, groups):
    tok_ref, dh_ref, g1_ref, g2grad_ref, table_ref, wq_ref, wk_ref, wv_ref = refs[:8]
    dqkv_refs, band_refs = refs[8 : 8 + groups], refs[8 + groups : 8 + 2 * groups]
    tgrad_ref, small_out, g1_acc, small_ref = refs[8 + 2 * groups :]
    step = pl.program_id(0)
    last = pl.num_programs(0) - 1
    own_width = dqkv_refs[0].shape[3]
    heads = band_refs[0].shape[0]
    dn1 = None
    for index, weight in enumerate((wq_ref, wk_ref, wv_ref)):
        whole_grad = jnp.concatenate([ref[0, index] for ref in dqkv_refs], axis=1)
        part = dot(whole_grad, weight[...], 1, 1)
        dn1 = part if dn1 is None else dn1 + part
    x = tok_ref[0].astype(F32)
    scale = rms_scale(x)
    g1_part = jnp.sum(dn1 * x * scale, axis=0, keepdims=True)
    tgrad_ref[0] = (dh_ref[0] + norm_back(dn1, x, scale, gain_row(g1_ref))).astype(BF16)

    @pl.when(step == 0)
    def _():
        g1_acc[...] = g1_part

    @pl.when(step > 0)
    def _():
        g1_acc[...] += g1_part

    @pl.when(step == last)
    def _():
        width = small_ref.shape[1]
        small_ref[...] = jnp.zeros_like(small_ref)
        for at in range(width // BLK):
            lanes = slice(at * BLK, (at + 1) * BLK)
            small_ref[at : at + 1, BLK : 2 * BLK] = g1_acc[:, lanes]
            small_ref[at : at + 1, 2 * BLK : 3 * BLK] = g2grad_ref[:, lanes]
        for group in range(groups):
            band = band_refs[group][...]
            high = band.astype(BF16)
            rest = band - high.astype(F32)
            low = rest.astype(BF16)
            least = (rest - low.astype(F32)).astype(BF16)
            table = table_ref[...]
            bias = dot(high, table) + dot(low, table) + dot(least, table)
            small_ref[group * heads : (group + 1) * heads, : bias.shape[1]] = bias
        small_out[...] = small_ref[...].astype(BF16)


def finish(tokens, dh, g1, g2grad, table, wq, wk, wv, dqkvs, bands):
    rows, length, width = tokens.shape
    groups = len(dqkvs)
    lead = groups * bands[0].shape[0]
    return pl.pallas_call(
        functools.partial(finish_kernel, groups=groups),
        name="finish_rows",
        grid=(rows,),
        in_specs=[per_row((length, width))] * 2
        + [whole(a.shape) for a in (g1, g2grad, table, wq, wk, wv)]
        + [per_row(d.shape[1:]) for d in dqkvs]
        + [whole(b.shape) for b in bands],
        out_specs=[per_row((length, width)), whole((lead, width))],
        out_shape=[
            jax.ShapeDtypeStruct(tokens.shape, BF16),
            jax.ShapeDtypeStruct((lead, width), BF16),
        ],
        scratch_shapes=[pltpu.VMEM((1, width), F32), pltpu.VMEM((lead, width), F32)],
        compiler_params=pltpu.CompilerParams(vmem_limit_bytes=VMEM_SMALL),
    )(tokens, dh, g1, g2grad, table, wq, wk, wv, *dqkvs, *bands)


def band_table(length):
    buckets = bucket_offsets(length)
    zero = length - 1
    table = np.zeros((6 * BLK, NB), np.float32)
    for column in range(4 * BLK):
        offset = column - BLK if column < 3 * BLK else column - 5 * BLK
        if -2 * BLK < offset < 2 * BLK and abs(offset) < length:
            table[column, buckets[zero + offset]] = 1.0
    far = buckets[: zero - BLK], buckets[zero + BLK + 1 :]
    assert len(set(far[0])) == 1 and len(set(far[1])) == 1
    table[4 * BLK : 5 * BLK, far[0][0]] = 1.0
    table[5 * BLK :, far[1][0]] = 1.0
    return table


def unpack_big_kernel(where_ref, near_ref, far_ref, win_out, wo_out, all_ref, *, masks):
    total = len(masks)
    width = wo_out.shape[1]
    chunk = 2 * near_ref.shape[0] // total
    for p in range(total):
        ref, at = (near_ref, p) if p < total // 2 else (far_ref, p - total // 2)
        first = pl.multiple_of((where_ref[0] ^ masks[p]) * chunk, chunk)
        all_ref[pl.ds(first, chunk), :] = ref[at * chunk : (at + 1) * chunk, :].astype(F32)
    parts = win_out.shape[1] // width
    for part in range(parts):
        win_out[:, part * width : (part + 1) * width] = all_ref[part * width : (part + 1) * width, :]
    wo_out[...] = all_ref[parts * width : (parts + 1) * width, :]


def unpack_big(where, near, far, inner, width, masks):
    vmem = pl.BlockSpec(memory_space=pltpu.VMEM)
    return pl.pallas_call(
        functools.partial(unpack_big_kernel, masks=masks),
        name="unpack_ffn",
        in_specs=[pl.BlockSpec(memory_space=pltpu.SMEM), vmem, vmem],
        out_shape=[
            jax.ShapeDtypeStruct((width, inner), F32),
            jax.ShapeDtypeStruct((width, width), F32),
        ],
        scratch_shapes=[pltpu.VMEM((2 * near.shape[0], width), F32)],
        compiler_params=pltpu.CompilerParams(vmem_limit_bytes=VMEM_SMALL),
    )(where, near, far)


def unpack_qkv_kernel(
    where_ref, near_ref, far_ref, wq_out, wk_out, wv_out, g1_out, g2_out, bias_out,
    all_ref, small_all, *, masks
):
    total = len(masks)
    width = wq_out.shape[1]
    lead = bias_out.shape[0]
    rows = 2 * near_ref.shape[0] // total
    chunk = rows - lead
    for p in range(total):
        ref, at = (near_ref, p) if p < total // 2 else (far_ref, p - total // 2)
        owner = where_ref[0] ^ masks[p]
        piece = ref[at * rows : (at + 1) * rows, :].astype(F32)
        all_ref[pl.ds(pl.multiple_of(owner * chunk, chunk), chunk), :] = piece[:chunk]
        small_all[pl.ds(pl.multiple_of(owner * lead, lead), lead), :] = piece[
            chunk:, : small_all.shape[1]
        ]
    small = small_all[:lead, :]
    for p in range(1, total):
        small = small + small_all[p * lead : (p + 1) * lead, :]
    for index, ref in enumerate((wq_out, wk_out, wv_out)):
        ref[...] = all_ref[index * width : (index + 1) * width, :]
    for at in range(width // BLK):
        lanes = slice(at * BLK, (at + 1) * BLK)
        g1_out[:, lanes] = small[at : at + 1, BLK : 2 * BLK]
        g2_out[:, lanes] = small[at : at + 1, 2 * BLK : 3 * BLK]
    bias_out[...] = small[:, : bias_out.shape[1]]


def unpack_qkv(where, near, far, width, heads, masks):
    full = lambda *s: jax.ShapeDtypeStruct(s, F32)
    vmem = pl.BlockSpec(memory_space=pltpu.VMEM)
    total = len(masks)
    return pl.pallas_call(
        functools.partial(unpack_qkv_kernel, masks=masks),
        name="unpack_attn",
        in_specs=[pl.BlockSpec(memory_space=pltpu.SMEM), vmem, vmem],
        out_shape=[full(width, width)] * 3 + [full(1, width)] * 2 + [full(heads, NB)],
        scratch_shapes=[
            pltpu.VMEM((2 * near.shape[0] - total * heads, width), F32),
            pltpu.VMEM((total * heads, 3 * BLK), F32),
        ],
        compiler_params=pltpu.CompilerParams(vmem_limit_bytes=VMEM_SMALL),
    )(where, near, far)


def bit_groups(wide, narrow):
    total = wide * narrow
    assert total & (total - 1) == 0 and narrow & (narrow - 1) == 0
    bits = [1 << s for s in range(total.bit_length() - 1)]
    outer = [b for b in bits if b >= narrow]
    inner = [b for b in bits if b < narrow]
    pairs = lambda items: [items[i : i + 2] for i in range(0, len(items), 2)]
    return [outer[:1]] + pairs(outer[1:]) + pairs(inner)


def group_masks(group):
    return chunk_masks(group)[1:]


def swap(values, mask, total):
    return lax.ppermute(values, AXES, [(i, i ^ mask) for i in range(total)])


def after(values, *others):
    return lax.optimization_barrier((values,) + others)[0]


def split_rows(values, count):
    rows = values.shape[0] // count
    return [values[i * rows : (i + 1) * rows] for i in range(count)]


class Gather:
    def __init__(self, values, groups, total):
        self.pieces, self.left, self.total = [values], list(reversed(groups)), total

    def step(self, *hold):
        if self.left:
            values = self.pieces[0]
            if len(self.pieces) > 1:
                pieces = lax.optimization_barrier(tuple(self.pieces) + hold)[: len(self.pieces)]
                values = jnp.concatenate(pieces, axis=0)
            masks = group_masks(self.left.pop(0))
            self.pieces = [values] + [swap(values, mask, self.total) for mask in masks]

    def rest(self):
        while self.left:
            self.step()
        return self.pieces


class Scatter:
    def __init__(self, blocks, groups, total):
        self.blocks, self.left, self.total = list(blocks), list(groups), total

    def step(self, *hold):
        if self.left:
            masks = group_masks(self.left.pop(0))
            got = [swap(b, mask, self.total) for b, mask in zip(self.blocks[1:], masks)]
            if hold:
                got = list(lax.optimization_barrier(tuple(got) + hold)[: len(got)])
            count = 1 << len(self.left[0]) if self.left else 1
            parts = [split_rows(b, count) for b in [self.blocks[0]] + got]
            self.blocks = []
            for column in zip(*parts):
                value = column[0].astype(F32)
                for other in column[1:]:
                    value = value + other.astype(F32)
                self.blocks.append(value.astype(BF16))

    def rest(self):
        while self.left:
            self.step()
        return self.blocks[0]


GROUPS = 2


def local(
    tokens, seg_ids, positives, norm1_gain, w_query, w_key, w_value, w_attn_out,
    rel_bias, norm2_gain, w_in, w_ffn_out, w_proj,
):
    rows, length, width = tokens.shape
    heads = rel_bias.shape[1]
    slots = length // QLEN
    inner = w_in.shape[1]
    wide, narrow = lax.axis_size("wide"), lax.axis_size("narrow")
    total = wide * narrow
    linear = lax.axis_index("wide") * narrow + lax.axis_index("narrow")
    where = jnp.full((1,), linear, jnp.int32)
    groups = bit_groups(wide, narrow)
    masks = chunk_masks([b for g in groups for b in g])
    buckets = bucket_offsets(length)
    hot = np.zeros((NB, 2 * length), np.float32)
    hot[buckets, np.arange(2 * length - 1)] = 1.0

    n1, q, k, v, probs, mixed, hidden, n2, act, abar, pooled = forward(
        seg_ids, tokens, norm1_gain, w_query, w_key, w_value, w_attn_out, rel_bias.T,
        jnp.asarray(hot, BF16), norm2_gain, w_in, w_ffn_out, slots,
    )
    slot = Gather(pooled, groups, total)
    slot.step()
    slot.step()
    acts = Gather(after(abar, slot.pieces[0]), groups, total)
    acts.step()
    near, far = slot.rest()
    loss, grad_proj, dm_own, dm_low = contrast_call(
        where, near, far, positives, w_proj, slots, masks
    )
    dh, do, big_keep, big_send, grad_g2 = ffn_back(
        where, seg_ids, dm_own, act, n2, hidden, mixed, norm2_gain, w_in, w_ffn_out, w_attn_out,
        masks,
    )
    acts.step(do)
    big = Scatter([big_keep, big_send], groups, total)
    dqkvs, bands, before, tie = [], [], [], acts.pieces[:1]
    for _ in range(GROUPS):
        dqkv, band, *grads = attn_back(
            where, n1, q, k, v, probs, mixed, after(do, *tie), before, GROUPS, masks
        )
        dqkvs.append(dqkv)
        bands.append(band)
        before = before + grads[:1]
        if len(before) == 1:
            big.step(band)
            acts.step(band)
            tie = big.blocks + acts.pieces[:1]
    qkv = Scatter(grads, groups, total)
    tokens_grad, small = finish(
        tokens, dh, norm1_gain, grad_g2, jnp.asarray(band_table(length), BF16),
        w_query, w_key, w_value, dqkvs, bands,
    )
    qkv.step(small)
    big.step(*qkv.blocks)
    grad_ffn_out = ffn_out_grad(where, *acts.rest(), after(dm_low, *big.blocks), masks)
    qkv.step(grad_ffn_out)
    big.step(*qkv.blocks)
    big_all = Gather(big.rest(), groups, total)
    big_all.step()
    qkv.step(big_all.pieces[0])
    qkv_all = Gather(jnp.concatenate([qkv.rest(), small], axis=0), groups, total)
    qkv_all.step()
    big_all.step(qkv_all.pieces[0])
    qkv_all.step(big_all.pieces[0])
    big_all.step(qkv_all.pieces[0])
    win, wo = unpack_big(where, *big_all.rest(), inner, width, masks)
    qkv_all.step(wo)
    wq, wk, wv, grad_g1, grad_g2, grad_bias = unpack_qkv(
        where, *qkv_all.rest(), width, heads, masks
    )
    return (
        loss[0, 0],
        tokens_grad,
        grad_g1[0],
        wq,
        wk,
        wv,
        wo,
        grad_bias.T,
        grad_g2[0],
        win,
        grad_ffn_out,
        grad_proj,
    )


def solution(mesh):
    rows = P(AXES, None, None)
    in_specs = (rows, P(AXES, None)) + (P(),) * 11
    out_specs = (P(), rows) + (P(),) * 10
    return jax.shard_map(local, mesh=mesh, in_specs=in_specs, out_specs=out_specs, check_vma=False)
```

```python
import functools

import jax
import jax.numpy as jnp
import numpy as np
from jax import lax
from jax.experimental import pallas as pl
from jax.experimental.pallas import tpu as pltpu
from jax.sharding import PartitionSpec as P

NB = 32
MAXD = 128
QLEN = 64
PPR = 2

EPS_NORM = 1e-06
LOGIT_SCALE = 50.0
MASKED = -1e30
HIGHEST = lax.Precision.HIGHEST
F32 = jnp.float32
BF16 = jnp.bfloat16
AXES = ("wide", "narrow")
BLK = 128
VMEM_LIMIT = 60 * 1024 * 1024
VMEM_SHARED = 44 * 1024 * 1024
VMEM_SMALL = 28 * 1024 * 1024


def bucket_offsets(length):
    offset = np.arange(-(length - 1), length)
    half_count = NB // 2
    exact_span = half_count // 2
    distance = -offset
    bucket = (distance < 0).astype(np.int64) * half_count
    distance = np.abs(distance)
    far_bucket = exact_span + (
        np.log(np.maximum(distance, 1) / exact_span)
        / np.log(MAXD / exact_span)
        * (half_count - exact_span)
    ).astype(np.int64)
    far_bucket = np.minimum(far_bucket, half_count - 1)
    bucket = bucket + np.where(distance < exact_span, distance, far_bucket)
    return bucket.astype(np.int32)


def dot(left, right, left_dim=1, right_dim=0):
    return lax.dot_general(
        left, right, (((left_dim,), (right_dim,)), ((), ())), preferred_element_type=F32
    )


def split_two(values):
    high = values.astype(BF16)
    return high, (values - high.astype(F32)).astype(BF16)


def rms_scale(values):
    return lax.rsqrt(jnp.mean(values * values, axis=-1, keepdims=True) + EPS_NORM)


def norm_back(grad_normed, inputs, scale, gain):
    scaled = grad_normed * gain
    return scale * scaled - inputs * (
        scale * scale * scale * jnp.mean(inputs * scaled, axis=-1, keepdims=True)
    )


def slot_onehot(seg_row, slot_count):
    length = seg_row.shape[1]
    return seg_row == lax.broadcasted_iota(jnp.int32, (slot_count, length), 0)


def gain_row(ref):
    return ref[...].astype(F32).reshape(1, ref.shape[0])


def forward_kernel(
    seg_ref, tok_ref, g1_ref, wq_ref, wk_ref, wv_ref, rel_ref, hot_ref, g2_ref,
    wo_hbm, win_hbm, wout_hbm,
    n1_out, q_out, k_out, v_out, p_out, o_out, hid_out, n2_out, act_out, abar_ref, m_ref,
    strip_ref, mask_ref, asum_ref, hsum_ref, wo_ref, win_ref, wout_ref,
    n1_ref, q_ref, k_ref, v_ref, p_ref, o_ref, hid_ref, n2_ref, act_ref, in_sem, out_sem, p_sem,
):
    step = pl.program_id(0)
    row_count = pl.num_programs(0)
    length, width = tok_ref.shape[1:]
    heads = p_ref.shape[0]
    head_size = width // heads
    blocks = length // BLK
    slots = length // QLEN

    def fetch(index, source, target):
        return pltpu.make_async_copy(source, target, in_sem.at[index])

    fetches = [fetch(0, wo_hbm, wo_ref), fetch(1, win_hbm, win_ref), fetch(2, wout_hbm, wout_ref)]
    singles = [
        pltpu.make_async_copy(source, target.at[step], out_sem.at[index])
        for index, (source, target) in enumerate(
            [
                (n1_ref, n1_out), (q_ref, q_out), (k_ref, k_out), (v_ref, v_out),
                (o_ref, o_out), (hid_ref, hid_out), (n2_ref, n2_out), (act_ref, act_out),
            ]
        )
    ]

    def put_pair(index):
        two = pl.ds(index * 2, 2)
        return pltpu.make_async_copy(p_ref.at[two], p_out.at[step, two], p_sem.at[index])

    @pl.when(step == 0)
    def _():
        for copy in fetches:
            copy.start()
        off_bias = dot(rel_ref[...], hot_ref[...])
        for head in range(heads):
            wide = jnp.broadcast_to(off_bias[head : head + 1, :], (BLK, 2 * length))
            rolled = pltpu.roll(wide, 2 * length - BLK + 1, 1, stride=1, stride_axis=0)
            strip_ref[head] = rolled[:, : 2 * length - BLK]

    x = tok_ref[0].astype(F32)
    n1 = (x * rms_scale(x) * gain_row(g1_ref)).astype(BF16)
    n1_ref[...] = n1
    q_ref[...] = dot(n1, wq_ref[...]).astype(BF16)
    k_ref[...] = dot(n1, wk_ref[...]).astype(BF16)
    v_ref[...] = dot(n1, wv_ref[...]).astype(BF16)
    for copy in singles[:4]:
        copy.start()
    onehot = slot_onehot(seg_ref[pl.ds(step, 1), :], slots)
    onehot_f = onehot.astype(F32)
    onehot_low = onehot_f.astype(BF16)
    same = dot(onehot_low, onehot_low, 0, 0)
    mask_ref[...] = jnp.where(same > 0.5, 0.0, MASKED)
    low_lane = lax.broadcasted_iota(jnp.int32, (BLK, 2 * head_size), 1) < head_size
    low_all = lax.broadcasted_iota(jnp.int32, (length, 2 * head_size), 1) < head_size

    def pair(index, carry):
        lanes = pl.ds(pl.multiple_of(index * 2 * head_size, 2 * head_size), 2 * head_size)
        k_pair = k_ref[:, lanes]
        v_pair = v_ref[:, lanes]
        for block in range(blocks):
            rows = slice(block * BLK, (block + 1) * BLK)
            q_pair = q_ref[rows, lanes]
            for part in range(2):
                head = index * 2 + part
                keep = low_lane if part == 0 else jnp.logical_not(low_lane)
                q_head = jnp.where(keep, q_pair, jnp.zeros_like(q_pair))
                start = (blocks - 1 - block) * BLK
                scores = dot(q_head, k_pair, 1, 1)
                scores = scores + strip_ref[head, :, start : start + length] + mask_ref[rows, :]
                top = jnp.max(scores, axis=-1, keepdims=True)
                exps = jnp.exp(scores - top)
                total = jnp.sum(exps, axis=-1, keepdims=True)
                p_ref[head, rows, :] = (exps * (1.0 / total)).astype(BF16)
        put_pair(index).start()
        mixed = [dot(p_ref[index * 2 + part], v_pair) for part in range(2)]
        o_ref[:, lanes] = jnp.where(low_all, mixed[0], mixed[1]).astype(BF16)
        return carry

    lax.fori_loop(0, heads // 2, pair, 0)
    singles[4].start()

    @pl.when(step == 0)
    def _():
        for copy in fetches:
            copy.wait()

    hidden = x + dot(o_ref[...], wo_ref[...])
    hid_ref[...] = hidden
    n2 = (hidden * rms_scale(hidden) * gain_row(g2_ref)).astype(BF16)
    n2_ref[...] = n2
    singles[5].start()
    singles[6].start()
    act = jnp.maximum(dot(n2, win_ref[...]), 0.0).astype(BF16)
    act_ref[...] = act
    singles[7].start()
    counts = jnp.maximum(jnp.sum(onehot_f, axis=-1, keepdims=True), 1.0)
    asum = dot(onehot_low, act) / counts
    high, low = split_two(hidden)
    hsum = (dot(onehot_low, high) + dot(onehot_low, low)) / counts
    asum_ref[pl.ds(step * slots, slots), :] = asum
    hsum_ref[pl.ds(step * slots, slots), :] = hsum

    @pl.when(step == row_count - 1)
    def _():
        high, low = split_two(asum_ref[...])
        abar_ref[...] = high
        pooled = hsum_ref[...] + dot(high, wout_ref[...]) + dot(low, wout_ref[...])
        m_ref[...] = pooled.astype(BF16)

    for copy in singles:
        copy.wait()
    for index in range(heads // 2):
        put_pair(index).wait()


def whole(shape):
    return pl.BlockSpec(shape, lambda r: (0,) * len(shape))


def per_row(shape):
    return pl.BlockSpec((1,) + shape, lambda r: (r,) + (0,) * len(shape))


def forward(seg, tokens, g1, wq, wk, wv, wo, rel_bias, hot, g2, win, wout, slots):
    rows, length, width = tokens.shape
    heads = rel_bias.shape[0]
    inner = win.shape[1]
    low = lambda *s: jax.ShapeDtypeStruct(s, BF16)
    rlw = (rows, length, width)
    away = pl.BlockSpec(memory_space=pl.ANY)
    return pl.pallas_call(
        forward_kernel,
        name="forward_rows",
        grid=(rows,),
        in_specs=[whole(seg.shape), per_row((length, width))]
        + [whole(a.shape) for a in (g1, wq, wk, wv, rel_bias, hot, g2)]
        + [away] * 3,
        out_specs=[away] * 9 + [whole((rows * slots, inner)), whole((rows * slots, width))],
        out_shape=[low(*rlw)] * 4
        + [low(rows, heads, length, length), low(*rlw), jax.ShapeDtypeStruct(rlw, F32), low(*rlw)]
        + [low(rows, length, inner), low(rows * slots, inner), low(rows * slots, width)],
        scratch_shapes=[
            pltpu.VMEM((heads, BLK, 2 * length - BLK), F32),
            pltpu.VMEM((length, length), F32),
            pltpu.VMEM((rows * slots, inner), F32),
            pltpu.VMEM((rows * slots, width), F32),
            pltpu.VMEM(wo.shape, BF16),
            pltpu.VMEM(win.shape, BF16),
            pltpu.VMEM(wout.shape, BF16),
        ]
        + [pltpu.VMEM((length, width), BF16)] * 4
        + [
            pltpu.VMEM((heads, length, length), BF16),
            pltpu.VMEM((length, width), BF16),
            pltpu.VMEM((length, width), F32),
            pltpu.VMEM((length, width), BF16),
            pltpu.VMEM((length, inner), BF16),
            pltpu.SemaphoreType.DMA((3,)),
            pltpu.SemaphoreType.DMA((8,)),
            pltpu.SemaphoreType.DMA((heads // 2,)),
        ],
        compiler_params=pltpu.CompilerParams(vmem_limit_bytes=VMEM_LIMIT),
    )(seg, tokens, g1, wq, wk, wv, rel_bias, hot, g2, wo, win, wout)


def chunk_masks(order):
    count = len(order)
    return [
        sum(bit for place, bit in enumerate(order) if p >> (count - 1 - place) & 1)
        for p in range(1 << count)
    ]


def padded_rows(rows, total):
    return -(-rows // (16 * total)) * 16 * total


def take_chunks(source_ref, keep_ref, send_ref, where, masks):
    total = len(masks)
    chunk = 2 * keep_ref.shape[0] // total
    for p in range(total):
        first = pl.multiple_of((where ^ masks[p]) * chunk, chunk)
        values = source_ref[pl.ds(first, chunk), :].astype(BF16)
        ref, at = (keep_ref, p) if p < total // 2 else (send_ref, p - total // 2)
        ref[at * chunk : (at + 1) * chunk, :] = values


def contrast(pooled, targets, w_proj, slots):
    half = pooled.shape[0] // 2
    z = dot(pooled, w_proj)
    inv = lax.rsqrt(jnp.sum(z * z, axis=-1, keepdims=True) + EPS_NORM)
    unit = z * inv
    emb = unit.astype(BF16)
    emb_q, emb_p = emb[:half], emb[half:]
    logits = LOGIT_SCALE * dot(emb_p, emb_q, 1, 1)
    line = lax.broadcasted_iota(jnp.int32, (half, half), 0)
    logits = jnp.where(line % slots < PPR, logits, MASKED)
    hits = line == (targets // PPR) * slots + targets % PPR
    top = jnp.max(logits, axis=0, keepdims=True)
    exps = jnp.exp(logits - top)
    sums = jnp.sum(exps, axis=0, keepdims=True)
    picked = jnp.sum(jnp.where(hits, logits, 0.0), axis=0, keepdims=True)
    loss = jnp.sum(top + jnp.log(sums) - picked, axis=1, keepdims=True)
    weights = (exps / sums - hits.astype(F32)).astype(BF16)
    grad_q = LOGIT_SCALE * dot(weights, emb_p, 0, 0)
    grad_p = LOGIT_SCALE * dot(weights, emb_q)
    grad = jnp.concatenate([grad_q, grad_p], axis=0)
    dz = (inv * (grad - unit * jnp.sum(grad * unit, axis=-1, keepdims=True))).astype(BF16)
    grad_proj = dot(pooled, dz, 0, 0)
    dm = dot(dz, w_proj, 1, 1)
    return loss, grad_proj, dm


def contrast_kernel(
    where_ref, near_ref, far_ref, target_ref, wp_ref,
    loss_ref, gproj_ref, own_ref, low_ref, pooled_ref, dm_ref, *, slots, masks
):
    total = len(masks)
    chunk = own_ref.shape[0]
    firsts = [pl.multiple_of((where_ref[0] ^ mask) * chunk, chunk) for mask in masks]
    for p in range(total):
        ref, at = (near_ref, p) if p < total // 2 else (far_ref, p - total // 2)
        pooled_ref[pl.ds(firsts[p], chunk), :] = ref[at * chunk : (at + 1) * chunk, :]
    targets = target_ref[...].reshape(1, target_ref.shape[0])
    loss, grad_proj, dm = contrast(pooled_ref[...], targets, wp_ref[...], slots)
    loss_ref[...] = loss
    gproj_ref[...] = grad_proj
    dm_ref[...] = dm
    own_ref[...] = dm_ref[pl.ds(firsts[0], chunk), :]
    low_ref[...] = dm.astype(BF16)


def contrast_call(where, near, far, targets, w_proj, slots, masks):
    count, width = 2 * near.shape[0], near.shape[1]
    total = len(masks)
    chunk = count // total
    if count > 1024:
        both = jnp.concatenate([near, far], axis=0).reshape(total, chunk, width)
        places = where ^ jnp.asarray(np.asarray(masks, np.int32))
        pooled = jnp.zeros_like(both).at[places].set(both).reshape(count, width)
        loss, grad_proj, dm = contrast(pooled, targets.reshape(1, -1), w_proj, slots)
        own = dm.reshape(total, chunk, width)[where[0]]
        return loss, grad_proj, own, dm.astype(BF16)
    vmem = pl.BlockSpec(memory_space=pltpu.VMEM)
    return pl.pallas_call(
        functools.partial(contrast_kernel, slots=slots, masks=masks),
        name="contrast_all",
        in_specs=[pl.BlockSpec(memory_space=pltpu.SMEM)] + [vmem] * 4,
        out_shape=[
            jax.ShapeDtypeStruct((1, 1), F32),
            jax.ShapeDtypeStruct(w_proj.shape, F32),
            jax.ShapeDtypeStruct((chunk, width), F32),
            jax.ShapeDtypeStruct((count, width), BF16),
        ],
        scratch_shapes=[pltpu.VMEM((count, width), BF16), pltpu.VMEM((count, width), F32)],
        compiler_params=pltpu.CompilerParams(vmem_limit_bytes=VMEM_SHARED),
    )(where, near, far, targets, w_proj)


def ffn_out_kernel(where_ref, near_ref, far_ref, dm_ref, out_ref, all_ref, *, masks):
    total = len(masks)
    chunk = all_ref.shape[0] // total
    for p in range(total):
        ref, at = (near_ref, p) if p < total // 2 else (far_ref, p - total // 2)
        first = pl.multiple_of((where_ref[0] ^ masks[p]) * chunk, chunk)
        all_ref[pl.ds(first, chunk), :] = ref[at * chunk : (at + 1) * chunk, :]
    out_ref[...] = dot(all_ref[...], dm_ref[...], 0, 0)


def ffn_out_grad(where, near, far, dm, masks):
    half, inner = near.shape
    width = dm.shape[1]
    side = pl.BlockSpec((half, width), lambda i: (0, i))
    return pl.pallas_call(
        functools.partial(ffn_out_kernel, masks=masks),
        name="ffn_out_grad",
        grid=(inner // width,),
        in_specs=[pl.BlockSpec(memory_space=pltpu.SMEM), side, side, whole(dm.shape)],
        out_specs=pl.BlockSpec((width, width), lambda i: (i, 0)),
        out_shape=jax.ShapeDtypeStruct((inner, width), F32),
        scratch_shapes=[pltpu.VMEM((2 * half, width), BF16)],
        compiler_params=pltpu.CompilerParams(vmem_limit_bytes=VMEM_SHARED),
    )(where, near, far, dm)


def ffn_back_kernel(
    where_ref, seg_ref, dm_ref, act_ref, n2_ref, hid_ref, o_ref, g2_ref, win_ref, wout_ref, wo_ref,
    dh_ref, do_ref, keep_ref, send_ref, g2grad_ref,
    acc_ref, du_all, dhb_all, g2_acc, *, masks
):
    step = pl.program_id(0)
    last = pl.num_programs(0) - 1
    length, width = hid_ref.shape[1:]
    slots = length // QLEN

    onehot = slot_onehot(seg_ref[pl.ds(step, 1), :], slots)
    onehot_f = onehot.astype(F32)
    onehot_low = onehot_f.astype(BF16)
    counts = jnp.maximum(jnp.sum(onehot_f, axis=-1, keepdims=True), 1.0)
    dy_slot = dm_ref[pl.ds(pl.multiple_of(step * slots, slots), slots), :] / counts
    dyb_slot = dy_slot.astype(BF16)
    dact_slot = dot(dyb_slot, wout_ref[...], 1, 1).astype(BF16)
    dact = dot(onehot_low, dact_slot, 0, 0).astype(BF16)
    act = act_ref[0]
    du = jnp.where(act > 0, dact, jnp.zeros_like(dact))
    here = pl.ds(pl.multiple_of(step * length, length), length)
    du_all[here, :] = du
    dn2 = dot(du, win_ref[...], 1, 1)
    hidden = hid_ref[0]
    scale = rms_scale(hidden)
    g2_part = jnp.sum(dn2 * hidden * scale, axis=0, keepdims=True)
    high, low = split_two(dy_slot)
    dy = dot(onehot_low, high, 0, 0) + dot(onehot_low, low, 0, 0)
    dh = dy + norm_back(dn2, hidden, scale, gain_row(g2_ref))
    dh_ref[0] = dh
    dhb = dh.astype(BF16)
    dhb_all[here, :] = dhb
    do_ref[0] = dot(dhb, wo_ref[...], 1, 1).astype(BF16)

    @pl.when(step == 0)
    def _():
        g2_acc[...] = g2_part

    @pl.when(step > 0)
    def _():
        g2_acc[...] += g2_part

    @pl.when(step == last)
    def _():
        rows, inner = n2_ref.shape[0], du_all.shape[1]
        turned = n2_ref[...].reshape(rows * length, width).T
        for at in range(0, inner, width):
            acc_ref[at : at + width, :] = dot(turned, du_all[:, at : at + width]).astype(BF16)
        turned = o_ref[...].reshape(rows * length, width).T
        acc_ref[inner : inner + width, :] = dot(turned, dhb_all[...]).astype(BF16)
        if acc_ref.shape[0] > inner + width:
            acc_ref[inner + width :, :] = jnp.zeros_like(acc_ref[inner + width :, :])
        take_chunks(acc_ref, keep_ref, send_ref, where_ref[0], masks)
        g2grad_ref[...] = g2_acc[...]


def ffn_back(where, seg, dm, act, n2, hidden, mixed, g2, win, wout, wo, masks):
    rows, length, width = hidden.shape
    inner = win.shape[1]
    lines = padded_rows(inner + width, len(masks))
    return pl.pallas_call(
        functools.partial(ffn_back_kernel, masks=masks),
        name="ffn_back",
        grid=(rows,),
        in_specs=[pl.BlockSpec(memory_space=pltpu.SMEM), whole(seg.shape), whole(dm.shape)]
        + [per_row((length, inner)), whole(n2.shape), per_row((length, width)), whole(mixed.shape)]
        + [whole(a.shape) for a in (g2, win, wout, wo)],
        out_specs=[per_row((length, width))] * 2
        + [whole((lines // 2, width))] * 2
        + [whole((1, width))],
        out_shape=[
            jax.ShapeDtypeStruct(hidden.shape, F32),
            jax.ShapeDtypeStruct(hidden.shape, BF16),
            jax.ShapeDtypeStruct((lines // 2, width), BF16),
            jax.ShapeDtypeStruct((lines // 2, width), BF16),
            jax.ShapeDtypeStruct((1, width), F32),
        ],
        scratch_shapes=[
            pltpu.VMEM((lines, width), BF16),
            pltpu.VMEM((rows * length, inner), BF16),
            pltpu.VMEM((rows * length, width), BF16),
            pltpu.VMEM((1, width), F32),
        ],
        compiler_params=pltpu.CompilerParams(vmem_limit_bytes=VMEM_SHARED),
    )(where, seg, dm, act, n2, hidden, mixed, g2, win, wout, wo)


def attn_back_kernel(*refs, group, masks):
    where_ref, n1_ref, q_ref, k_ref, v_ref, p_ref, o_ref, do_ref = refs[:8]
    before_refs = refs[8 : 8 + group]
    tail = refs[8 + group :]
    dqkv_ref, band_ref, grad_refs = tail[0], tail[1], tail[2:-4]
    dkt_ref, dvt_ref, acc_ref, wacc_ref = tail[-4:]
    step = pl.program_id(0)
    last = pl.num_programs(0) - 1
    length, width = n1_ref.shape[1:]
    heads = p_ref.shape[1]
    own_width = q_ref.shape[2]
    head_size = own_width // heads
    blocks = length // BLK
    low_lane = lax.broadcasted_iota(jnp.int32, (length, 2 * head_size), 1) < head_size

    @pl.when(step == 0)
    def _():
        acc_ref[...] = jnp.zeros_like(acc_ref)

    def pair(index, carry):
        lanes = pl.ds(pl.multiple_of(index * 2 * head_size, 2 * head_size), 2 * head_size)
        q_pair = q_ref[0, :, lanes]
        k_pair = k_ref[0, :, lanes]
        v_pair = v_ref[0, :, lanes]
        do_pair = do_ref[0, :, lanes]
        q_turned = q_pair.T
        do_turned = do_pair.T
        product = do_pair.astype(F32) * o_ref[0, :, lanes].astype(F32)
        dq_parts = []
        for part in range(2):
            head = index * 2 + part
            keep = low_lane if part == 0 else jnp.logical_not(low_lane)
            do_head = jnp.where(keep, do_pair, jnp.zeros_like(do_pair))
            delta = jnp.sum(jnp.where(keep, product, 0.0), axis=-1, keepdims=True)
            probs = p_ref[0, head]
            dprobs = dot(do_head, v_pair, 1, 1)
            ds = probs.astype(F32) * (dprobs - delta)
            ds_low = ds.astype(BF16)
            sums = {}
            for i in range(blocks):
                for j in range(blocks):
                    place = max(-2, min(2, j - i)) + 2
                    tile = ds[i * BLK : (i + 1) * BLK, j * BLK : (j + 1) * BLK]
                    sums[place] = tile if place not in sums else sums[place] + tile
            for place, value in sums.items():
                acc_ref[head, :, place * BLK : (place + 1) * BLK] += value
            dq_parts.append(dot(ds_low, k_pair))
            own = slice(part * head_size, (part + 1) * head_size)
            place = pl.ds(pl.multiple_of(head * head_size, head_size), head_size)
            dkt_ref[place, :] = dot(q_turned[own], ds_low).astype(BF16)
            dvt_ref[place, :] = dot(do_turned[own], probs).astype(BF16)
        dqkv_ref[0, 0, :, lanes] = jnp.where(low_lane, dq_parts[0], dq_parts[1]).astype(BF16)
        return carry

    lax.fori_loop(0, heads // 2, pair, 0)
    dq = dqkv_ref[0, 0]
    dk = dkt_ref[...].T
    dv = dvt_ref[...].T
    dqkv_ref[0, 1] = dk
    dqkv_ref[0, 2] = dv
    parts = [dot(n1_ref[0], d, 0, 0) for d in (dq, dk, dv)]

    here = slice(group * own_width, (group + 1) * own_width)
    if len(grad_refs) == 1:
        here = slice(0, own_width)

    @pl.when(step == 0)
    def _():
        for index in range(3):
            wacc_ref[index * width : (index + 1) * width, here] = parts[index]

    @pl.when(step > 0)
    def _():
        for index in range(3):
            wacc_ref[index * width : (index + 1) * width, here] += parts[index]

    @pl.when(step == last)
    def _():
        if len(grad_refs) == 1:
            grad_refs[0][...] = wacc_ref[...].astype(BF16)
        else:
            for index, ref in enumerate(before_refs):
                lanes = slice(index * own_width, (index + 1) * own_width)
                wacc_ref[: 3 * width, lanes] = ref[...].astype(F32)
            if wacc_ref.shape[0] > 3 * width:
                wacc_ref[3 * width :, :] = jnp.zeros_like(wacc_ref[3 * width :, :])
            take_chunks(wacc_ref, grad_refs[0], grad_refs[1], where_ref[0], masks)
        for head in range(heads):
            far_low = jnp.sum(acc_ref[head, :, :BLK], axis=0, keepdims=True)
            far_high = jnp.sum(acc_ref[head, :, 4 * BLK :], axis=0, keepdims=True)
            band = jnp.concatenate(
                [acc_ref[head, :, BLK : 4 * BLK], jnp.zeros((BLK, BLK), F32)], axis=1
            )
            rows = BLK // 2
            while rows >= 1:
                band = band[:rows] + pltpu.roll(band[rows:], 4 * BLK - rows, 1)
                rows //= 2
            band_ref[head : head + 1, : 4 * BLK] = band
            band_ref[head : head + 1, 4 * BLK : 5 * BLK] = far_low
            band_ref[head : head + 1, 5 * BLK :] = far_high


def attn_back(where, n1, q, k, v, probs, mixed, do, before, groups, masks):
    group = len(before)
    rows, length, width = n1.shape
    heads = probs.shape[1] // groups
    own_width = width // groups
    lanes = pl.BlockSpec((1, length, own_width), lambda r: (r, 0, group))
    low = lambda *s: jax.ShapeDtypeStruct(s, BF16)
    if group < groups - 1:
        grads = [low(3 * width, own_width)]
        acc = (3 * width, own_width)
    else:
        lines = padded_rows(3 * width, len(masks))
        grads = [low(lines // 2, width)] * 2
        acc = (lines, width)
    return pl.pallas_call(
        functools.partial(attn_back_kernel, group=group, masks=masks),
        name=f"attn_back_{group}",
        grid=(rows,),
        in_specs=[pl.BlockSpec(memory_space=pltpu.SMEM), per_row((length, width))]
        + [lanes] * 3
        + [pl.BlockSpec((1, heads, length, length), lambda r: (r, group, 0, 0)), lanes, lanes]
        + [whole(g.shape) for g in before],
        out_specs=[per_row((3, length, own_width)), whole((heads, 6 * BLK))]
        + [whole(g.shape) for g in grads],
        out_shape=[
            low(rows, 3, length, own_width),
            jax.ShapeDtypeStruct((heads, 6 * BLK), F32),
        ]
        + grads,
        scratch_shapes=[
            pltpu.VMEM((own_width, length), BF16),
            pltpu.VMEM((own_width, length), BF16),
            pltpu.VMEM((heads, BLK, 5 * BLK), F32),
            pltpu.VMEM(acc, F32),
        ],
        compiler_params=pltpu.CompilerParams(vmem_limit_bytes=VMEM_SMALL),
    )(where, n1, q, k, v, probs, mixed, do, *before)


def finish_kernel(*refs, groups):
    tok_ref, dh_ref, g1_ref, g2grad_ref, table_ref, wq_ref, wk_ref, wv_ref = refs[:8]
    dqkv_refs, band_refs = refs[8 : 8 + groups], refs[8 + groups : 8 + 2 * groups]
    tgrad_ref, small_out, g1_acc, small_ref = refs[8 + 2 * groups :]
    step = pl.program_id(0)
    last = pl.num_programs(0) - 1
    own_width = dqkv_refs[0].shape[3]
    heads = band_refs[0].shape[0]
    dn1 = None
    for index, weight in enumerate((wq_ref, wk_ref, wv_ref)):
        whole_grad = jnp.concatenate([ref[0, index] for ref in dqkv_refs], axis=1)
        part = dot(whole_grad, weight[...], 1, 1)
        dn1 = part if dn1 is None else dn1 + part
    x = tok_ref[0].astype(F32)
    scale = rms_scale(x)
    g1_part = jnp.sum(dn1 * x * scale, axis=0, keepdims=True)
    tgrad_ref[0] = (dh_ref[0] + norm_back(dn1, x, scale, gain_row(g1_ref))).astype(BF16)

    @pl.when(step == 0)
    def _():
        g1_acc[...] = g1_part

    @pl.when(step > 0)
    def _():
        g1_acc[...] += g1_part

    @pl.when(step == last)
    def _():
        width = small_ref.shape[1]
        small_ref[...] = jnp.zeros_like(small_ref)
        for at in range(width // BLK):
            lanes = slice(at * BLK, (at + 1) * BLK)
            small_ref[at : at + 1, BLK : 2 * BLK] = g1_acc[:, lanes]
            small_ref[at : at + 1, 2 * BLK : 3 * BLK] = g2grad_ref[:, lanes]
        for group in range(groups):
            band = band_refs[group][...]
            high = band.astype(BF16)
            rest = band - high.astype(F32)
            low = rest.astype(BF16)
            least = (rest - low.astype(F32)).astype(BF16)
            table = table_ref[...]
            bias = dot(high, table) + dot(low, table) + dot(least, table)
            small_ref[group * heads : (group + 1) * heads, : bias.shape[1]] = bias
        small_out[...] = small_ref[...].astype(BF16)


def finish(tokens, dh, g1, g2grad, table, wq, wk, wv, dqkvs, bands):
    rows, length, width = tokens.shape
    groups = len(dqkvs)
    lead = groups * bands[0].shape[0]
    return pl.pallas_call(
        functools.partial(finish_kernel, groups=groups),
        name="finish_rows",
        grid=(rows,),
        in_specs=[per_row((length, width))] * 2
        + [whole(a.shape) for a in (g1, g2grad, table, wq, wk, wv)]
        + [per_row(d.shape[1:]) for d in dqkvs]
        + [whole(b.shape) for b in bands],
        out_specs=[per_row((length, width)), whole((lead, width))],
        out_shape=[
            jax.ShapeDtypeStruct(tokens.shape, BF16),
            jax.ShapeDtypeStruct((lead, width), BF16),
        ],
        scratch_shapes=[pltpu.VMEM((1, width), F32), pltpu.VMEM((lead, width), F32)],
        compiler_params=pltpu.CompilerParams(vmem_limit_bytes=VMEM_SMALL),
    )(tokens, dh, g1, g2grad, table, wq, wk, wv, *dqkvs, *bands)


def band_table(length):
    buckets = bucket_offsets(length)
    zero = length - 1
    table = np.zeros((6 * BLK, NB), np.float32)
    for column in range(4 * BLK):
        offset = column - BLK if column < 3 * BLK else column - 5 * BLK
        if -2 * BLK < offset < 2 * BLK and abs(offset) < length:
            table[column, buckets[zero + offset]] = 1.0
    far = buckets[: zero - BLK], buckets[zero + BLK + 1 :]
    assert len(set(far[0])) == 1 and len(set(far[1])) == 1
    table[4 * BLK : 5 * BLK, far[0][0]] = 1.0
    table[5 * BLK :, far[1][0]] = 1.0
    return table


def unpack_big_kernel(where_ref, near_ref, far_ref, win_out, wo_out, all_ref, *, masks):
    total = len(masks)
    width = wo_out.shape[1]
    chunk = 2 * near_ref.shape[0] // total
    for p in range(total):
        ref, at = (near_ref, p) if p < total // 2 else (far_ref, p - total // 2)
        first = pl.multiple_of((where_ref[0] ^ masks[p]) * chunk, chunk)
        all_ref[pl.ds(first, chunk), :] = ref[at * chunk : (at + 1) * chunk, :].astype(F32)
    parts = win_out.shape[1] // width
    for part in range(parts):
        win_out[:, part * width : (part + 1) * width] = all_ref[part * width : (part + 1) * width, :]
    wo_out[...] = all_ref[parts * width : (parts + 1) * width, :]


def unpack_big(where, near, far, inner, width, masks):
    vmem = pl.BlockSpec(memory_space=pltpu.VMEM)
    return pl.pallas_call(
        functools.partial(unpack_big_kernel, masks=masks),
        name="unpack_ffn",
        in_specs=[pl.BlockSpec(memory_space=pltpu.SMEM), vmem, vmem],
        out_shape=[
            jax.ShapeDtypeStruct((width, inner), F32),
            jax.ShapeDtypeStruct((width, width), F32),
        ],
        scratch_shapes=[pltpu.VMEM((2 * near.shape[0], width), F32)],
        compiler_params=pltpu.CompilerParams(vmem_limit_bytes=VMEM_SMALL),
    )(where, near, far)


def unpack_qkv_kernel(
    where_ref, near_ref, far_ref, wq_out, wk_out, wv_out, g1_out, g2_out, bias_out,
    all_ref, small_all, *, masks
):
    total = len(masks)
    width = wq_out.shape[1]
    lead = bias_out.shape[0]
    rows = 2 * near_ref.shape[0] // total
    chunk = rows - lead
    for p in range(total):
        ref, at = (near_ref, p) if p < total // 2 else (far_ref, p - total // 2)
        owner = where_ref[0] ^ masks[p]
        piece = ref[at * rows : (at + 1) * rows, :].astype(F32)
        all_ref[pl.ds(pl.multiple_of(owner * chunk, chunk), chunk), :] = piece[:chunk]
        small_all[pl.ds(pl.multiple_of(owner * lead, lead), lead), :] = piece[
            chunk:, : small_all.shape[1]
        ]
    small = small_all[:lead, :]
    for p in range(1, total):
        small = small + small_all[p * lead : (p + 1) * lead, :]
    for index, ref in enumerate((wq_out, wk_out, wv_out)):
        ref[...] = all_ref[index * width : (index + 1) * width, :]
    for at in range(width // BLK):
        lanes = slice(at * BLK, (at + 1) * BLK)
        g1_out[:, lanes] = small[at : at + 1, BLK : 2 * BLK]
        g2_out[:, lanes] = small[at : at + 1, 2 * BLK : 3 * BLK]
    bias_out[...] = small[:, : bias_out.shape[1]]


def unpack_qkv(where, near, far, width, heads, masks):
    full = lambda *s: jax.ShapeDtypeStruct(s, F32)
    vmem = pl.BlockSpec(memory_space=pltpu.VMEM)
    total = len(masks)
    return pl.pallas_call(
        functools.partial(unpack_qkv_kernel, masks=masks),
        name="unpack_attn",
        in_specs=[pl.BlockSpec(memory_space=pltpu.SMEM), vmem, vmem],
        out_shape=[full(width, width)] * 3 + [full(1, width)] * 2 + [full(heads, NB)],
        scratch_shapes=[
            pltpu.VMEM((2 * near.shape[0] - total * heads, width), F32),
            pltpu.VMEM((total * heads, 3 * BLK), F32),
        ],
        compiler_params=pltpu.CompilerParams(vmem_limit_bytes=VMEM_SMALL),
    )(where, near, far)


def bit_groups(wide, narrow):
    total = wide * narrow
    assert total & (total - 1) == 0 and narrow & (narrow - 1) == 0
    bits = [1 << s for s in range(total.bit_length() - 1)]
    outer = [b for b in bits if b >= narrow]
    inner = [b for b in bits if b < narrow]
    pairs = lambda items: [items[i : i + 2] for i in range(0, len(items), 2)]
    return [outer[:1]] + pairs(outer[1:]) + pairs(inner)


def group_masks(group):
    return chunk_masks(group)[1:]


def swap(values, mask, total):
    return lax.ppermute(values, AXES, [(i, i ^ mask) for i in range(total)])


def after(values, *others):
    return lax.optimization_barrier((values,) + others)[0]


def split_rows(values, count):
    rows = values.shape[0] // count
    return [values[i * rows : (i + 1) * rows] for i in range(count)]


class Gather:
    def __init__(self, values, groups, total):
        self.pieces, self.left, self.total = [values], list(reversed(groups)), total

    def step(self, *hold):
        if self.left:
            values = self.pieces[0]
            if len(self.pieces) > 1:
                pieces = lax.optimization_barrier(tuple(self.pieces) + hold)[: len(self.pieces)]
                values = jnp.concatenate(pieces, axis=0)
            masks = group_masks(self.left.pop(0))
            self.pieces = [values] + [swap(values, mask, self.total) for mask in masks]

    def rest(self):
        while self.left:
            self.step()
        return self.pieces


class Scatter:
    def __init__(self, blocks, groups, total):
        self.blocks, self.left, self.total = list(blocks), list(groups), total

    def step(self, *hold):
        if self.left:
            masks = group_masks(self.left.pop(0))
            got = [swap(b, mask, self.total) for b, mask in zip(self.blocks[1:], masks)]
            if hold:
                got = list(lax.optimization_barrier(tuple(got) + hold)[: len(got)])
            count = 1 << len(self.left[0]) if self.left else 1
            parts = [split_rows(b, count) for b in [self.blocks[0]] + got]
            self.blocks = []
            for column in zip(*parts):
                value = column[0].astype(F32)
                for other in column[1:]:
                    value = value + other.astype(F32)
                self.blocks.append(value.astype(BF16))

    def rest(self):
        while self.left:
            self.step()
        return self.blocks[0]


GROUPS = 2


def local(
    tokens, seg_ids, positives, norm1_gain, w_query, w_key, w_value, w_attn_out,
    rel_bias, norm2_gain, w_in, w_ffn_out, w_proj,
):
    rows, length, width = tokens.shape
    heads = rel_bias.shape[1]
    slots = length // QLEN
    inner = w_in.shape[1]
    wide, narrow = lax.axis_size("wide"), lax.axis_size("narrow")
    total = wide * narrow
    linear = lax.axis_index("wide") * narrow + lax.axis_index("narrow")
    where = jnp.full((1,), linear, jnp.int32)
    groups = bit_groups(wide, narrow)
    masks = chunk_masks([b for g in groups for b in g])
    buckets = bucket_offsets(length)
    hot = np.zeros((NB, 2 * length), np.float32)
    hot[buckets, np.arange(2 * length - 1)] = 1.0

    n1, q, k, v, probs, mixed, hidden, n2, act, abar, pooled = forward(
        seg_ids, tokens, norm1_gain, w_query, w_key, w_value, w_attn_out, rel_bias.T,
        jnp.asarray(hot, BF16), norm2_gain, w_in, w_ffn_out, slots,
    )
    slot = Gather(pooled, groups, total)
    slot.step()
    slot.step()
    acts = Gather(abar, groups, total)
    acts.step()
    slot.step(*acts.pieces)
    near, far = slot.rest()
    loss, grad_proj, dm_own, dm_low = contrast_call(
        where, near, far, positives, w_proj, slots, masks
    )
    dh, do, big_keep, big_send, grad_g2 = ffn_back(
        where, seg_ids, dm_own, act, n2, hidden, mixed, norm2_gain, w_in, w_ffn_out, w_attn_out,
        masks,
    )
    acts.step(do)
    big = Scatter([big_keep, big_send], groups, total)
    dqkvs, bands, before, tie = [], [], [], acts.pieces[:1]
    for _ in range(GROUPS):
        dqkv, band, *grads = attn_back(
            where, n1, q, k, v, probs, mixed, after(do, *tie), before, GROUPS, masks
        )
        dqkvs.append(dqkv)
        bands.append(band)
        before = before + grads[:1]
        if len(before) == 1:
            big.step(band)
            acts.step(band)
            tie = big.blocks + acts.pieces[:1]
    tokens_grad, small = finish(
        tokens, dh, norm1_gain, grad_g2, jnp.asarray(band_table(length), BF16),
        w_query, w_key, w_value, dqkvs, bands,
    )
    big.step(small)
    qkv = Scatter([grads[0], after(grads[1], *big.blocks)], groups, total)
    qkv.step()
    grad_ffn_out = ffn_out_grad(where, *acts.rest(), after(dm_low, *qkv.blocks), masks)
    qkv.step(grad_ffn_out)
    big.step(*qkv.blocks)
    big_all = Gather(big.rest(), groups, total)
    big_all.step()
    qkv.step(big_all.pieces[0])
    qkv_all = Gather(jnp.concatenate([qkv.rest(), small], axis=0), groups, total)
    qkv_all.step()
    big_all.step(qkv_all.pieces[0])
    qkv_all.step(big_all.pieces[0])
    big_all.step(qkv_all.pieces[0])
    win, wo = unpack_big(where, *big_all.rest(), inner, width, masks)
    qkv_all.step(wo)
    wq, wk, wv, grad_g1, grad_g2, grad_bias = unpack_qkv(
        where, *qkv_all.rest(), width, heads, masks
    )
    return (
        loss[0, 0],
        tokens_grad,
        grad_g1[0],
        wq,
        wk,
        wv,
        wo,
        grad_bias.T,
        grad_g2[0],
        win,
        grad_ffn_out,
        grad_proj,
    )


def solution(mesh):
    rows = P(AXES, None, None)
    in_specs = (rows, P(AXES, None)) + (P(),) * 11
    out_specs = (P(), rows) + (P(),) * 10
    return jax.shard_map(local, mesh=mesh, in_specs=in_specs, out_specs=out_specs, check_vma=False)
```

```python
import functools

import jax
import jax.numpy as jnp
import numpy as np
from jax import lax
from jax.experimental import pallas as pl
from jax.experimental.pallas import tpu as pltpu
from jax.sharding import PartitionSpec as P

NB = 32
MAXD = 128
QLEN = 64
PPR = 2

EPS_NORM = 1e-06
LOGIT_SCALE = 50.0
MASKED = -1e30
HIGHEST = lax.Precision.HIGHEST
F32 = jnp.float32
BF16 = jnp.bfloat16
AXES = ("wide", "narrow")
BLK = 128
VMEM_LIMIT = 60 * 1024 * 1024
VMEM_SHARED = 44 * 1024 * 1024
VMEM_SMALL = 28 * 1024 * 1024


def bucket_offsets(length):
    offset = np.arange(-(length - 1), length)
    half_count = NB // 2
    exact_span = half_count // 2
    distance = -offset
    bucket = (distance < 0).astype(np.int64) * half_count
    distance = np.abs(distance)
    far_bucket = exact_span + (
        np.log(np.maximum(distance, 1) / exact_span)
        / np.log(MAXD / exact_span)
        * (half_count - exact_span)
    ).astype(np.int64)
    far_bucket = np.minimum(far_bucket, half_count - 1)
    bucket = bucket + np.where(distance < exact_span, distance, far_bucket)
    return bucket.astype(np.int32)


def dot(left, right, left_dim=1, right_dim=0):
    return lax.dot_general(
        left, right, (((left_dim,), (right_dim,)), ((), ())), preferred_element_type=F32
    )


def split_two(values):
    high = values.astype(BF16)
    return high, (values - high.astype(F32)).astype(BF16)


def rms_scale(values):
    return lax.rsqrt(jnp.mean(values * values, axis=-1, keepdims=True) + EPS_NORM)


def norm_back(grad_normed, inputs, scale, gain):
    scaled = grad_normed * gain
    return scale * scaled - inputs * (
        scale * scale * scale * jnp.mean(inputs * scaled, axis=-1, keepdims=True)
    )


def slot_onehot(seg_row, slot_count):
    length = seg_row.shape[1]
    return seg_row == lax.broadcasted_iota(jnp.int32, (slot_count, length), 0)


def gain_row(ref):
    return ref[...].astype(F32).reshape(1, ref.shape[0])


def forward_kernel(
    seg_ref, tok_ref, g1_ref, wq_ref, wk_ref, wv_ref, rel_ref, hot_ref, g2_ref,
    wo_hbm, win_hbm, wout_hbm,
    n1_out, q_out, k_out, v_out, p_out, o_out, hid_out, n2_out, act_out, abar_ref, m_ref,
    strip_ref, mask_ref, asum_ref, hsum_ref, wo_ref, win_ref, wout_ref,
    n1_ref, q_ref, k_ref, v_ref, p_ref, o_ref, hid_ref, n2_ref, act_ref, in_sem, out_sem, late_sem, p_sem,
):
    step = pl.program_id(0)
    row_count = pl.num_programs(0)
    length, width = tok_ref.shape[1:]
    heads = p_ref.shape[0]
    head_size = width // heads
    blocks = length // BLK
    slots = length // QLEN

    def fetch(index, source, target):
        return pltpu.make_async_copy(source, target, in_sem.at[index])

    fetches = [fetch(0, wo_hbm, wo_ref), fetch(1, win_hbm, win_ref), fetch(2, wout_hbm, wout_ref)]
    singles = [
        pltpu.make_async_copy(source, target.at[step], out_sem.at[index])
        for index, (source, target) in enumerate(
            [
                (n1_ref, n1_out), (q_ref, q_out), (k_ref, k_out), (v_ref, v_out),
            ]
        )
    ]

    def put_late(index, row):
        source, target = (
            (o_ref, o_out), (hid_ref, hid_out), (n2_ref, n2_out), (act_ref, act_out)
        )[index]
        return pltpu.make_async_copy(source.at[row], target.at[row], late_sem.at[index, row])

    def put_pair(index):
        two = pl.ds(index * 2, 2)
        return pltpu.make_async_copy(p_ref.at[two], p_out.at[step, two], p_sem.at[index])

    @pl.when(step == 0)
    def _():
        for copy in fetches:
            copy.start()
        off_bias = dot(rel_ref[...], hot_ref[...])
        for head in range(heads):
            wide = jnp.broadcast_to(off_bias[head : head + 1, :], (BLK, 2 * length))
            rolled = pltpu.roll(wide, 2 * length - BLK + 1, 1, stride=1, stride_axis=0)
            strip_ref[head] = rolled[:, : 2 * length - BLK]

    x = tok_ref[0].astype(F32)
    n1 = (x * rms_scale(x) * gain_row(g1_ref)).astype(BF16)
    n1_ref[...] = n1
    q_ref[...] = dot(n1, wq_ref[...]).astype(BF16)
    k_ref[...] = dot(n1, wk_ref[...]).astype(BF16)
    v_ref[...] = dot(n1, wv_ref[...]).astype(BF16)
    for copy in singles:
        copy.start()
    onehot = slot_onehot(seg_ref[pl.ds(step, 1), :], slots)
    onehot_f = onehot.astype(F32)
    onehot_low = onehot_f.astype(BF16)
    same = dot(onehot_low, onehot_low, 0, 0)
    mask_ref[...] = jnp.where(same > 0.5, 0.0, MASKED)
    low_lane = lax.broadcasted_iota(jnp.int32, (BLK, 2 * head_size), 1) < head_size
    low_all = lax.broadcasted_iota(jnp.int32, (length, 2 * head_size), 1) < head_size

    def pair(index, carry):
        lanes = pl.ds(pl.multiple_of(index * 2 * head_size, 2 * head_size), 2 * head_size)
        k_pair = k_ref[:, lanes]
        v_pair = v_ref[:, lanes]
        for block in range(blocks):
            rows = slice(block * BLK, (block + 1) * BLK)
            q_pair = q_ref[rows, lanes]
            for part in range(2):
                head = index * 2 + part
                keep = low_lane if part == 0 else jnp.logical_not(low_lane)
                q_head = jnp.where(keep, q_pair, jnp.zeros_like(q_pair))
                start = (blocks - 1 - block) * BLK
                scores = dot(q_head, k_pair, 1, 1)
                scores = scores + strip_ref[head, :, start : start + length] + mask_ref[rows, :]
                top = jnp.max(scores, axis=-1, keepdims=True)
                exps = jnp.exp(scores - top)
                total = jnp.sum(exps, axis=-1, keepdims=True)
                p_ref[head, rows, :] = (exps * (1.0 / total)).astype(BF16)
        put_pair(index).start()
        mixed = [dot(p_ref[index * 2 + part], v_pair) for part in range(2)]
        o_ref[step, :, lanes] = jnp.where(low_all, mixed[0], mixed[1]).astype(BF16)
        return carry

    lax.fori_loop(0, heads // 2, pair, 0)
    put_late(0, step).start()

    @pl.when(step == 0)
    def _():
        for copy in fetches:
            copy.wait()

    hidden = x + dot(o_ref[step], wo_ref[...])
    hid_ref[step] = hidden
    n2 = (hidden * rms_scale(hidden) * gain_row(g2_ref)).astype(BF16)
    n2_ref[step] = n2
    put_late(1, step).start()
    put_late(2, step).start()
    act = jnp.maximum(dot(n2, win_ref[...]), 0.0).astype(BF16)
    act_ref[step] = act
    put_late(3, step).start()
    counts = jnp.maximum(jnp.sum(onehot_f, axis=-1, keepdims=True), 1.0)
    asum = dot(onehot_low, act) / counts
    high, low = split_two(hidden)
    hsum = (dot(onehot_low, high) + dot(onehot_low, low)) / counts
    asum_ref[pl.ds(step * slots, slots), :] = asum
    hsum_ref[pl.ds(step * slots, slots), :] = hsum

    @pl.when(step == row_count - 1)
    def _():
        high, low = split_two(asum_ref[...])
        abar_ref[...] = high
        pooled = hsum_ref[...] + dot(high, wout_ref[...]) + dot(low, wout_ref[...])
        m_ref[...] = pooled.astype(BF16)
        for row in range(act_ref.shape[0]):
            for index in range(4):
                put_late(index, row).wait()

    for copy in singles:
        copy.wait()
    for index in range(heads // 2):
        put_pair(index).wait()


def whole(shape):
    return pl.BlockSpec(shape, lambda r: (0,) * len(shape))


def per_row(shape):
    return pl.BlockSpec((1,) + shape, lambda r: (r,) + (0,) * len(shape))


def forward(seg, tokens, g1, wq, wk, wv, wo, rel_bias, hot, g2, win, wout, slots):
    rows, length, width = tokens.shape
    heads = rel_bias.shape[0]
    inner = win.shape[1]
    low = lambda *s: jax.ShapeDtypeStruct(s, BF16)
    rlw = (rows, length, width)
    away = pl.BlockSpec(memory_space=pl.ANY)
    return pl.pallas_call(
        forward_kernel,
        name="forward_rows",
        grid=(rows,),
        in_specs=[whole(seg.shape), per_row((length, width))]
        + [whole(a.shape) for a in (g1, wq, wk, wv, rel_bias, hot, g2)]
        + [away] * 3,
        out_specs=[away] * 9 + [whole((rows * slots, inner)), whole((rows * slots, width))],
        out_shape=[low(*rlw)] * 4
        + [low(rows, heads, length, length), low(*rlw), jax.ShapeDtypeStruct(rlw, F32), low(*rlw)]
        + [low(rows, length, inner), low(rows * slots, inner), low(rows * slots, width)],
        scratch_shapes=[
            pltpu.VMEM((heads, BLK, 2 * length - BLK), F32),
            pltpu.VMEM((length, length), F32),
            pltpu.VMEM((rows * slots, inner), F32),
            pltpu.VMEM((rows * slots, width), F32),
            pltpu.VMEM(wo.shape, BF16),
            pltpu.VMEM(win.shape, BF16),
            pltpu.VMEM(wout.shape, BF16),
        ]
        + [pltpu.VMEM((length, width), BF16)] * 4
        + [
            pltpu.VMEM((heads, length, length), BF16),
            pltpu.VMEM(rlw, BF16),
            pltpu.VMEM(rlw, F32),
            pltpu.VMEM(rlw, BF16),
            pltpu.VMEM((rows, length, inner), BF16),
            pltpu.SemaphoreType.DMA((3,)),
            pltpu.SemaphoreType.DMA((4,)),
            pltpu.SemaphoreType.DMA((4, rows)),
            pltpu.SemaphoreType.DMA((heads // 2,)),
        ],
        compiler_params=pltpu.CompilerParams(vmem_limit_bytes=VMEM_LIMIT),
    )(seg, tokens, g1, wq, wk, wv, rel_bias, hot, g2, wo, win, wout)


def chunk_masks(order):
    count = len(order)
    return [
        sum(bit for place, bit in enumerate(order) if p >> (count - 1 - place) & 1)
        for p in range(1 << count)
    ]


def padded_rows(rows, total):
    return -(-rows // (16 * total)) * 16 * total


def take_chunks(source_ref, keep_ref, send_ref, where, masks):
    total = len(masks)
    chunk = 2 * keep_ref.shape[0] // total
    for p in range(total):
        first = pl.multiple_of((where ^ masks[p]) * chunk, chunk)
        values = source_ref[pl.ds(first, chunk), :].astype(BF16)
        ref, at = (keep_ref, p) if p < total // 2 else (send_ref, p - total // 2)
        ref[at * chunk : (at + 1) * chunk, :] = values


def contrast(pooled, targets, w_proj, slots):
    half = pooled.shape[0] // 2
    z = dot(pooled, w_proj)
    inv = lax.rsqrt(jnp.sum(z * z, axis=-1, keepdims=True) + EPS_NORM)
    unit = z * inv
    emb = unit.astype(BF16)
    emb_q, emb_p = emb[:half], emb[half:]
    logits = LOGIT_SCALE * dot(emb_p, emb_q, 1, 1)
    line = lax.broadcasted_iota(jnp.int32, (half, half), 0)
    logits = jnp.where(line % slots < PPR, logits, MASKED)
    hits = line == (targets // PPR) * slots + targets % PPR
    top = jnp.max(logits, axis=0, keepdims=True)
    exps = jnp.exp(logits - top)
    sums = jnp.sum(exps, axis=0, keepdims=True)
    picked = jnp.sum(jnp.where(hits, logits, 0.0), axis=0, keepdims=True)
    loss = jnp.sum(top + jnp.log(sums) - picked, axis=1, keepdims=True)
    weights = (exps / sums - hits.astype(F32)).astype(BF16)
    grad_q = LOGIT_SCALE * dot(weights, emb_p, 0, 0)
    grad_p = LOGIT_SCALE * dot(weights, emb_q)
    grad = jnp.concatenate([grad_q, grad_p], axis=0)
    dz = (inv * (grad - unit * jnp.sum(grad * unit, axis=-1, keepdims=True))).astype(BF16)
    grad_proj = dot(pooled, dz, 0, 0)
    dm = dot(dz, w_proj, 1, 1)
    return loss, grad_proj, dm


def contrast_kernel(
    where_ref, near_ref, far_ref, target_ref, wp_ref,
    loss_ref, gproj_ref, own_ref, low_ref, pooled_ref, dm_ref, *, slots, masks
):
    total = len(masks)
    chunk = own_ref.shape[0]
    firsts = [pl.multiple_of((where_ref[0] ^ mask) * chunk, chunk) for mask in masks]
    for p in range(total):
        ref, at = (near_ref, p) if p < total // 2 else (far_ref, p - total // 2)
        pooled_ref[pl.ds(firsts[p], chunk), :] = ref[at * chunk : (at + 1) * chunk, :]
    targets = target_ref[...].reshape(1, target_ref.shape[0])
    loss, grad_proj, dm = contrast(pooled_ref[...], targets, wp_ref[...], slots)
    loss_ref[...] = loss
    gproj_ref[...] = grad_proj
    dm_ref[...] = dm
    own_ref[...] = dm_ref[pl.ds(firsts[0], chunk), :]
    low_ref[...] = dm.astype(BF16)


def contrast_call(where, near, far, targets, w_proj, slots, masks):
    count, width = 2 * near.shape[0], near.shape[1]
    total = len(masks)
    chunk = count // total
    if count > 1024:
        both = jnp.concatenate([near, far], axis=0).reshape(total, chunk, width)
        places = where ^ jnp.asarray(np.asarray(masks, np.int32))
        pooled = jnp.zeros_like(both).at[places].set(both).reshape(count, width)
        loss, grad_proj, dm = contrast(pooled, targets.reshape(1, -1), w_proj, slots)
        own = dm.reshape(total, chunk, width)[where[0]]
        return loss, grad_proj, own, dm.astype(BF16)
    vmem = pl.BlockSpec(memory_space=pltpu.VMEM)
    return pl.pallas_call(
        functools.partial(contrast_kernel, slots=slots, masks=masks),
        name="contrast_all",
        in_specs=[pl.BlockSpec(memory_space=pltpu.SMEM)] + [vmem] * 4,
        out_shape=[
            jax.ShapeDtypeStruct((1, 1), F32),
            jax.ShapeDtypeStruct(w_proj.shape, F32),
            jax.ShapeDtypeStruct((chunk, width), F32),
            jax.ShapeDtypeStruct((count, width), BF16),
        ],
        scratch_shapes=[pltpu.VMEM((count, width), BF16), pltpu.VMEM((count, width), F32)],
        compiler_params=pltpu.CompilerParams(vmem_limit_bytes=VMEM_SHARED),
    )(where, near, far, targets, w_proj)


def ffn_out_kernel(where_ref, near_ref, far_ref, dm_ref, out_ref, all_ref, *, masks):
    total = len(masks)
    chunk = all_ref.shape[0] // total
    for p in range(total):
        ref, at = (near_ref, p) if p < total // 2 else (far_ref, p - total // 2)
        first = pl.multiple_of((where_ref[0] ^ masks[p]) * chunk, chunk)
        all_ref[pl.ds(first, chunk), :] = ref[at * chunk : (at + 1) * chunk, :]
    out_ref[...] = dot(all_ref[...], dm_ref[...], 0, 0)


def ffn_out_grad(where, near, far, dm, masks):
    half, inner = near.shape
    width = dm.shape[1]
    side = pl.BlockSpec((half, width), lambda i: (0, i))
    return pl.pallas_call(
        functools.partial(ffn_out_kernel, masks=masks),
        name="ffn_out_grad",
        grid=(inner // width,),
        in_specs=[pl.BlockSpec(memory_space=pltpu.SMEM), side, side, whole(dm.shape)],
        out_specs=pl.BlockSpec((width, width), lambda i: (i, 0)),
        out_shape=jax.ShapeDtypeStruct((inner, width), F32),
        scratch_shapes=[pltpu.VMEM((2 * half, width), BF16)],
        compiler_params=pltpu.CompilerParams(vmem_limit_bytes=VMEM_SHARED),
    )(where, near, far, dm)


def ffn_back_kernel(
    where_ref, seg_ref, dm_ref, act_ref, n2_ref, hid_ref, o_ref, g2_ref, win_ref, wout_ref, wo_ref,
    dh_ref, do_ref, keep_ref, send_ref, g2grad_ref,
    acc_ref, du_all, dhb_all, g2_acc, *, masks
):
    step = pl.program_id(0)
    last = pl.num_programs(0) - 1
    length, width = hid_ref.shape[1:]
    slots = length // QLEN

    onehot = slot_onehot(seg_ref[pl.ds(step, 1), :], slots)
    onehot_f = onehot.astype(F32)
    onehot_low = onehot_f.astype(BF16)
    counts = jnp.maximum(jnp.sum(onehot_f, axis=-1, keepdims=True), 1.0)
    dy_slot = dm_ref[pl.ds(pl.multiple_of(step * slots, slots), slots), :] / counts
    dyb_slot = dy_slot.astype(BF16)
    dact_slot = dot(dyb_slot, wout_ref[...], 1, 1).astype(BF16)
    dact = dot(onehot_low, dact_slot, 0, 0).astype(BF16)
    act = act_ref[0]
    du = jnp.where(act > 0, dact, jnp.zeros_like(dact))
    here = pl.ds(pl.multiple_of(step * length, length), length)
    du_all[here, :] = du
    dn2 = dot(du, win_ref[...], 1, 1)
    hidden = hid_ref[0]
    scale = rms_scale(hidden)
    g2_part = jnp.sum(dn2 * hidden * scale, axis=0, keepdims=True)
    high, low = split_two(dy_slot)
    dy = dot(onehot_low, high, 0, 0) + dot(onehot_low, low, 0, 0)
    dh = dy + norm_back(dn2, hidden, scale, gain_row(g2_ref))
    dh_ref[0] = dh
    dhb = dh.astype(BF16)
    dhb_all[here, :] = dhb
    do_ref[0] = dot(dhb, wo_ref[...], 1, 1).astype(BF16)

    @pl.when(step == 0)
    def _():
        g2_acc[...] = g2_part

    @pl.when(step > 0)
    def _():
        g2_acc[...] += g2_part

    @pl.when(step == last)
    def _():
        rows, inner = n2_ref.shape[0], du_all.shape[1]
        turned = n2_ref[...].reshape(rows * length, width).T
        for at in range(0, inner, width):
            acc_ref[at : at + width, :] = dot(turned, du_all[:, at : at + width]).astype(BF16)
        turned = o_ref[...].reshape(rows * length, width).T
        acc_ref[inner : inner + width, :] = dot(turned, dhb_all[...]).astype(BF16)
        if acc_ref.shape[0] > inner + width:
            acc_ref[inner + width :, :] = jnp.zeros_like(acc_ref[inner + width :, :])
        take_chunks(acc_ref, keep_ref, send_ref, where_ref[0], masks)
        g2grad_ref[...] = g2_acc[...]


def ffn_back(where, seg, dm, act, n2, hidden, mixed, g2, win, wout, wo, masks):
    rows, length, width = hidden.shape
    inner = win.shape[1]
    lines = padded_rows(inner + width, len(masks))
    return pl.pallas_call(
        functools.partial(ffn_back_kernel, masks=masks),
        name="ffn_back",
        grid=(rows,),
        in_specs=[pl.BlockSpec(memory_space=pltpu.SMEM), whole(seg.shape), whole(dm.shape)]
        + [per_row((length, inner)), whole(n2.shape), per_row((length, width)), whole(mixed.shape)]
        + [whole(a.shape) for a in (g2, win, wout, wo)],
        out_specs=[per_row((length, width))] * 2
        + [whole((lines // 2, width))] * 2
        + [whole((1, width))],
        out_shape=[
            jax.ShapeDtypeStruct(hidden.shape, F32),
            jax.ShapeDtypeStruct(hidden.shape, BF16),
            jax.ShapeDtypeStruct((lines // 2, width), BF16),
            jax.ShapeDtypeStruct((lines // 2, width), BF16),
            jax.ShapeDtypeStruct((1, width), F32),
        ],
        scratch_shapes=[
            pltpu.VMEM((lines, width), BF16),
            pltpu.VMEM((rows * length, inner), BF16),
            pltpu.VMEM((rows * length, width), BF16),
            pltpu.VMEM((1, width), F32),
        ],
        compiler_params=pltpu.CompilerParams(vmem_limit_bytes=VMEM_SHARED),
    )(where, seg, dm, act, n2, hidden, mixed, g2, win, wout, wo)


def attn_back_kernel(*refs, group, masks):
    where_ref, n1_ref, q_ref, k_ref, v_ref, p_ref, o_ref, do_ref = refs[:8]
    before_refs = refs[8 : 8 + group]
    tail = refs[8 + group :]
    dqkv_ref, band_ref, grad_refs = tail[0], tail[1], tail[2:-4]
    dkt_ref, dvt_ref, acc_ref, wacc_ref = tail[-4:]
    step = pl.program_id(0)
    last = pl.num_programs(0) - 1
    length, width = n1_ref.shape[1:]
    heads = p_ref.shape[1]
    own_width = q_ref.shape[2]
    head_size = own_width // heads
    blocks = length // BLK
    low_lane = lax.broadcasted_iota(jnp.int32, (length, 2 * head_size), 1) < head_size

    @pl.when(step == 0)
    def _():
        acc_ref[...] = jnp.zeros_like(acc_ref)

    def pair(index, carry):
        lanes = pl.ds(pl.multiple_of(index * 2 * head_size, 2 * head_size), 2 * head_size)
        q_pair = q_ref[0, :, lanes]
        k_pair = k_ref[0, :, lanes]
        v_pair = v_ref[0, :, lanes]
        do_pair = do_ref[0, :, lanes]
        q_turned = q_pair.T
        do_turned = do_pair.T
        product = do_pair.astype(F32) * o_ref[0, :, lanes].astype(F32)
        dq_parts = []
        for part in range(2):
            head = index * 2 + part
            keep = low_lane if part == 0 else jnp.logical_not(low_lane)
            do_head = jnp.where(keep, do_pair, jnp.zeros_like(do_pair))
            delta = jnp.sum(jnp.where(keep, product, 0.0), axis=-1, keepdims=True)
            probs = p_ref[0, head]
            dprobs = dot(do_head, v_pair, 1, 1)
            ds = probs.astype(F32) * (dprobs - delta)
            ds_low = ds.astype(BF16)
            sums = {}
            for i in range(blocks):
                for j in range(blocks):
                    place = max(-2, min(2, j - i)) + 2
                    tile = ds[i * BLK : (i + 1) * BLK, j * BLK : (j + 1) * BLK]
                    sums[place] = tile if place not in sums else sums[place] + tile
            for place, value in sums.items():
                acc_ref[head, :, place * BLK : (place + 1) * BLK] += value
            dq_parts.append(dot(ds_low, k_pair))
            own = slice(part * head_size, (part + 1) * head_size)
            place = pl.ds(pl.multiple_of(head * head_size, head_size), head_size)
            dkt_ref[place, :] = dot(q_turned[own], ds_low).astype(BF16)
            dvt_ref[place, :] = dot(do_turned[own], probs).astype(BF16)
        dqkv_ref[0, 0, :, lanes] = jnp.where(low_lane, dq_parts[0], dq_parts[1]).astype(BF16)
        return carry

    lax.fori_loop(0, heads // 2, pair, 0)
    dq = dqkv_ref[0, 0]
    dk = dkt_ref[...].T
    dv = dvt_ref[...].T
    dqkv_ref[0, 1] = dk
    dqkv_ref[0, 2] = dv
    parts = [dot(n1_ref[0], d, 0, 0) for d in (dq, dk, dv)]

    here = slice(group * own_width, (group + 1) * own_width)
    if len(grad_refs) == 1:
        here = slice(0, own_width)

    @pl.when(step == 0)
    def _():
        for index in range(3):
            wacc_ref[index * width : (index + 1) * width, here] = parts[index]

    @pl.when(step > 0)
    def _():
        for index in range(3):
            wacc_ref[index * width : (index + 1) * width, here] += parts[index]

    @pl.when(step == last)
    def _():
        if len(grad_refs) == 1:
            grad_refs[0][...] = wacc_ref[...].astype(BF16)
        else:
            for index, ref in enumerate(before_refs):
                lanes = slice(index * own_width, (index + 1) * own_width)
                wacc_ref[: 3 * width, lanes] = ref[...].astype(F32)
            if wacc_ref.shape[0] > 3 * width:
                wacc_ref[3 * width :, :] = jnp.zeros_like(wacc_ref[3 * width :, :])
            take_chunks(wacc_ref, grad_refs[0], grad_refs[1], where_ref[0], masks)
        for head in range(heads):
            far_low = jnp.sum(acc_ref[head, :, :BLK], axis=0, keepdims=True)
            far_high = jnp.sum(acc_ref[head, :, 4 * BLK :], axis=0, keepdims=True)
            band = jnp.concatenate(
                [acc_ref[head, :, BLK : 4 * BLK], jnp.zeros((BLK, BLK), F32)], axis=1
            )
            rows = BLK // 2
            while rows >= 1:
                band = band[:rows] + pltpu.roll(band[rows:], 4 * BLK - rows, 1)
                rows //= 2
            band_ref[head : head + 1, : 4 * BLK] = band
            band_ref[head : head + 1, 4 * BLK : 5 * BLK] = far_low
            band_ref[head : head + 1, 5 * BLK :] = far_high


def attn_back(where, n1, q, k, v, probs, mixed, do, before, groups, masks):
    group = len(before)
    rows, length, width = n1.shape
    heads = probs.shape[1] // groups
    own_width = width // groups
    lanes = pl.BlockSpec((1, length, own_width), lambda r: (r, 0, group))
    low = lambda *s: jax.ShapeDtypeStruct(s, BF16)
    if group < groups - 1:
        grads = [low(3 * width, own_width)]
        acc = (3 * width, own_width)
    else:
        lines = padded_rows(3 * width, len(masks))
        grads = [low(lines // 2, width)] * 2
        acc = (lines, width)
    return pl.pallas_call(
        functools.partial(attn_back_kernel, group=group, masks=masks),
        name=f"attn_back_{group}",
        grid=(rows,),
        in_specs=[pl.BlockSpec(memory_space=pltpu.SMEM), per_row((length, width))]
        + [lanes] * 3
        + [pl.BlockSpec((1, heads, length, length), lambda r: (r, group, 0, 0)), lanes, lanes]
        + [whole(g.shape) for g in before],
        out_specs=[per_row((3, length, own_width)), whole((heads, 6 * BLK))]
        + [whole(g.shape) for g in grads],
        out_shape=[
            low(rows, 3, length, own_width),
            jax.ShapeDtypeStruct((heads, 6 * BLK), F32),
        ]
        + grads,
        scratch_shapes=[
            pltpu.VMEM((own_width, length), BF16),
            pltpu.VMEM((own_width, length), BF16),
            pltpu.VMEM((heads, BLK, 5 * BLK), F32),
            pltpu.VMEM(acc, F32),
        ],
        compiler_params=pltpu.CompilerParams(vmem_limit_bytes=VMEM_SMALL),
    )(where, n1, q, k, v, probs, mixed, do, *before)


def finish_kernel(*refs, groups):
    tok_ref, dh_ref, g1_ref, g2grad_ref, table_ref, wq_ref, wk_ref, wv_ref = refs[:8]
    dqkv_refs, band_refs = refs[8 : 8 + groups], refs[8 + groups : 8 + 2 * groups]
    tgrad_ref, small_out, g1_acc, small_ref = refs[8 + 2 * groups :]
    step = pl.program_id(0)
    last = pl.num_programs(0) - 1
    own_width = dqkv_refs[0].shape[3]
    heads = band_refs[0].shape[0]
    dn1 = None
    for index, weight in enumerate((wq_ref, wk_ref, wv_ref)):
        whole_grad = jnp.concatenate([ref[0, index] for ref in dqkv_refs], axis=1)
        part = dot(whole_grad, weight[...], 1, 1)
        dn1 = part if dn1 is None else dn1 + part
    x = tok_ref[0].astype(F32)
    scale = rms_scale(x)
    g1_part = jnp.sum(dn1 * x * scale, axis=0, keepdims=True)
    tgrad_ref[0] = (dh_ref[0] + norm_back(dn1, x, scale, gain_row(g1_ref))).astype(BF16)

    @pl.when(step == 0)
    def _():
        g1_acc[...] = g1_part

    @pl.when(step > 0)
    def _():
        g1_acc[...] += g1_part

    @pl.when(step == last)
    def _():
        width = small_ref.shape[1]
        small_ref[...] = jnp.zeros_like(small_ref)
        for at in range(width // BLK):
            lanes = slice(at * BLK, (at + 1) * BLK)
            small_ref[at : at + 1, BLK : 2 * BLK] = g1_acc[:, lanes]
            small_ref[at : at + 1, 2 * BLK : 3 * BLK] = g2grad_ref[:, lanes]
        for group in range(groups):
            band = band_refs[group][...]
            high = band.astype(BF16)
            rest = band - high.astype(F32)
            low = rest.astype(BF16)
            least = (rest - low.astype(F32)).astype(BF16)
            table = table_ref[...]
            bias = dot(high, table) + dot(low, table) + dot(least, table)
            small_ref[group * heads : (group + 1) * heads, : bias.shape[1]] = bias
        small_out[...] = small_ref[...].astype(BF16)


def finish(tokens, dh, g1, g2grad, table, wq, wk, wv, dqkvs, bands):
    rows, length, width = tokens.shape
    groups = len(dqkvs)
    lead = groups * bands[0].shape[0]
    return pl.pallas_call(
        functools.partial(finish_kernel, groups=groups),
        name="finish_rows",
        grid=(rows,),
        in_specs=[per_row((length, width))] * 2
        + [whole(a.shape) for a in (g1, g2grad, table, wq, wk, wv)]
        + [per_row(d.shape[1:]) for d in dqkvs]
        + [whole(b.shape) for b in bands],
        out_specs=[per_row((length, width)), whole((lead, width))],
        out_shape=[
            jax.ShapeDtypeStruct(tokens.shape, BF16),
            jax.ShapeDtypeStruct((lead, width), BF16),
        ],
        scratch_shapes=[pltpu.VMEM((1, width), F32), pltpu.VMEM((lead, width), F32)],
        compiler_params=pltpu.CompilerParams(vmem_limit_bytes=VMEM_SMALL),
    )(tokens, dh, g1, g2grad, table, wq, wk, wv, *dqkvs, *bands)


def band_table(length):
    buckets = bucket_offsets(length)
    zero = length - 1
    table = np.zeros((6 * BLK, NB), np.float32)
    for column in range(4 * BLK):
        offset = column - BLK if column < 3 * BLK else column - 5 * BLK
        if -2 * BLK < offset < 2 * BLK and abs(offset) < length:
            table[column, buckets[zero + offset]] = 1.0
    far = buckets[: zero - BLK], buckets[zero + BLK + 1 :]
    assert len(set(far[0])) == 1 and len(set(far[1])) == 1
    table[4 * BLK : 5 * BLK, far[0][0]] = 1.0
    table[5 * BLK :, far[1][0]] = 1.0
    return table


def unpack_big_kernel(where_ref, near_ref, far_ref, win_out, wo_out, all_ref, *, masks):
    total = len(masks)
    width = wo_out.shape[1]
    chunk = 2 * near_ref.shape[0] // total
    for p in range(total):
        ref, at = (near_ref, p) if p < total // 2 else (far_ref, p - total // 2)
        first = pl.multiple_of((where_ref[0] ^ masks[p]) * chunk, chunk)
        all_ref[pl.ds(first, chunk), :] = ref[at * chunk : (at + 1) * chunk, :].astype(F32)
    parts = win_out.shape[1] // width
    for part in range(parts):
        win_out[:, part * width : (part + 1) * width] = all_ref[part * width : (part + 1) * width, :]
    wo_out[...] = all_ref[parts * width : (parts + 1) * width, :]


def unpack_big(where, near, far, inner, width, masks):
    vmem = pl.BlockSpec(memory_space=pltpu.VMEM)
    return pl.pallas_call(
        functools.partial(unpack_big_kernel, masks=masks),
        name="unpack_ffn",
        in_specs=[pl.BlockSpec(memory_space=pltpu.SMEM), vmem, vmem],
        out_shape=[
            jax.ShapeDtypeStruct((width, inner), F32),
            jax.ShapeDtypeStruct((width, width), F32),
        ],
        scratch_shapes=[pltpu.VMEM((2 * near.shape[0], width), F32)],
        compiler_params=pltpu.CompilerParams(vmem_limit_bytes=VMEM_SMALL),
    )(where, near, far)


def unpack_qkv_kernel(
    where_ref, near_ref, far_ref, wq_out, wk_out, wv_out, g1_out, g2_out, bias_out,
    all_ref, small_all, *, masks
):
    total = len(masks)
    width = wq_out.shape[1]
    lead = bias_out.shape[0]
    rows = 2 * near_ref.shape[0] // total
    chunk = rows - lead
    for p in range(total):
        ref, at = (near_ref, p) if p < total // 2 else (far_ref, p - total // 2)
        owner = where_ref[0] ^ masks[p]
        piece = ref[at * rows : (at + 1) * rows, :].astype(F32)
        all_ref[pl.ds(pl.multiple_of(owner * chunk, chunk), chunk), :] = piece[:chunk]
        small_all[pl.ds(pl.multiple_of(owner * lead, lead), lead), :] = piece[
            chunk:, : small_all.shape[1]
        ]
    small = small_all[:lead, :]
    for p in range(1, total):
        small = small + small_all[p * lead : (p + 1) * lead, :]
    for index, ref in enumerate((wq_out, wk_out, wv_out)):
        ref[...] = all_ref[index * width : (index + 1) * width, :]
    for at in range(width // BLK):
        lanes = slice(at * BLK, (at + 1) * BLK)
        g1_out[:, lanes] = small[at : at + 1, BLK : 2 * BLK]
        g2_out[:, lanes] = small[at : at + 1, 2 * BLK : 3 * BLK]
    bias_out[...] = small[:, : bias_out.shape[1]]


def unpack_qkv(where, near, far, width, heads, masks):
    full = lambda *s: jax.ShapeDtypeStruct(s, F32)
    vmem = pl.BlockSpec(memory_space=pltpu.VMEM)
    total = len(masks)
    return pl.pallas_call(
        functools.partial(unpack_qkv_kernel, masks=masks),
        name="unpack_attn",
        in_specs=[pl.BlockSpec(memory_space=pltpu.SMEM), vmem, vmem],
        out_shape=[full(width, width)] * 3 + [full(1, width)] * 2 + [full(heads, NB)],
        scratch_shapes=[
            pltpu.VMEM((2 * near.shape[0] - total * heads, width), F32),
            pltpu.VMEM((total * heads, 3 * BLK), F32),
        ],
        compiler_params=pltpu.CompilerParams(vmem_limit_bytes=VMEM_SMALL),
    )(where, near, far)


def bit_groups(wide, narrow):
    total = wide * narrow
    assert total & (total - 1) == 0 and narrow & (narrow - 1) == 0
    bits = [1 << s for s in range(total.bit_length() - 1)]
    outer = [b for b in bits if b >= narrow]
    inner = [b for b in bits if b < narrow]
    pairs = lambda items: [items[i : i + 2] for i in range(0, len(items), 2)]
    return [outer[:1]] + pairs(outer[1:]) + pairs(inner)


def group_masks(group):
    return chunk_masks(group)[1:]


def swap(values, mask, total):
    return lax.ppermute(values, AXES, [(i, i ^ mask) for i in range(total)])


def after(values, *others):
    return lax.optimization_barrier((values,) + others)[0]


def split_rows(values, count):
    rows = values.shape[0] // count
    return [values[i * rows : (i + 1) * rows] for i in range(count)]


class Gather:
    def __init__(self, values, groups, total):
        self.pieces, self.left, self.total = [values], list(reversed(groups)), total

    def step(self, *hold):
        if self.left:
            values = self.pieces[0]
            if len(self.pieces) > 1:
                pieces = lax.optimization_barrier(tuple(self.pieces) + hold)[: len(self.pieces)]
                values = jnp.concatenate(pieces, axis=0)
            masks = group_masks(self.left.pop(0))
            self.pieces = [values] + [swap(values, mask, self.total) for mask in masks]

    def rest(self):
        while self.left:
            self.step()
        return self.pieces


class Scatter:
    def __init__(self, blocks, groups, total):
        self.blocks, self.left, self.total = list(blocks), list(groups), total

    def step(self, *hold):
        if self.left:
            masks = group_masks(self.left.pop(0))
            got = [swap(b, mask, self.total) for b, mask in zip(self.blocks[1:], masks)]
            if hold:
                got = list(lax.optimization_barrier(tuple(got) + hold)[: len(got)])
            count = 1 << len(self.left[0]) if self.left else 1
            parts = [split_rows(b, count) for b in [self.blocks[0]] + got]
            self.blocks = []
            for column in zip(*parts):
                value = column[0].astype(F32)
                for other in column[1:]:
                    value = value + other.astype(F32)
                self.blocks.append(value.astype(BF16))

    def rest(self):
        while self.left:
            self.step()
        return self.blocks[0]


GROUPS = 2


def local(
    tokens, seg_ids, positives, norm1_gain, w_query, w_key, w_value, w_attn_out,
    rel_bias, norm2_gain, w_in, w_ffn_out, w_proj,
):
    rows, length, width = tokens.shape
    heads = rel_bias.shape[1]
    slots = length // QLEN
    inner = w_in.shape[1]
    wide, narrow = lax.axis_size("wide"), lax.axis_size("narrow")
    total = wide * narrow
    linear = lax.axis_index("wide") * narrow + lax.axis_index("narrow")
    where = jnp.full((1,), linear, jnp.int32)
    groups = bit_groups(wide, narrow)
    masks = chunk_masks([b for g in groups for b in g])
    buckets = bucket_offsets(length)
    hot = np.zeros((NB, 2 * length), np.float32)
    hot[buckets, np.arange(2 * length - 1)] = 1.0

    n1, q, k, v, probs, mixed, hidden, n2, act, abar, pooled = forward(
        seg_ids, tokens, norm1_gain, w_query, w_key, w_value, w_attn_out, rel_bias.T,
        jnp.asarray(hot, BF16), norm2_gain, w_in, w_ffn_out, slots,
    )
    slot = Gather(pooled, groups, total)
    slot.step()
    slot.step()
    acts = Gather(abar, groups, total)
    acts.step()
    slot.step(*acts.pieces)
    near, far = slot.rest()
    loss, grad_proj, dm_own, dm_low = contrast_call(
        where, near, far, positives, w_proj, slots, masks
    )
    dh, do, big_keep, big_send, grad_g2 = ffn_back(
        where, seg_ids, dm_own, act, n2, hidden, mixed, norm2_gain, w_in, w_ffn_out, w_attn_out,
        masks,
    )
    acts.step(do)
    big = Scatter([big_keep, big_send], groups, total)
    dqkvs, bands, before, tie = [], [], [], acts.pieces[:1]
    for _ in range(GROUPS):
        dqkv, band, *grads = attn_back(
            where, n1, q, k, v, probs, mixed, after(do, *tie), before, GROUPS, masks
        )
        dqkvs.append(dqkv)
        bands.append(band)
        before = before + grads[:1]
        if len(before) == 1:
            big.step(band)
            acts.step(band)
            tie = big.blocks + acts.pieces[:1]
    tokens_grad, small = finish(
        tokens, dh, norm1_gain, grad_g2, jnp.asarray(band_table(length), BF16),
        w_query, w_key, w_value, dqkvs, bands,
    )
    big.step(small)
    qkv = Scatter([grads[0], after(grads[1], *big.blocks)], groups, total)
    qkv.step()
    big.step(*qkv.blocks)
    big_all = Gather(big.rest(), groups, total)
    big_all.step()
    qkv.step(big_all.pieces[0])
    big_all.step(*qkv.blocks)
    qkv.step(big_all.pieces[0])
    qkv_all = Gather(jnp.concatenate([qkv.rest(), small], axis=0), groups, total)
    qkv_all.step()
    grad_ffn_out = ffn_out_grad(where, *acts.rest(), after(dm_low, qkv_all.pieces[0]), masks)
    qkv_all.step(grad_ffn_out)
    big_all.step(qkv_all.pieces[0])
    win, wo = unpack_big(where, *big_all.rest(), inner, width, masks)
    qkv_all.step(wo)
    wq, wk, wv, grad_g1, grad_g2, grad_bias = unpack_qkv(
        where, *qkv_all.rest(), width, heads, masks
    )
    return (
        loss[0, 0],
        tokens_grad,
        grad_g1[0],
        wq,
        wk,
        wv,
        wo,
        grad_bias.T,
        grad_g2[0],
        win,
        grad_ffn_out,
        grad_proj,
    )


def solution(mesh):
    rows = P(AXES, None, None)
    in_specs = (rows, P(AXES, None)) + (P(),) * 11
    out_specs = (P(), rows) + (P(),) * 10
    return jax.shard_map(local, mesh=mesh, in_specs=in_specs, out_specs=out_specs, check_vma=False)
```

```python
import functools

import jax
import jax.numpy as jnp
import numpy as np
from jax import lax
from jax.experimental import pallas as pl
from jax.experimental.pallas import tpu as pltpu
from jax.sharding import PartitionSpec as P

NB = 32
MAXD = 128
QLEN = 64
PPR = 2

EPS_NORM = 1e-06
LOGIT_SCALE = 50.0
MASKED = -1e30
HIGHEST = lax.Precision.HIGHEST
F32 = jnp.float32
BF16 = jnp.bfloat16
AXES = ("wide", "narrow")
BLK = 128
VMEM_LIMIT = 60 * 1024 * 1024
VMEM_SHARED = 44 * 1024 * 1024
VMEM_SMALL = 28 * 1024 * 1024


def bucket_offsets(length):
    offset = np.arange(-(length - 1), length)
    half_count = NB // 2
    exact_span = half_count // 2
    distance = -offset
    bucket = (distance < 0).astype(np.int64) * half_count
    distance = np.abs(distance)
    far_bucket = exact_span + (
        np.log(np.maximum(distance, 1) / exact_span)
        / np.log(MAXD / exact_span)
        * (half_count - exact_span)
    ).astype(np.int64)
    far_bucket = np.minimum(far_bucket, half_count - 1)
    bucket = bucket + np.where(distance < exact_span, distance, far_bucket)
    return bucket.astype(np.int32)


def dot(left, right, left_dim=1, right_dim=0):
    return lax.dot_general(
        left, right, (((left_dim,), (right_dim,)), ((), ())), preferred_element_type=F32
    )


def split_two(values):
    high = values.astype(BF16)
    return high, (values - high.astype(F32)).astype(BF16)


def rms_scale(values):
    return lax.rsqrt(jnp.mean(values * values, axis=-1, keepdims=True) + EPS_NORM)


def norm_back(grad_normed, inputs, scale, gain):
    scaled = grad_normed * gain
    return scale * scaled - inputs * (
        scale * scale * scale * jnp.mean(inputs * scaled, axis=-1, keepdims=True)
    )


def slot_onehot(seg_row, slot_count):
    length = seg_row.shape[1]
    return seg_row == lax.broadcasted_iota(jnp.int32, (slot_count, length), 0)


def gain_row(ref):
    return ref[...].astype(F32).reshape(1, ref.shape[0])


def forward_kernel(
    seg_ref, tok_ref, g1_ref, wq_ref, wk_ref, wv_ref, rel_ref, hot_ref, g2_ref,
    wo_hbm, win_hbm, wout_hbm,
    n1_out, q_out, k_out, v_out, p_out, o_out, hid_out, n2_out, act_out, abar_ref, m_ref,
    strip_ref, mask_ref, asum_ref, hsum_ref, wo_ref, win_ref, wout_ref,
    n1_ref, q_ref, k_ref, v_ref, p_ref, o_ref, hid_ref, n2_ref, act_ref, in_sem, out_sem, late_sem, p_sem,
):
    step = pl.program_id(0)
    row_count = pl.num_programs(0)
    length, width = tok_ref.shape[1:]
    heads = p_ref.shape[0]
    head_size = width // heads
    blocks = length // BLK
    slots = length // QLEN

    def fetch(index, source, target):
        return pltpu.make_async_copy(source, target, in_sem.at[index])

    fetches = [fetch(0, wo_hbm, wo_ref), fetch(1, win_hbm, win_ref), fetch(2, wout_hbm, wout_ref)]
    singles = [
        pltpu.make_async_copy(source, target.at[step], out_sem.at[index])
        for index, (source, target) in enumerate(
            [
                (n1_ref, n1_out), (q_ref, q_out), (k_ref, k_out), (v_ref, v_out),
            ]
        )
    ]

    def put_late(index, row):
        source, target = (
            (o_ref, o_out), (hid_ref, hid_out), (n2_ref, n2_out), (act_ref, act_out)
        )[index]
        return pltpu.make_async_copy(source.at[row], target.at[row], late_sem.at[index, row])

    def put_pair(index):
        two = pl.ds(index * 2, 2)
        return pltpu.make_async_copy(p_ref.at[two], p_out.at[step, two], p_sem.at[index])

    @pl.when(step == 0)
    def _():
        for copy in fetches:
            copy.start()
        off_bias = dot(rel_ref[...], hot_ref[...])
        for head in range(heads):
            wide = jnp.broadcast_to(off_bias[head : head + 1, :], (BLK, 2 * length))
            rolled = pltpu.roll(wide, 2 * length - BLK + 1, 1, stride=1, stride_axis=0)
            strip_ref[head] = rolled[:, : 2 * length - BLK]

    x = tok_ref[0].astype(F32)
    n1 = (x * rms_scale(x) * gain_row(g1_ref)).astype(BF16)
    n1_ref[...] = n1
    q_ref[...] = dot(n1, wq_ref[...]).astype(BF16)
    k_ref[...] = dot(n1, wk_ref[...]).astype(BF16)
    v_ref[...] = dot(n1, wv_ref[...]).astype(BF16)
    for copy in singles:
        copy.start()
    onehot = slot_onehot(seg_ref[pl.ds(step, 1), :], slots)
    onehot_f = onehot.astype(F32)
    onehot_low = onehot_f.astype(BF16)
    same = dot(onehot_low, onehot_low, 0, 0)
    mask_ref[...] = jnp.where(same > 0.5, 0.0, MASKED)
    low_lane = lax.broadcasted_iota(jnp.int32, (BLK, 2 * head_size), 1) < head_size
    low_all = lax.broadcasted_iota(jnp.int32, (length, 2 * head_size), 1) < head_size

    def pair(index, carry):
        lanes = pl.ds(pl.multiple_of(index * 2 * head_size, 2 * head_size), 2 * head_size)
        k_pair = k_ref[:, lanes]
        v_pair = v_ref[:, lanes]
        for block in range(blocks):
            rows = slice(block * BLK, (block + 1) * BLK)
            q_pair = q_ref[rows, lanes]
            for part in range(2):
                head = index * 2 + part
                keep = low_lane if part == 0 else jnp.logical_not(low_lane)
                q_head = jnp.where(keep, q_pair, jnp.zeros_like(q_pair))
                start = (blocks - 1 - block) * BLK
                scores = dot(q_head, k_pair, 1, 1)
                scores = scores + strip_ref[head, :, start : start + length] + mask_ref[rows, :]
                top = jnp.max(scores, axis=-1, keepdims=True)
                exps = jnp.exp(scores - top)
                total = jnp.sum(exps, axis=-1, keepdims=True)
                p_ref[head, rows, :] = (exps * (1.0 / total)).astype(BF16)
        put_pair(index).start()
        mixed = [dot(p_ref[index * 2 + part], v_pair) for part in range(2)]
        o_ref[step, :, lanes] = jnp.where(low_all, mixed[0], mixed[1]).astype(BF16)
        return carry

    lax.fori_loop(0, heads // 2, pair, 0)
    put_late(0, step).start()

    @pl.when(step == 0)
    def _():
        for copy in fetches:
            copy.wait()

    hidden = x + dot(o_ref[step], wo_ref[...])
    hid_ref[step] = hidden
    n2 = (hidden * rms_scale(hidden) * gain_row(g2_ref)).astype(BF16)
    n2_ref[step] = n2
    put_late(1, step).start()
    put_late(2, step).start()
    act = jnp.maximum(dot(n2, win_ref[...]), 0.0).astype(BF16)
    act_ref[step] = act
    put_late(3, step).start()
    counts = jnp.maximum(jnp.sum(onehot_f, axis=-1, keepdims=True), 1.0)
    asum = dot(onehot_low, act) / counts
    high, low = split_two(hidden)
    hsum = (dot(onehot_low, high) + dot(onehot_low, low)) / counts
    asum_ref[pl.ds(step * slots, slots), :] = asum
    hsum_ref[pl.ds(step * slots, slots), :] = hsum

    @pl.when(step == row_count - 1)
    def _():
        high, low = split_two(asum_ref[...])
        abar_ref[...] = high
        pooled = hsum_ref[...] + dot(high, wout_ref[...]) + dot(low, wout_ref[...])
        m_ref[...] = pooled.astype(BF16)
        for row in range(act_ref.shape[0]):
            for index in range(4):
                put_late(index, row).wait()

    for copy in singles:
        copy.wait()
    for index in range(heads // 2):
        put_pair(index).wait()


def whole(shape):
    return pl.BlockSpec(shape, lambda r: (0,) * len(shape))


def per_row(shape):
    return pl.BlockSpec((1,) + shape, lambda r: (r,) + (0,) * len(shape))


def forward(seg, tokens, g1, wq, wk, wv, wo, rel_bias, hot, g2, win, wout, slots):
    rows, length, width = tokens.shape
    heads = rel_bias.shape[0]
    inner = win.shape[1]
    low = lambda *s: jax.ShapeDtypeStruct(s, BF16)
    rlw = (rows, length, width)
    away = pl.BlockSpec(memory_space=pl.ANY)
    return pl.pallas_call(
        forward_kernel,
        name="forward_rows",
        grid=(rows,),
        in_specs=[whole(seg.shape), per_row((length, width))]
        + [whole(a.shape) for a in (g1, wq, wk, wv, rel_bias, hot, g2)]
        + [away] * 3,
        out_specs=[away] * 9 + [whole((rows * slots, inner)), whole((rows * slots, width))],
        out_shape=[low(*rlw)] * 4
        + [low(rows, heads, length, length), low(*rlw), jax.ShapeDtypeStruct(rlw, F32), low(*rlw)]
        + [low(rows, length, inner), low(rows * slots, inner), low(rows * slots, width)],
        scratch_shapes=[
            pltpu.VMEM((heads, BLK, 2 * length - BLK), F32),
            pltpu.VMEM((length, length), F32),
            pltpu.VMEM((rows * slots, inner), F32),
            pltpu.VMEM((rows * slots, width), F32),
            pltpu.VMEM(wo.shape, BF16),
            pltpu.VMEM(win.shape, BF16),
            pltpu.VMEM(wout.shape, BF16),
        ]
        + [pltpu.VMEM((length, width), BF16)] * 4
        + [
            pltpu.VMEM((heads, length, length), BF16),
            pltpu.VMEM(rlw, BF16),
            pltpu.VMEM(rlw, F32),
            pltpu.VMEM(rlw, BF16),
            pltpu.VMEM((rows, length, inner), BF16),
            pltpu.SemaphoreType.DMA((3,)),
            pltpu.SemaphoreType.DMA((4,)),
            pltpu.SemaphoreType.DMA((4, rows)),
            pltpu.SemaphoreType.DMA((heads // 2,)),
        ],
        compiler_params=pltpu.CompilerParams(vmem_limit_bytes=VMEM_LIMIT),
    )(seg, tokens, g1, wq, wk, wv, rel_bias, hot, g2, wo, win, wout)


def chunk_masks(order):
    count = len(order)
    return [
        sum(bit for place, bit in enumerate(order) if p >> (count - 1 - place) & 1)
        for p in range(1 << count)
    ]


def padded_rows(rows, total):
    return -(-rows // (16 * total)) * 16 * total


def take_chunks(source_ref, keep_ref, send_ref, where, masks):
    total = len(masks)
    chunk = 2 * keep_ref.shape[0] // total
    for p in range(total):
        first = pl.multiple_of((where ^ masks[p]) * chunk, chunk)
        values = source_ref[pl.ds(first, chunk), :].astype(BF16)
        ref, at = (keep_ref, p) if p < total // 2 else (send_ref, p - total // 2)
        ref[at * chunk : (at + 1) * chunk, :] = values


def contrast(pooled, targets, w_proj, slots):
    half = pooled.shape[0] // 2
    z = dot(pooled, w_proj)
    inv = lax.rsqrt(jnp.sum(z * z, axis=-1, keepdims=True) + EPS_NORM)
    unit = z * inv
    emb = unit.astype(BF16)
    emb_q, emb_p = emb[:half], emb[half:]
    logits = LOGIT_SCALE * dot(emb_p, emb_q, 1, 1)
    line = lax.broadcasted_iota(jnp.int32, (half, half), 0)
    logits = jnp.where(line % slots < PPR, logits, MASKED)
    hits = line == (targets // PPR) * slots + targets % PPR
    top = jnp.max(logits, axis=0, keepdims=True)
    exps = jnp.exp(logits - top)
    sums = jnp.sum(exps, axis=0, keepdims=True)
    picked = jnp.sum(jnp.where(hits, logits, 0.0), axis=0, keepdims=True)
    loss = jnp.sum(top + jnp.log(sums) - picked, axis=1, keepdims=True)
    weights = (exps / sums - hits.astype(F32)).astype(BF16)
    grad_q = LOGIT_SCALE * dot(weights, emb_p, 0, 0)
    grad_p = LOGIT_SCALE * dot(weights, emb_q)
    grad = jnp.concatenate([grad_q, grad_p], axis=0)
    dz = (inv * (grad - unit * jnp.sum(grad * unit, axis=-1, keepdims=True))).astype(BF16)
    grad_proj = dot(pooled, dz, 0, 0)
    dm = dot(dz, w_proj, 1, 1)
    return loss, grad_proj, dm


def contrast_kernel(
    where_ref, near_ref, far_ref, target_ref, wp_ref,
    loss_ref, gproj_ref, own_ref, low_ref, pooled_ref, dm_ref, *, slots, masks
):
    total = len(masks)
    chunk = own_ref.shape[0]
    firsts = [pl.multiple_of((where_ref[0] ^ mask) * chunk, chunk) for mask in masks]
    for p in range(total):
        ref, at = (near_ref, p) if p < total // 2 else (far_ref, p - total // 2)
        pooled_ref[pl.ds(firsts[p], chunk), :] = ref[at * chunk : (at + 1) * chunk, :]
    targets = target_ref[...].reshape(1, target_ref.shape[0])
    loss, grad_proj, dm = contrast(pooled_ref[...], targets, wp_ref[...], slots)
    loss_ref[...] = loss
    gproj_ref[...] = grad_proj
    dm_ref[...] = dm
    own_ref[...] = dm_ref[pl.ds(firsts[0], chunk), :]
    low_ref[...] = dm.astype(BF16)


def contrast_call(where, near, far, targets, w_proj, slots, masks):
    count, width = 2 * near.shape[0], near.shape[1]
    total = len(masks)
    chunk = count // total
    if count > 1024:
        both = jnp.concatenate([near, far], axis=0).reshape(total, chunk, width)
        places = where ^ jnp.asarray(np.asarray(masks, np.int32))
        pooled = jnp.zeros_like(both).at[places].set(both).reshape(count, width)
        loss, grad_proj, dm = contrast(pooled, targets.reshape(1, -1), w_proj, slots)
        own = dm.reshape(total, chunk, width)[where[0]]
        return loss, grad_proj, own, dm.astype(BF16)
    vmem = pl.BlockSpec(memory_space=pltpu.VMEM)
    return pl.pallas_call(
        functools.partial(contrast_kernel, slots=slots, masks=masks),
        name="contrast_all",
        in_specs=[pl.BlockSpec(memory_space=pltpu.SMEM)] + [vmem] * 4,
        out_shape=[
            jax.ShapeDtypeStruct((1, 1), F32),
            jax.ShapeDtypeStruct(w_proj.shape, F32),
            jax.ShapeDtypeStruct((chunk, width), F32),
            jax.ShapeDtypeStruct((count, width), BF16),
        ],
        scratch_shapes=[pltpu.VMEM((count, width), BF16), pltpu.VMEM((count, width), F32)],
        compiler_params=pltpu.CompilerParams(vmem_limit_bytes=VMEM_SHARED),
    )(where, near, far, targets, w_proj)


def ffn_out_kernel(where_ref, near_ref, far_ref, dm_ref, out_ref, all_ref, *, masks):
    total = len(masks)
    chunk = all_ref.shape[0] // total
    for p in range(total):
        ref, at = (near_ref, p) if p < total // 2 else (far_ref, p - total // 2)
        first = pl.multiple_of((where_ref[0] ^ masks[p]) * chunk, chunk)
        all_ref[pl.ds(first, chunk), :] = ref[at * chunk : (at + 1) * chunk, :]
    out_ref[...] = dot(all_ref[...], dm_ref[...], 0, 0)


def ffn_out_grad(where, near, far, dm, masks):
    half, inner = near.shape
    width = dm.shape[1]
    side = pl.BlockSpec((half, width), lambda i: (0, i))
    return pl.pallas_call(
        functools.partial(ffn_out_kernel, masks=masks),
        name="ffn_out_grad",
        grid=(inner // width,),
        in_specs=[pl.BlockSpec(memory_space=pltpu.SMEM), side, side, whole(dm.shape)],
        out_specs=pl.BlockSpec((width, width), lambda i: (i, 0)),
        out_shape=jax.ShapeDtypeStruct((inner, width), F32),
        scratch_shapes=[pltpu.VMEM((2 * half, width), BF16)],
        compiler_params=pltpu.CompilerParams(vmem_limit_bytes=VMEM_SHARED),
    )(where, near, far, dm)


def ffn_back_kernel(
    where_ref, seg_ref, dm_ref, act_ref, n2_ref, hid_ref, o_ref, g2_ref, win_ref, wout_ref, wo_ref,
    dh_ref, do_ref, keep_ref, send_ref, g2grad_ref,
    acc_ref, du_all, dhb_all, g2_acc, *, masks
):
    step = pl.program_id(0)
    last = pl.num_programs(0) - 1
    length, width = hid_ref.shape[1:]
    slots = length // QLEN

    onehot = slot_onehot(seg_ref[pl.ds(step, 1), :], slots)
    onehot_f = onehot.astype(F32)
    onehot_low = onehot_f.astype(BF16)
    counts = jnp.maximum(jnp.sum(onehot_f, axis=-1, keepdims=True), 1.0)
    dy_slot = dm_ref[pl.ds(pl.multiple_of(step * slots, slots), slots), :] / counts
    dyb_slot = dy_slot.astype(BF16)
    dact_slot = dot(dyb_slot, wout_ref[...], 1, 1).astype(BF16)
    dact = dot(onehot_low, dact_slot, 0, 0).astype(BF16)
    act = act_ref[0]
    du = jnp.where(act > 0, dact, jnp.zeros_like(dact))
    here = pl.ds(pl.multiple_of(step * length, length), length)
    du_all[here, :] = du
    dn2 = dot(du, win_ref[...], 1, 1)
    hidden = hid_ref[0]
    scale = rms_scale(hidden)
    g2_part = jnp.sum(dn2 * hidden * scale, axis=0, keepdims=True)
    high, low = split_two(dy_slot)
    dy = dot(onehot_low, high, 0, 0) + dot(onehot_low, low, 0, 0)
    dh = dy + norm_back(dn2, hidden, scale, gain_row(g2_ref))
    dh_ref[0] = dh
    dhb = dh.astype(BF16)
    dhb_all[here, :] = dhb
    do_ref[0] = dot(dhb, wo_ref[...], 1, 1).astype(BF16)

    @pl.when(step == 0)
    def _():
        g2_acc[...] = g2_part

    @pl.when(step > 0)
    def _():
        g2_acc[...] += g2_part

    @pl.when(step == last)
    def _():
        rows, inner = n2_ref.shape[0], du_all.shape[1]
        turned = n2_ref[...].reshape(rows * length, width).T
        for at in range(0, inner, width):
            acc_ref[at : at + width, :] = dot(turned, du_all[:, at : at + width]).astype(BF16)
        turned = o_ref[...].reshape(rows * length, width).T
        acc_ref[inner : inner + width, :] = dot(turned, dhb_all[...]).astype(BF16)
        if acc_ref.shape[0] > inner + width:
            acc_ref[inner + width :, :] = jnp.zeros_like(acc_ref[inner + width :, :])
        take_chunks(acc_ref, keep_ref, send_ref, where_ref[0], masks)
        g2grad_ref[...] = g2_acc[...]


def ffn_back(where, seg, dm, act, n2, hidden, mixed, g2, win, wout, wo, masks):
    rows, length, width = hidden.shape
    inner = win.shape[1]
    lines = padded_rows(inner + width, len(masks))
    return pl.pallas_call(
        functools.partial(ffn_back_kernel, masks=masks),
        name="ffn_back",
        grid=(rows,),
        in_specs=[pl.BlockSpec(memory_space=pltpu.SMEM), whole(seg.shape), whole(dm.shape)]
        + [per_row((length, inner)), whole(n2.shape), per_row((length, width)), whole(mixed.shape)]
        + [whole(a.shape) for a in (g2, win, wout, wo)],
        out_specs=[per_row((length, width))] * 2
        + [whole((lines // 2, width))] * 2
        + [whole((1, width))],
        out_shape=[
            jax.ShapeDtypeStruct(hidden.shape, F32),
            jax.ShapeDtypeStruct(hidden.shape, BF16),
            jax.ShapeDtypeStruct((lines // 2, width), BF16),
            jax.ShapeDtypeStruct((lines // 2, width), BF16),
            jax.ShapeDtypeStruct((1, width), F32),
        ],
        scratch_shapes=[
            pltpu.VMEM((lines, width), BF16),
            pltpu.VMEM((rows * length, inner), BF16),
            pltpu.VMEM((rows * length, width), BF16),
            pltpu.VMEM((1, width), F32),
        ],
        compiler_params=pltpu.CompilerParams(vmem_limit_bytes=VMEM_SHARED),
    )(where, seg, dm, act, n2, hidden, mixed, g2, win, wout, wo)


def attn_back_kernel(*refs, group, masks):
    where_ref, n1_ref, q_ref, k_ref, v_ref, p_ref, o_ref, do_ref = refs[:8]
    before_refs = refs[8 : 8 + group]
    tail = refs[8 + group :]
    dqkv_ref, band_ref, grad_refs = tail[0], tail[1], tail[2:-4]
    dkt_ref, dvt_ref, acc_ref, wacc_ref = tail[-4:]
    step = pl.program_id(0)
    last = pl.num_programs(0) - 1
    length, width = n1_ref.shape[1:]
    heads = p_ref.shape[1]
    own_width = q_ref.shape[2]
    head_size = own_width // heads
    blocks = length // BLK
    low_lane = lax.broadcasted_iota(jnp.int32, (length, 2 * head_size), 1) < head_size

    @pl.when(step == 0)
    def _():
        acc_ref[...] = jnp.zeros_like(acc_ref)

    def pair(index, carry):
        lanes = pl.ds(pl.multiple_of(index * 2 * head_size, 2 * head_size), 2 * head_size)
        q_pair = q_ref[0, :, lanes]
        k_pair = k_ref[0, :, lanes]
        v_pair = v_ref[0, :, lanes]
        do_pair = do_ref[0, :, lanes]
        q_turned = q_pair.T
        do_turned = do_pair.T
        product = do_pair.astype(F32) * o_ref[0, :, lanes].astype(F32)
        dq_parts = []
        for part in range(2):
            head = index * 2 + part
            keep = low_lane if part == 0 else jnp.logical_not(low_lane)
            do_head = jnp.where(keep, do_pair, jnp.zeros_like(do_pair))
            delta = jnp.sum(jnp.where(keep, product, 0.0), axis=-1, keepdims=True)
            probs = p_ref[0, head]
            dprobs = dot(do_head, v_pair, 1, 1)
            ds = probs.astype(F32) * (dprobs - delta)
            ds_low = ds.astype(BF16)
            sums = {}
            for i in range(blocks):
                for j in range(blocks):
                    place = max(-2, min(2, j - i)) + 2
                    tile = ds[i * BLK : (i + 1) * BLK, j * BLK : (j + 1) * BLK]
                    sums[place] = tile if place not in sums else sums[place] + tile
            for place, value in sums.items():
                acc_ref[head, :, place * BLK : (place + 1) * BLK] += value
            dq_parts.append(dot(ds_low, k_pair))
            own = slice(part * head_size, (part + 1) * head_size)
            place = pl.ds(pl.multiple_of(head * head_size, head_size), head_size)
            dkt_ref[place, :] = dot(q_turned[own], ds_low).astype(BF16)
            dvt_ref[place, :] = dot(do_turned[own], probs).astype(BF16)
        dqkv_ref[0, 0, :, lanes] = jnp.where(low_lane, dq_parts[0], dq_parts[1]).astype(BF16)
        return carry

    lax.fori_loop(0, heads // 2, pair, 0)
    dq = dqkv_ref[0, 0]
    dk = dkt_ref[...].T
    dv = dvt_ref[...].T
    dqkv_ref[0, 1] = dk
    dqkv_ref[0, 2] = dv
    parts = [dot(n1_ref[0], d, 0, 0) for d in (dq, dk, dv)]

    here = slice(group * own_width, (group + 1) * own_width)
    if len(grad_refs) == 1:
        here = slice(0, own_width)

    @pl.when(step == 0)
    def _():
        for index in range(3):
            wacc_ref[index * width : (index + 1) * width, here] = parts[index]

    @pl.when(step > 0)
    def _():
        for index in range(3):
            wacc_ref[index * width : (index + 1) * width, here] += parts[index]

    @pl.when(step == last)
    def _():
        if len(grad_refs) == 1:
            grad_refs[0][...] = wacc_ref[...].astype(BF16)
        else:
            for index, ref in enumerate(before_refs):
                lanes = slice(index * own_width, (index + 1) * own_width)
                wacc_ref[: 3 * width, lanes] = ref[...].astype(F32)
            if wacc_ref.shape[0] > 3 * width:
                wacc_ref[3 * width :, :] = jnp.zeros_like(wacc_ref[3 * width :, :])
            take_chunks(wacc_ref, grad_refs[0], grad_refs[1], where_ref[0], masks)
        for head in range(heads):
            far_low = jnp.sum(acc_ref[head, :, :BLK], axis=0, keepdims=True)
            far_high = jnp.sum(acc_ref[head, :, 4 * BLK :], axis=0, keepdims=True)
            band = jnp.concatenate(
                [acc_ref[head, :, BLK : 4 * BLK], jnp.zeros((BLK, BLK), F32)], axis=1
            )
            rows = BLK // 2
            while rows >= 1:
                band = band[:rows] + pltpu.roll(band[rows:], 4 * BLK - rows, 1)
                rows //= 2
            band_ref[head : head + 1, : 4 * BLK] = band
            band_ref[head : head + 1, 4 * BLK : 5 * BLK] = far_low
            band_ref[head : head + 1, 5 * BLK :] = far_high


def attn_back(where, n1, q, k, v, probs, mixed, do, before, groups, masks):
    group = len(before)
    rows, length, width = n1.shape
    heads = probs.shape[1] // groups
    own_width = width // groups
    lanes = pl.BlockSpec((1, length, own_width), lambda r: (r, 0, group))
    low = lambda *s: jax.ShapeDtypeStruct(s, BF16)
    if group < groups - 1:
        grads = [low(3 * width, own_width)]
        acc = (3 * width, own_width)
    else:
        lines = padded_rows(3 * width, len(masks))
        grads = [low(lines // 2, width)] * 2
        acc = (lines, width)
    return pl.pallas_call(
        functools.partial(attn_back_kernel, group=group, masks=masks),
        name=f"attn_back_{group}",
        grid=(rows,),
        in_specs=[pl.BlockSpec(memory_space=pltpu.SMEM), per_row((length, width))]
        + [lanes] * 3
        + [pl.BlockSpec((1, heads, length, length), lambda r: (r, group, 0, 0)), lanes, lanes]
        + [whole(g.shape) for g in before],
        out_specs=[per_row((3, length, own_width)), whole((heads, 6 * BLK))]
        + [whole(g.shape) for g in grads],
        out_shape=[
            low(rows, 3, length, own_width),
            jax.ShapeDtypeStruct((heads, 6 * BLK), F32),
        ]
        + grads,
        scratch_shapes=[
            pltpu.VMEM((own_width, length), BF16),
            pltpu.VMEM((own_width, length), BF16),
            pltpu.VMEM((heads, BLK, 5 * BLK), F32),
            pltpu.VMEM(acc, F32),
        ],
        compiler_params=pltpu.CompilerParams(vmem_limit_bytes=VMEM_SMALL),
    )(where, n1, q, k, v, probs, mixed, do, *before)


def finish_kernel(*refs, groups):
    tok_ref, dh_ref, g1_ref, g2grad_ref, table_ref, wq_ref, wk_ref, wv_ref = refs[:8]
    dqkv_refs, band_refs = refs[8 : 8 + groups], refs[8 + groups : 8 + 2 * groups]
    tgrad_ref, small_out, g1_acc, small_ref = refs[8 + 2 * groups :]
    step = pl.program_id(0)
    last = pl.num_programs(0) - 1
    own_width = dqkv_refs[0].shape[3]
    heads = band_refs[0].shape[0]
    dn1 = None
    for index, weight in enumerate((wq_ref, wk_ref, wv_ref)):
        whole_grad = jnp.concatenate([ref[0, index] for ref in dqkv_refs], axis=1)
        part = dot(whole_grad, weight[...], 1, 1)
        dn1 = part if dn1 is None else dn1 + part
    x = tok_ref[0].astype(F32)
    scale = rms_scale(x)
    g1_part = jnp.sum(dn1 * x * scale, axis=0, keepdims=True)
    tgrad_ref[0] = (dh_ref[0] + norm_back(dn1, x, scale, gain_row(g1_ref))).astype(BF16)

    @pl.when(step == 0)
    def _():
        g1_acc[...] = g1_part

    @pl.when(step > 0)
    def _():
        g1_acc[...] += g1_part

    @pl.when(step == last)
    def _():
        width = small_ref.shape[1]
        small_ref[...] = jnp.zeros_like(small_ref)
        for at in range(width // BLK):
            lanes = slice(at * BLK, (at + 1) * BLK)
            small_ref[at : at + 1, BLK : 2 * BLK] = g1_acc[:, lanes]
            small_ref[at : at + 1, 2 * BLK : 3 * BLK] = g2grad_ref[:, lanes]
        for group in range(groups):
            band = band_refs[group][...]
            high = band.astype(BF16)
            rest = band - high.astype(F32)
            low = rest.astype(BF16)
            least = (rest - low.astype(F32)).astype(BF16)
            table = table_ref[...]
            bias = dot(high, table) + dot(low, table) + dot(least, table)
            small_ref[group * heads : (group + 1) * heads, : bias.shape[1]] = bias
        small_out[...] = small_ref[...].astype(BF16)


def finish(tokens, dh, g1, g2grad, table, wq, wk, wv, dqkvs, bands):
    rows, length, width = tokens.shape
    groups = len(dqkvs)
    lead = groups * bands[0].shape[0]
    return pl.pallas_call(
        functools.partial(finish_kernel, groups=groups),
        name="finish_rows",
        grid=(rows,),
        in_specs=[per_row((length, width))] * 2
        + [whole(a.shape) for a in (g1, g2grad, table, wq, wk, wv)]
        + [per_row(d.shape[1:]) for d in dqkvs]
        + [whole(b.shape) for b in bands],
        out_specs=[per_row((length, width)), whole((lead, width))],
        out_shape=[
            jax.ShapeDtypeStruct(tokens.shape, BF16),
            jax.ShapeDtypeStruct((lead, width), BF16),
        ],
        scratch_shapes=[pltpu.VMEM((1, width), F32), pltpu.VMEM((lead, width), F32)],
        compiler_params=pltpu.CompilerParams(vmem_limit_bytes=VMEM_SMALL),
    )(tokens, dh, g1, g2grad, table, wq, wk, wv, *dqkvs, *bands)


def band_table(length):
    buckets = bucket_offsets(length)
    zero = length - 1
    table = np.zeros((6 * BLK, NB), np.float32)
    for column in range(4 * BLK):
        offset = column - BLK if column < 3 * BLK else column - 5 * BLK
        if -2 * BLK < offset < 2 * BLK and abs(offset) < length:
            table[column, buckets[zero + offset]] = 1.0
    far = buckets[: zero - BLK], buckets[zero + BLK + 1 :]
    assert len(set(far[0])) == 1 and len(set(far[1])) == 1
    table[4 * BLK : 5 * BLK, far[0][0]] = 1.0
    table[5 * BLK :, far[1][0]] = 1.0
    return table


def unpack_big_kernel(where_ref, near_ref, far_ref, win_out, wo_out, all_ref, *, masks):
    total = len(masks)
    width = wo_out.shape[1]
    chunk = 2 * near_ref.shape[0] // total
    for p in range(total):
        ref, at = (near_ref, p) if p < total // 2 else (far_ref, p - total // 2)
        first = pl.multiple_of((where_ref[0] ^ masks[p]) * chunk, chunk)
        all_ref[pl.ds(first, chunk), :] = ref[at * chunk : (at + 1) * chunk, :].astype(F32)
    parts = win_out.shape[1] // width
    for part in range(parts):
        win_out[:, part * width : (part + 1) * width] = all_ref[part * width : (part + 1) * width, :]
    wo_out[...] = all_ref[parts * width : (parts + 1) * width, :]


def unpack_big(where, near, far, inner, width, masks):
    vmem = pl.BlockSpec(memory_space=pltpu.VMEM)
    return pl.pallas_call(
        functools.partial(unpack_big_kernel, masks=masks),
        name="unpack_ffn",
        in_specs=[pl.BlockSpec(memory_space=pltpu.SMEM), vmem, vmem],
        out_shape=[
            jax.ShapeDtypeStruct((width, inner), F32),
            jax.ShapeDtypeStruct((width, width), F32),
        ],
        scratch_shapes=[pltpu.VMEM((2 * near.shape[0], width), F32)],
        compiler_params=pltpu.CompilerParams(vmem_limit_bytes=VMEM_SMALL),
    )(where, near, far)


def unpack_qkv_kernel(
    where_ref, near_ref, far_ref, wq_out, wk_out, wv_out, g1_out, g2_out, bias_out,
    all_ref, small_all, *, masks
):
    total = len(masks)
    width = wq_out.shape[1]
    lead = bias_out.shape[0]
    rows = 2 * near_ref.shape[0] // total
    chunk = rows - lead
    for p in range(total):
        ref, at = (near_ref, p) if p < total // 2 else (far_ref, p - total // 2)
        owner = where_ref[0] ^ masks[p]
        piece = ref[at * rows : (at + 1) * rows, :].astype(F32)
        all_ref[pl.ds(pl.multiple_of(owner * chunk, chunk), chunk), :] = piece[:chunk]
        small_all[pl.ds(pl.multiple_of(owner * lead, lead), lead), :] = piece[
            chunk:, : small_all.shape[1]
        ]
    small = small_all[:lead, :]
    for p in range(1, total):
        small = small + small_all[p * lead : (p + 1) * lead, :]
    for index, ref in enumerate((wq_out, wk_out, wv_out)):
        ref[...] = all_ref[index * width : (index + 1) * width, :]
    for at in range(width // BLK):
        lanes = slice(at * BLK, (at + 1) * BLK)
        g1_out[:, lanes] = small[at : at + 1, BLK : 2 * BLK]
        g2_out[:, lanes] = small[at : at + 1, 2 * BLK : 3 * BLK]
    bias_out[...] = small[:, : bias_out.shape[1]]


def unpack_qkv(where, near, far, width, heads, masks):
    full = lambda *s: jax.ShapeDtypeStruct(s, F32)
    vmem = pl.BlockSpec(memory_space=pltpu.VMEM)
    total = len(masks)
    return pl.pallas_call(
        functools.partial(unpack_qkv_kernel, masks=masks),
        name="unpack_attn",
        in_specs=[pl.BlockSpec(memory_space=pltpu.SMEM), vmem, vmem],
        out_shape=[full(width, width)] * 3 + [full(1, width)] * 2 + [full(heads, NB)],
        scratch_shapes=[
            pltpu.VMEM((2 * near.shape[0] - total * heads, width), F32),
            pltpu.VMEM((total * heads, 3 * BLK), F32),
        ],
        compiler_params=pltpu.CompilerParams(vmem_limit_bytes=VMEM_SMALL),
    )(where, near, far)


def bit_groups(wide, narrow):
    total = wide * narrow
    assert total & (total - 1) == 0 and narrow & (narrow - 1) == 0
    bits = [1 << s for s in range(total.bit_length() - 1)]
    outer = [b for b in bits if b >= narrow]
    inner = [b for b in bits if b < narrow]
    pairs = lambda items: [items[i : i + 2] for i in range(0, len(items), 2)]
    return [outer[:1]] + pairs(outer[1:]) + pairs(inner)


def group_masks(group):
    return chunk_masks(group)[1:]


def swap(values, mask, total):
    return lax.ppermute(values, AXES, [(i, i ^ mask) for i in range(total)])


def after(values, *others):
    return lax.optimization_barrier((values,) + others)[0]


def split_rows(values, count):
    rows = values.shape[0] // count
    return [values[i * rows : (i + 1) * rows] for i in range(count)]


class Gather:
    def __init__(self, values, groups, total):
        self.pieces, self.left, self.total = [values], list(reversed(groups)), total

    def step(self, *hold):
        if self.left:
            values = self.pieces[0]
            if len(self.pieces) > 1:
                pieces = lax.optimization_barrier(tuple(self.pieces) + hold)[: len(self.pieces)]
                values = jnp.concatenate(pieces, axis=0)
            masks = group_masks(self.left.pop(0))
            self.pieces = [values] + [swap(values, mask, self.total) for mask in masks]

    def rest(self):
        while self.left:
            self.step()
        return self.pieces


class Scatter:
    def __init__(self, blocks, groups, total):
        self.blocks, self.left, self.total = list(blocks), list(groups), total

    def step(self, *hold):
        if self.left:
            masks = group_masks(self.left.pop(0))
            got = [swap(b, mask, self.total) for b, mask in zip(self.blocks[1:], masks)]
            if hold:
                got = list(lax.optimization_barrier(tuple(got) + hold)[: len(got)])
            count = 1 << len(self.left[0]) if self.left else 1
            parts = [split_rows(b, count) for b in [self.blocks[0]] + got]
            self.blocks = []
            for column in zip(*parts):
                value = column[0].astype(F32)
                for other in column[1:]:
                    value = value + other.astype(F32)
                self.blocks.append(value.astype(BF16))

    def rest(self):
        while self.left:
            self.step()
        return self.blocks[0]


GROUPS = 2


def local(
    tokens, seg_ids, positives, norm1_gain, w_query, w_key, w_value, w_attn_out,
    rel_bias, norm2_gain, w_in, w_ffn_out, w_proj,
):
    rows, length, width = tokens.shape
    heads = rel_bias.shape[1]
    slots = length // QLEN
    inner = w_in.shape[1]
    wide, narrow = lax.axis_size("wide"), lax.axis_size("narrow")
    total = wide * narrow
    linear = lax.axis_index("wide") * narrow + lax.axis_index("narrow")
    where = jnp.full((1,), linear, jnp.int32)
    groups = bit_groups(wide, narrow)
    masks = chunk_masks([b for g in groups for b in g])
    buckets = bucket_offsets(length)
    hot = np.zeros((NB, 2 * length), np.float32)
    hot[buckets, np.arange(2 * length - 1)] = 1.0

    n1, q, k, v, probs, mixed, hidden, n2, act, abar, pooled = forward(
        seg_ids, tokens, norm1_gain, w_query, w_key, w_value, w_attn_out, rel_bias.T,
        jnp.asarray(hot, BF16), norm2_gain, w_in, w_ffn_out, slots,
    )
    slot = Gather(pooled, groups, total)
    slot.step()
    slot.step()
    acts = Gather(abar, groups, total)
    acts.step()
    slot.step(*acts.pieces)
    near, far = slot.rest()
    loss, grad_proj, dm_own, dm_low = contrast_call(
        where, near, far, positives, w_proj, slots, masks
    )
    dh, do, big_keep, big_send, grad_g2 = ffn_back(
        where, seg_ids, dm_own, act, n2, hidden, mixed, norm2_gain, w_in, w_ffn_out, w_attn_out,
        masks,
    )
    acts.step(do)
    big = Scatter([big_keep, big_send], groups, total)
    dqkvs, bands, before, tie = [], [], [], acts.pieces[:1]
    for _ in range(GROUPS):
        dqkv, band, *grads = attn_back(
            where, n1, q, k, v, probs, mixed, after(do, *tie), before, GROUPS, masks
        )
        dqkvs.append(dqkv)
        bands.append(band)
        before = before + grads[:1]
        if len(before) == 1:
            big.step(band)
            acts.step(band)
            tie = big.blocks + acts.pieces[:1]
    tokens_grad, small = finish(
        tokens, dh, norm1_gain, grad_g2, jnp.asarray(band_table(length), BF16),
        w_query, w_key, w_value, dqkvs, bands,
    )
    big.step(small)
    qkv = Scatter([grads[0], after(grads[1], *big.blocks)], groups, total)
    qkv.step()
    big.step(*qkv.blocks)
    big_all = Gather(big.rest(), groups, total)
    big_all.step()
    qkv.step(big_all.pieces[0])
    big_all.step(*qkv.blocks)
    qkv.step(big_all.pieces[0])
    qkv_all = Gather(jnp.concatenate([qkv.rest(), small], axis=0), groups, total)
    qkv_all.step()
    grad_ffn_out = ffn_out_grad(where, *acts.rest(), after(dm_low, *qkv_all.pieces), masks)
    qkv_all.step(grad_ffn_out)
    big_all.step(qkv_all.pieces[0])
    win, wo = unpack_big(where, *big_all.rest(), inner, width, masks)
    qkv_all.step(wo)
    wq, wk, wv, grad_g1, grad_g2, grad_bias = unpack_qkv(
        where, *qkv_all.rest(), width, heads, masks
    )
    return (
        loss[0, 0],
        tokens_grad,
        grad_g1[0],
        wq,
        wk,
        wv,
        wo,
        grad_bias.T,
        grad_g2[0],
        win,
        grad_ffn_out,
        grad_proj,
    )


def solution(mesh):
    rows = P(AXES, None, None)
    in_specs = (rows, P(AXES, None)) + (P(),) * 11
    out_specs = (P(), rows) + (P(),) * 10
    return jax.shard_map(local, mesh=mesh, in_specs=in_specs, out_specs=out_specs, check_vma=False)
```
